256 devices in a mesh: patch: 64 (over z, y, core), sub: 4 (over x).
Axes of the slice: x: 4, y: 4, z: 8, core: 2. Of those that a mesh axis runs over, the one named last changes fastest.
Arguments:
- sources: int32 [128, 16], replicated, may hold values from 0 to 131071
- diag_coef: float32 [131072], P(('patch', 'sub')), may hold values from 1 to 2
- tiles: float32 [1024, 6, 128, 128], P(('patch', 'sub')), may hold values from -0.109375 to 0.109375
- tile_cols: int32 [1024, 6], P(('patch', 'sub')), may hold values from 0 to 7
- send_rows: int32 [256, 4, 128], P(('patch', 'sub')), may hold values from 0 to 511
- recv_rows: int32 [256, 512], P(('patch', 'sub')), may hold values from 0 to 511, each once within a row
- bounds: float32 [2], replicated, may hold values from 0.3 to 3.2, as said below
Outputs:
- solution: float32 [131072, 128], P(('patch', 'sub'))
- res_norm: float32 [128], replicated
The draws below stay inside these ranges and needn't reach their ends.
Inputs may be any that keep to these rules, and one draw needn't show every extreme that they name: bounds[0] lies in 0.3 to 0.5 and bounds[1] in 2.6 to 3.2.
All inputs are finite; a program needn't handle non-finite values.
Results may differ from the reference program's by a relative error of at most 0.0001.
Values sent between devices are 32-bit elements; how exact they have to be, the bound alone decides.
A program may use at most 64 MiB of HBM per device.

```python
import jax
import jax.numpy as jnp
from jax import lax

BLOCK = 128
BLK_DEV = 4
NB = 6
K = 128
S = 128
ITERS = 8
V_DEV = 512
VERTS = 131072
BLOCKS = 1024
H = 512
HB = 4
NSRC = 16
N_PATCH = 64
N_SUB = 4
DEVICES = 256


def draw_bounds(key, part):
    first_key, second_key = jax.random.split(key)
    lower_end = jax.random.uniform(first_key, (), jnp.float32, 0.3, 0.5)
    upper_end = jax.random.uniform(second_key, (), jnp.float32, 2.6, 3.2)
    return jnp.stack([lower_end, upper_end]).astype(jnp.float32)


def with_ends(drawn, own_key, smallest, largest):
    longest = drawn.shape.index(max(drawn.shape))
    spots = []
    for shift in (0, 1):
        where = [jax.random.randint(jax.random.fold_in(own_key, axis), (), 0, length) for axis, length in enumerate(drawn.shape)]
        where[longest] = (where[longest] + shift) % drawn.shape[longest]
        spots.append(tuple(where))
    return drawn.at[spots[0]].set(smallest).at[spots[1]].set(largest)


def block_scale(rng, extent, cuts, low, high):
    def one(position, shards_of):
        draws = jax.random.uniform(jax.random.fold_in(jax.random.fold_in(rng, 6), position), (shards_of,), jnp.float32, low / len(cuts), high / len(cuts))
        return jnp.repeat(jnp.exp(draws), extent[position] // shards_of).reshape((-1,) + (1,) * (len(extent) - position - 1))

    level = one(*cuts[0])
    for cut in cuts[1:]:
        level = level * one(*cut)
    return level


def noise(key, dims, width, most, pieces=(), held_as=jnp.bfloat16):
    values = width * jax.random.normal(key, dims, jnp.float32)
    if pieces:
        values = values * block_scale(key, dims, pieces, -0.22, 0.18)
    return jnp.clip(values, -most, most).astype(held_as)


def setup_inputs(seed: int = 0) -> dict:
    keys = jax.random.split(jax.random.key(seed), 8)
    sources = with_ends(jax.random.randint(keys[0], (K, NSRC), 0, VERTS), jax.random.fold_in(keys[0], 1), 0, VERTS - 1).astype(jnp.int32)
    diag_coef = jnp.clip(1.0 + 1.0 * jax.random.uniform(keys[1], (VERTS,), jnp.float32) ** block_scale(keys[1], (VERTS,), ((0, 256),), -0.2, 0.2), 1.0, 2.0)
    tiles = noise(keys[2], (BLOCKS, NB, BLOCK, BLOCK), (4 * NB * BLOCK) ** -0.5, 0.109375, ((0, 256),), jnp.float32)
    tile_cols = with_ends(jax.random.randint(keys[3], (BLOCKS, NB), 0, BLK_DEV + HB), jax.random.fold_in(keys[3], 1), 0, (BLK_DEV + HB) - 1).astype(jnp.int32)
    send_rows = with_ends(jax.random.randint(keys[4], (DEVICES, 4, S), 0, V_DEV), jax.random.fold_in(keys[4], 1), 0, V_DEV - 1).astype(jnp.int32)
    recv_rows = jax.vmap(lambda own: jax.random.permutation(own, H))(jax.random.split(keys[5], DEVICES)).reshape((DEVICES, H)).astype(jnp.int32)
    bounds = draw_bounds(jax.random.fold_in(keys[7], 71), 0)
    return dict(sources=sources, diag_coef=diag_coef, tiles=tiles, tile_cols=tile_cols, send_rows=send_rows, recv_rows=recv_rows, bounds=bounds)


def build_right(sources, total_rows):
    columns = sources.shape[0]
    which = jnp.arange(columns, dtype=jnp.int32)[:, None]
    flat_index = (sources * columns + which).reshape(-1)
    counts = jax.ops.segment_sum(jnp.ones(flat_index.shape, jnp.float32), flat_index, num_segments=total_rows * columns)
    return counts.reshape(total_rows, columns)

def pick_rows(values, index):
    return values[index]

def operate(field, diag_coef, tiles, tile_cols, send_rows, recv_rows):
    devices = N_PATCH * N_SUB
    rows = BLK_DEV * BLOCK
    columns = field.shape[1]
    local = field.reshape(devices, rows, columns)
    packed = jax.vmap(pick_rows)(local, send_rows)
    packed = packed.reshape(N_PATCH, N_SUB, 4, S, columns)
    below_patch = jnp.roll(packed[:, :, 1], 1, axis=0)
    above_patch = jnp.roll(packed[:, :, 0], -1, axis=0)
    below_sub = jnp.roll(packed[:, :, 3], 1, axis=1)
    above_sub = jnp.roll(packed[:, :, 2], -1, axis=1)
    received = jnp.concatenate([below_patch, above_patch, below_sub, above_sub], axis=2)
    received = received.reshape(devices, 4 * S, columns)
    halo_rows = jax.vmap(pick_rows)(received, recv_rows)
    extended = jnp.concatenate([local, halo_rows], axis=1).reshape(devices, BLK_DEV + HB, BLOCK, columns)
    tile_blocks = tiles.reshape(devices, BLK_DEV, NB, BLOCK, BLOCK)
    col_blocks = tile_cols.reshape(devices, BLK_DEV, NB)

    def device_product(inputs):
        dev_tiles, dev_cols, dev_ext = inputs
        summed = jnp.zeros((BLK_DEV, BLOCK, columns), jnp.float32)
        for slot_index in range(NB):
            summed = summed + jnp.einsum('bij,bjk->bik', dev_tiles[:, slot_index], dev_ext[dev_cols[:, slot_index]], precision=lax.Precision.HIGHEST)
        return summed
    coupled = lax.map(device_product, (tile_blocks, col_blocks, extended)).reshape(devices * rows, columns)
    return diag_coef[:, None] * field + coupled

def reference(sources, diag_coef, tiles, tile_cols, send_rows, recv_rows, bounds):
    right_side = build_right(sources, VERTS)
    centre = (bounds[0] + bounds[1]) / 2.0
    half_width = (bounds[1] - bounds[0]) / 2.0
    ratio = centre / half_width
    damping = 1.0 / ratio
    solution = jnp.zeros_like(right_side)
    residual = right_side
    direction = right_side / centre
    for iteration in range(ITERS):
        solution = solution + direction
        residual = residual - operate(direction, diag_coef, tiles, tile_cols, send_rows, recv_rows)
        if iteration + 1 < ITERS:
            damping_next = 1.0 / (2.0 * ratio - damping)
            direction = damping_next * damping * direction + 2.0 * damping_next / half_width * residual
            damping = damping_next
    final = right_side - operate(solution, diag_coef, tiles, tile_cols, send_rows, recv_rows)
    res_norm = jnp.sqrt(lax.optimization_barrier(jnp.sum(final * final, axis=0)))
    return (solution, res_norm)
```

```python
import functools

import jax
import jax.numpy as jnp
from jax import lax
from jax.experimental import pallas as pl
from jax.experimental.pallas import tpu as pltpu
from jax.sharding import PartitionSpec as P

MESH = pl.DeviceIdType.MESH
ITERS = 8
GROUPS = 2
PLANES = 8
CUT = 256

NT = (((1,), (1,)), ((), ()))


def dot(a, b):
    return jnp.dot(a, b, preferred_element_type=jnp.float32)


def dot_nt(a, b):
    return lax.dot_general(a, b, NT, preferred_element_type=jnp.float32)


def split(value):
    high = value.astype(jnp.bfloat16)
    low = (value - high.astype(jnp.float32)).astype(jnp.bfloat16)
    return high, low


def one_hot(equal):
    return jnp.where(equal, 1.0, 0.0).astype(jnp.bfloat16)


def kernel(
    shape,
    src_hbm,
    diag_hbm,
    cols_hbm,
    send_hbm,
    recv_hbm,
    bounds_hbm,
    tiles_hbm,
    x_out,
    norm_out,
    src_lanes,
    diag,
    cols,
    send_rows,
    recv_rows,
    bounds,
    tiles,
    place,
    pick,
    tile_pair,
    w_high,
    w_low,
    ext,
    b_own,
    r_own,
    d_own,
    x_own,
    r_pack,
    d_pack,
    x_pack,
    part,
    coef,
    send_buf,
    recv_buf,
    plane_send,
    plane_recv,
    axis_send,
    axis_recv,
    load_sems,
    send_sem,
    recv_sem,
    norm_sems,
):
    n_patch, n_sub, planes = shape
    f32 = jnp.float32
    k_all, rows = b_own.shape
    per_row = tiles.shape[1]
    blk_rows = tiles.shape[0]
    tile = tiles.shape[2]
    n_blocks = place.shape[0]
    halo_blocks = n_blocks - blk_rows
    dirs = 4
    groups = send_sem.shape[1]
    k_group = k_all // groups

    p = lax.axis_index("patch")
    s = lax.axis_index("sub")
    plane = n_patch // planes
    in_plane = plane * n_sub
    my_plane = lax.div(p, plane)
    my_patch = lax.rem(p, plane)
    my_slot = my_patch * n_sub + s

    p_next = lax.rem(p + 1, n_patch)
    p_prev = lax.rem(p + n_patch - 1, n_patch)
    s_next = lax.rem(s + 1, n_sub)
    s_prev = lax.rem(s + n_sub - 1, n_sub)
    targets = ((p_prev, s), (p_next, s), (p, s_prev), (p, s_next))
    lands = (1, 0, 3, 2)

    def plane_target(offset):
        slot = lax.rem(my_slot + offset, in_plane)
        return (my_plane * plane + lax.div(slot, n_sub), lax.rem(slot, n_sub))

    def axis_target(offset):
        return (lax.rem(my_plane + offset, planes) * plane + my_patch, s)

    loads = [
        pltpu.make_async_copy(source, target, load_sems.at[i])
        for i, (source, target) in enumerate(
            (
                (src_hbm, src_lanes),
                (send_hbm, send_rows),
                (bounds_hbm, bounds),
                (recv_hbm, recv_rows),
                (cols_hbm, cols),
                (diag_hbm, diag),
                (tiles_hbm, tiles),
            )
        )
    ]
    for load in loads:
        load.start()
    barrier = pltpu.get_barrier_semaphore()
    greeted = 0
    for target in targets:
        pl.semaphore_signal(barrier, inc=1, device_id=target, device_id_type=MESH)
        greeted += 1
    for offset in range(1, in_plane):
        pl.semaphore_signal(barrier, inc=1, device_id=plane_target(offset), device_id_type=MESH)
        greeted += 1
    for offset in range(1, planes):
        pl.semaphore_signal(barrier, inc=1, device_id=axis_target(offset), device_id_type=MESH)
        greeted += 1

    for load in loads[:3]:
        load.wait()

    lower = jnp.full((8, rows), bounds[0], f32)
    upper = jnp.full((8, rows), bounds[1], f32)
    centre = (lower + upper) / 2.0
    half_width = (upper - lower) / 2.0
    ratio = centre / half_width
    damping = 1.0 / ratio
    for step in range(ITERS - 1):
        following = 1.0 / (2.0 * ratio - damping)
        coef[2 * step] = following * damping
        coef[2 * step + 1] = 2.0 * following / half_width
        damping = following
    inverse = (1.0 / centre)[0:1]

    first = (p * n_sub + s) * rows
    src = jnp.transpose(src_lanes[...])
    lane = lax.broadcasted_iota(jnp.int32, (1, tile), 1) + first
    chunk = 32
    for start in range(0, k_all, chunk):
        ids = [send_rows[j : j + 1, :] + first for j in range(dirs)]
        sums = [jnp.zeros((chunk, tile), f32) for _ in ids]
        for source in range(src.shape[1]):
            wide = jnp.broadcast_to(src[start : start + chunk, source : source + 1], (chunk, tile))
            sums = [jnp.where(wide == v, a + 1.0, a) for v, a in zip(ids, sums)]
        for j, total in enumerate(sums):
            r_pack[start : start + chunk, j * tile : (j + 1) * tile] = total
            scaled = total * inverse[:, :tile]
            d_pack[start : start + chunk, j * tile : (j + 1) * tile] = scaled
            x_pack[start : start + chunk, j * tile : (j + 1) * tile] = scaled
            send_buf[0, j, start : start + chunk, :] = scaled

    pl.semaphore_wait(barrier, greeted)

    def send(step, group, j):
        rows_of = pl.ds(group * k_group, k_group)
        return pltpu.make_async_remote_copy(
            src_ref=send_buf.at[step, j, rows_of, :],
            dst_ref=recv_buf.at[step, lands[j], rows_of, :],
            send_sem=send_sem.at[step, group, j],
            recv_sem=recv_sem.at[step, group, lands[j]],
            device_id=targets[j],
            device_id_type=MESH,
        )

    def start_sends(step, group):
        for j in (2, 3, 0, 1):
            send(step, group, j).start()

    def wait_recvs(step, group):
        for j in (0, 1, 2, 3):
            send(step, group, j).wait_recv()

    def wait_sends(step):
        for group in range(groups):
            for j in range(dirs):
                send(step, group, j).wait_send()

    for group in range(groups):
        start_sends(0, group)

    for start in range(0, k_all, chunk):
        sums = [jnp.zeros((chunk, tile), f32) for _ in range(blk_rows)]
        for source in range(src.shape[1]):
            wide = jnp.broadcast_to(src[start : start + chunk, source : source + 1], (chunk, tile))
            sums = [jnp.where(wide == lane + i * tile, a + 1.0, a) for i, a in enumerate(sums)]
        for i, total in enumerate(sums):
            where = (slice(start, start + chunk), slice(i * tile, (i + 1) * tile))
            b_own[where] = total
            r_own[where] = total
            scaled = total * inverse[:, :tile]
            d_own[where] = scaled
            x_own[where] = scaled
            high, low = split(scaled)
            ext[start : start + chunk, i * tile : (i + 1) * tile] = high
            ext[k_all + start : k_all + start + chunk, i * tile : (i + 1) * tile] = low

    loads[3].wait()

    eye = lax.broadcasted_iota(jnp.int32, (tile, tile), 0) == lax.broadcasted_iota(jnp.int32, (tile, tile), 1)
    row_id = lax.broadcasted_iota(jnp.int32, (rows, tile), 0)
    for c in range(n_blocks):
        if c < blk_rows:
            place[c] = jnp.zeros(place.shape[1:], jnp.bfloat16)
            place[c, c * tile : (c + 1) * tile, :] = one_hot(eye)
        else:
            h = c - blk_rows
            place[c, 0:rows, :] = jnp.zeros((rows, tile), jnp.bfloat16)
            place[c, rows : 2 * rows, :] = one_hot(recv_rows[:, h * tile : (h + 1) * tile] == row_id)
    for j in range(dirs):
        pick[:, j * tile : (j + 1) * tile] = one_hot(send_rows[j : j + 1, :] == row_id)

    for load in loads[4:]:
        load.wait()

    for b in range(blk_rows):
        for n in range(per_row):
            high, low = split(tiles[b, n])
            tile_pair[0:tile, n * tile : (n + 1) * tile] = high
            tile_pair[tile : 2 * tile, n * tile : (n + 1) * tile] = low
        pair = tile_pair[...]
        for start in range(0, 2 * rows, CUT):
            spots = [place[cols[b, n], start : start + CUT, :] for n in range(per_row)]
            both = dot_nt(jnp.concatenate(spots, axis=1), pair)
            block = both[:, :tile] + both[:, tile:]
            offset = b * tile - start
            if 0 <= offset < CUT:
                extra = jnp.where(eye, diag[b : b + 1, :], 0.0)
                pieces = [jnp.zeros((tile, tile), f32)] * (CUT // tile)
                pieces[offset // tile] = extra
                block = block + jnp.concatenate(pieces, axis=0)
            high, low = split(block)
            w_high[start : start + CUT, b * tile : (b + 1) * tile] = high
            w_low[start : start + CUT, b * tile : (b + 1) * tile] = low

    for start in range(0, 2 * rows, CUT):
        for weights in (w_high, w_low):
            weights[start : start + CUT, rows : 2 * rows] = dot(
                weights[start : start + CUT, 0:rows], pick[...]
            ).astype(jnp.bfloat16)

    def product(k_rows, n_cols):
        both = dot(ext[:, k_rows], w_high[k_rows, n_cols])
        return both[:k_all] + both[k_all:] + dot(ext[0:k_all, k_rows], w_low[k_rows, n_cols])

    own, got = slice(0, rows), slice(rows, 2 * rows)

    def packed_part():
        for start in range(0, rows, CUT):
            part[:, start : start + CUT] = product(own, slice(rows + start, rows + start + CUT))

    packed_part()

    def take_halo(step, group):
        at = pl.ds(group * k_group, k_group)
        wait_recvs(step, group)
        halo = jnp.concatenate([recv_buf[step, j, at, :] for j in range(dirs)], axis=1)
        return split(halo)

    def halo_product(high, low, n_cols):
        both = dot(jnp.concatenate([high, low], axis=0), w_high[got, n_cols])
        return both[:k_group] + both[k_group:] + dot(high, w_low[got, n_cols])

    def iteration(step, carry):
        alpha = coef[2 * step][0:1]
        beta = coef[2 * step + 1][0:1]
        last = (step == ITERS - 2).astype(f32)
        for group in range(groups):
            g0 = group * k_group
            at = slice(g0, g0 + k_group)
            high, low = take_halo(step, group)
            ext[at, got] = high
            ext[k_all + g0 : k_all + g0 + k_group, got] = low
            r_new = r_pack[at, :] - (part[at, :] + halo_product(high, low, slice(rows, 2 * rows)))
            d_new = alpha * d_pack[at, :] + beta * r_new
            x_old = x_pack[at, :]
            going = d_new + last * x_old
            for j in range(dirs):
                send_buf[step + 1, j, at, :] = going[:, j * tile : (j + 1) * tile]
            start_sends(step + 1, group)
            r_pack[at, :] = r_new
            d_pack[at, :] = d_new
            x_pack[at, :] = x_old + d_new
        wait_sends(step)
        for start in range(0, rows, CUT):
            at = slice(start, start + CUT)
            r_new = r_own[:, at] - product(slice(0, 2 * rows), at)
            d_new = alpha[:, at] * d_own[:, at] + beta[:, at] * r_new
            r_own[:, at] = r_new
            d_own[:, at] = d_new
        for start in range(0, rows, CUT):
            at = slice(start, start + CUT)
            d_new = d_own[:, at]
            x_old = x_own[:, at]
            x_own[:, at] = x_old + d_new
            high, low = split(d_new + last * x_old)
            ext[0:k_all, at] = high
            ext[k_all : 2 * k_all, at] = low
        packed_part()
        return carry

    lax.fori_loop(0, ITERS - 1, iteration, 0)

    for start in range(0, rows, CUT):
        at = slice(start, start + CUT)
        r_own[:, at] = b_own[:, at] - product(own, at)
    for i in range(blk_rows):
        x_out[i * tile : (i + 1) * tile, :] = jnp.transpose(x_own[:, i * tile : (i + 1) * tile])

    squares = []
    for group in range(groups):
        high, low = take_halo(ITERS - 1, group)
        final = r_own[group * k_group : (group + 1) * k_group, :] - halo_product(high, low, own)
        final = final * final
        total = final[:, 0:tile]
        for i in range(1, blk_rows):
            total = total + final[:, i * tile : (i + 1) * tile]
        squares.append(total)
    squares = jnp.transpose(jnp.concatenate(squares, axis=0))
    mine = jnp.sum(squares, axis=0, keepdims=True)

    plane_send[...] = mine
    plane_recv[my_slot] = mine
    plane_copies = [
        pltpu.make_async_remote_copy(
            src_ref=plane_send,
            dst_ref=plane_recv.at[my_slot],
            send_sem=norm_sems.at[0],
            recv_sem=norm_sems.at[1],
            device_id=plane_target(offset),
            device_id_type=MESH,
        )
        for offset in range(1, in_plane)
    ]
    for copy in plane_copies:
        copy.start()
    others = plane_recv.at[pl.ds(0, in_plane - 1)]
    pltpu.make_async_copy(others, others, norm_sems.at[1]).wait()
    mine = jnp.sum(plane_recv[...], axis=0)

    axis_send[...] = mine
    axis_recv[my_plane] = mine
    axis_copies = [
        pltpu.make_async_remote_copy(
            src_ref=axis_send,
            dst_ref=axis_recv.at[my_plane],
            send_sem=norm_sems.at[2],
            recv_sem=norm_sems.at[3],
            device_id=axis_target(offset),
            device_id_type=MESH,
        )
        for offset in range(1, planes)
    ]
    for copy in axis_copies:
        copy.start()
    wait_sends(ITERS - 1)
    pltpu.make_async_copy(others, others, norm_sems.at[0]).wait()
    others = axis_recv.at[pl.ds(0, planes - 1)]
    pltpu.make_async_copy(others, others, norm_sems.at[3]).wait()
    norm_out[...] = jnp.sqrt(jnp.sum(axis_recv[...], axis=0))
    pltpu.make_async_copy(others, others, norm_sems.at[2]).wait()


def on_device(n_patch, n_sub, planes, sources, diag_coef, tiles, tile_cols, send_rows, recv_rows, bounds):
    rows = diag_coef.shape[0]
    k_all = sources.shape[0]
    blk_rows, per_row, tile, _ = tiles.shape
    dirs = send_rows.shape[1]
    n_blocks = 2 * blk_rows
    f32, bf16 = jnp.float32, jnp.bfloat16
    vmem = pl.BlockSpec(memory_space=pltpu.VMEM)
    hbm = pl.BlockSpec(memory_space=pltpu.HBM)
    field = pltpu.VMEM((k_all, rows), f32)
    in_plane = n_patch // planes * n_sub
    x, norm = pl.pallas_call(
        functools.partial(kernel, (n_patch, n_sub, planes)),
        out_shape=(jax.ShapeDtypeStruct((rows, k_all), f32), jax.ShapeDtypeStruct((1, k_all), f32)),
        in_specs=[hbm] * 7,
        out_specs=(vmem, vmem),
        scratch_shapes=[
            pltpu.VMEM(sources.shape[::-1], jnp.int32),
            pltpu.VMEM((blk_rows, tile), f32),
            pltpu.SMEM(tile_cols.shape, jnp.int32),
            pltpu.VMEM(send_rows.shape[1:], jnp.int32),
            pltpu.VMEM(recv_rows.shape, jnp.int32),
            pltpu.SMEM(bounds.shape, f32),
            pltpu.VMEM(tiles.shape, f32),
            pltpu.VMEM((n_blocks, 2 * rows, tile), bf16),
            pltpu.VMEM((rows, rows), bf16),
            pltpu.VMEM((2 * tile, per_row * tile), bf16),
            pltpu.VMEM((2 * rows, 2 * rows), bf16),
            pltpu.VMEM((2 * rows, 2 * rows), bf16),
            pltpu.VMEM((2 * k_all, 2 * rows), bf16),
            field,
            field,
            field,
            field,
            field,
            field,
            field,
            field,
            pltpu.VMEM((2 * ITERS, 8, rows), f32),
            pltpu.VMEM((ITERS, dirs, k_all, tile), f32),
            pltpu.VMEM((ITERS, dirs, k_all, tile), f32),
            pltpu.VMEM((1, k_all), f32),
            pltpu.VMEM((in_plane, 1, k_all), f32),
            pltpu.VMEM((1, k_all), f32),
            pltpu.VMEM((planes, 1, k_all), f32),
            pltpu.SemaphoreType.DMA((7,)),
            pltpu.SemaphoreType.DMA((ITERS, GROUPS, dirs)),
            pltpu.SemaphoreType.DMA((ITERS, GROUPS, dirs)),
            pltpu.SemaphoreType.DMA((4,)),
        ],
        compiler_params=pltpu.CompilerParams(
            collective_id=0, has_side_effects=True, vmem_limit_bytes=67_043_328
        ),
    )(
        sources.T,
        diag_coef.reshape(blk_rows, tile),
        tile_cols,
        send_rows[0],
        recv_rows,
        bounds,
        tiles,
    )
    return x, norm[0]


def solution(mesh):
    n_patch, n_sub = mesh.shape["patch"], mesh.shape["sub"]
    both = ("patch", "sub")
    return jax.shard_map(
        functools.partial(on_device, n_patch, n_sub, PLANES),
        mesh=mesh,
        in_specs=(
            P(),
            P(both),
            P(both, None, None, None),
            P(both, None),
            P(both, None, None),
            P(both, None),
            P(),
        ),
        out_specs=(P(both, None), P()),
        check_vma=False,
    )
```

```python
import functools

import jax
import jax.numpy as jnp
from jax import lax
from jax.experimental import pallas as pl
from jax.experimental.pallas import tpu as pltpu
from jax.sharding import PartitionSpec as P

MESH = pl.DeviceIdType.MESH
ITERS = 8
GROUPS = 2
PLANES = 8
CUT = 256

NT = (((1,), (1,)), ((), ()))


def dot(a, b):
    return jnp.dot(a, b, preferred_element_type=jnp.float32)


def dot_nt(a, b):
    return lax.dot_general(a, b, NT, preferred_element_type=jnp.float32)


def split(value):
    high = value.astype(jnp.bfloat16)
    low = (value - high.astype(jnp.float32)).astype(jnp.bfloat16)
    return high, low


def one_hot(equal):
    return jnp.where(equal, 1.0, 0.0).astype(jnp.bfloat16)


def kernel(
    shape,
    src_hbm,
    diag_hbm,
    cols_hbm,
    send_hbm,
    recv_hbm,
    bounds_hbm,
    tiles_hbm,
    x_out,
    norm_out,
    src_lanes,
    diag,
    cols,
    send_rows,
    recv_rows,
    bounds,
    tiles,
    place,
    pick,
    tile_pair,
    w_high,
    w_low,
    ext,
    b_own,
    r_own,
    d_own,
    x_own,
    r_pack,
    d_pack,
    x_pack,
    part,
    coef,
    send_buf,
    recv_buf,
    plane_send,
    plane_recv,
    axis_send,
    axis_recv,
    load_sems,
    send_sem,
    recv_sem,
    norm_sems,
    out_buf,
    out_sem,
    hello_sems,
):
    n_patch, n_sub, planes = shape
    f32 = jnp.float32
    k_all, rows = b_own.shape
    per_row = tiles.shape[1]
    blk_rows = tiles.shape[0]
    tile = tiles.shape[2]
    n_blocks = place.shape[0]
    halo_blocks = n_blocks - blk_rows
    dirs = 4
    groups = send_sem.shape[1]
    k_group = k_all // groups

    p = lax.axis_index("patch")
    s = lax.axis_index("sub")
    plane = n_patch // planes
    in_plane = plane * n_sub
    my_plane = lax.div(p, plane)
    my_patch = lax.rem(p, plane)
    my_slot = my_patch * n_sub + s

    p_next = lax.rem(p + 1, n_patch)
    p_prev = lax.rem(p + n_patch - 1, n_patch)
    s_next = lax.rem(s + 1, n_sub)
    s_prev = lax.rem(s + n_sub - 1, n_sub)
    targets = ((p_prev, s), (p_next, s), (p, s_prev), (p, s_next))
    lands = (1, 0, 3, 2)

    def plane_target(offset):
        slot = lax.rem(my_slot + offset, in_plane)
        return (my_plane * plane + lax.div(slot, n_sub), lax.rem(slot, n_sub))

    def axis_target(offset):
        return (lax.rem(my_plane + offset, planes) * plane + my_patch, s)

    loads = [
        pltpu.make_async_copy(source, target, load_sems.at[i])
        for i, (source, target) in enumerate(
            (
                (src_hbm, src_lanes),
                (send_hbm, send_rows),
                (bounds_hbm, bounds),
                (recv_hbm, recv_rows),
                (cols_hbm, cols),
                (diag_hbm, diag),
                (tiles_hbm, tiles),
            )
        )
    ]
    for load in loads:
        load.start()
    barrier = pltpu.get_barrier_semaphore()
    greeted = 0
    for target in targets:
        pl.semaphore_signal(barrier, inc=1, device_id=target, device_id_type=MESH)
        greeted += 1
    for offset in (1, planes - 1):
        pl.semaphore_signal(barrier, inc=1, device_id=axis_target(offset), device_id_type=MESH)
        greeted += 1

    for load in loads[:3]:
        load.wait()

    lower = jnp.full((8, rows), bounds[0], f32)
    upper = jnp.full((8, rows), bounds[1], f32)
    centre = (lower + upper) / 2.0
    inverse = (1.0 / centre)[0:1]

    first = (p * n_sub + s) * rows
    src = jnp.transpose(src_lanes[...])
    lane = lax.broadcasted_iota(jnp.int32, (1, tile), 1) + first
    chunk = 32
    for start in range(0, k_all, chunk):
        ids = [send_rows[j : j + 1, :] + first for j in range(dirs)]
        sums = [jnp.zeros((chunk, tile), f32) for _ in ids]
        for source in range(src.shape[1]):
            wide = jnp.broadcast_to(src[start : start + chunk, source : source + 1], (chunk, tile))
            sums = [jnp.where(wide == v, a + 1.0, a) for v, a in zip(ids, sums)]
        for j, total in enumerate(sums):
            r_pack[start : start + chunk, j * tile : (j + 1) * tile] = total
            scaled = total * inverse[:, :tile]
            d_pack[start : start + chunk, j * tile : (j + 1) * tile] = scaled
            x_pack[start : start + chunk, j * tile : (j + 1) * tile] = scaled
            send_buf[0, j, start : start + chunk, :] = scaled

    pl.semaphore_wait(barrier, greeted)

    def send(step, group, j):
        rows_of = pl.ds(group * k_group, k_group)
        return pltpu.make_async_remote_copy(
            src_ref=send_buf.at[step, j, rows_of, :],
            dst_ref=recv_buf.at[step, lands[j], rows_of, :],
            send_sem=send_sem.at[step, group, j],
            recv_sem=recv_sem.at[step, group, lands[j]],
            device_id=targets[j],
            device_id_type=MESH,
        )

    def start_sends(step, group):
        for j in (2, 3, 0, 1):
            send(step, group, j).start()

    def wait_recvs(step, group):
        for j in (0, 1, 2, 3):
            send(step, group, j).wait_recv()

    def wait_sends(step):
        for group in range(groups):
            for j in range(dirs):
                send(step, group, j).wait_send()

    for group in range(groups):
        start_sends(0, group)

    def hello(distance):
        for offset in (distance, planes - distance):
            pl.semaphore_signal(
                hello_sems.at[distance - 1], inc=1, device_id=axis_target(offset), device_id_type=MESH
            )

    hello(1)

    half_width = (upper - lower) / 2.0
    ratio = centre / half_width
    damping = 1.0 / ratio
    for step in range(ITERS - 1):
        following = 1.0 / (2.0 * ratio - damping)
        coef[2 * step] = following * damping
        coef[2 * step + 1] = 2.0 * following / half_width
        damping = following

    for start in range(0, k_all, chunk):
        sums = [jnp.zeros((chunk, tile), f32) for _ in range(blk_rows)]
        for source in range(src.shape[1]):
            wide = jnp.broadcast_to(src[start : start + chunk, source : source + 1], (chunk, tile))
            sums = [jnp.where(wide == lane + i * tile, a + 1.0, a) for i, a in enumerate(sums)]
        for i, total in enumerate(sums):
            where = (slice(start, start + chunk), slice(i * tile, (i + 1) * tile))
            b_own[where] = total
            r_own[where] = total
            scaled = total * inverse[:, :tile]
            d_own[where] = scaled
            x_own[where] = scaled
            high, low = split(scaled)
            ext[start : start + chunk, i * tile : (i + 1) * tile] = high
            ext[k_all + start : k_all + start + chunk, i * tile : (i + 1) * tile] = low

    loads[3].wait()

    eye = lax.broadcasted_iota(jnp.int32, (tile, tile), 0) == lax.broadcasted_iota(jnp.int32, (tile, tile), 1)
    row_id = lax.broadcasted_iota(jnp.int32, (rows, tile), 0)
    for c in range(n_blocks):
        if c < blk_rows:
            place[c] = jnp.zeros(place.shape[1:], jnp.bfloat16)
            place[c, c * tile : (c + 1) * tile, :] = one_hot(eye)
        else:
            h = c - blk_rows
            place[c, 0:rows, :] = jnp.zeros((rows, tile), jnp.bfloat16)
            place[c, rows : 2 * rows, :] = one_hot(recv_rows[:, h * tile : (h + 1) * tile] == row_id)
    for j in range(dirs):
        pick[:, j * tile : (j + 1) * tile] = one_hot(send_rows[j : j + 1, :] == row_id)

    for load in loads[4:]:
        load.wait()

    for b in range(blk_rows):
        for n in range(per_row):
            high, low = split(tiles[b, n])
            tile_pair[0:tile, n * tile : (n + 1) * tile] = high
            tile_pair[tile : 2 * tile, n * tile : (n + 1) * tile] = low
        pair = tile_pair[...]
        for start in range(0, 2 * rows, CUT):
            spots = [place[cols[b, n], start : start + CUT, :] for n in range(per_row)]
            both = dot_nt(jnp.concatenate(spots, axis=1), pair)
            block = both[:, :tile] + both[:, tile:]
            offset = b * tile - start
            if 0 <= offset < CUT:
                extra = jnp.where(eye, diag[b : b + 1, :], 0.0)
                pieces = [jnp.zeros((tile, tile), f32)] * (CUT // tile)
                pieces[offset // tile] = extra
                block = block + jnp.concatenate(pieces, axis=0)
            high, low = split(block)
            w_high[start : start + CUT, b * tile : (b + 1) * tile] = high
            w_low[start : start + CUT, b * tile : (b + 1) * tile] = low

    for start in range(0, 2 * rows, CUT):
        for weights in (w_high, w_low):
            weights[start : start + CUT, rows : 2 * rows] = dot(
                weights[start : start + CUT, 0:rows], pick[...]
            ).astype(jnp.bfloat16)

    def product(k_rows, n_cols):
        both = dot(ext[:, k_rows], w_high[k_rows, n_cols])
        return both[:k_all] + both[k_all:] + dot(ext[0:k_all, k_rows], w_low[k_rows, n_cols])

    own, got = slice(0, rows), slice(rows, 2 * rows)

    def packed_part():
        for start in range(0, rows, CUT):
            part[:, start : start + CUT] = product(own, slice(rows + start, rows + start + CUT))

    packed_part()
    pl.semaphore_wait(hello_sems.at[0], 2)
    hello(2)

    def take_halo(step, group):
        at = pl.ds(group * k_group, k_group)
        wait_recvs(step, group)
        halo = jnp.concatenate([recv_buf[step, j, at, :] for j in range(dirs)], axis=1)
        return split(halo)

    def halo_product(high, low, n_cols):
        both = dot(jnp.concatenate([high, low], axis=0), w_high[got, n_cols])
        return both[:k_group] + both[k_group:] + dot(high, w_low[got, n_cols])

    def iteration(step, carry):
        alpha = coef[2 * step][0:1]
        beta = coef[2 * step + 1][0:1]
        last = (step == ITERS - 2).astype(f32)
        for group in range(groups):
            g0 = group * k_group
            at = slice(g0, g0 + k_group)
            high, low = take_halo(step, group)
            ext[at, got] = high
            ext[k_all + g0 : k_all + g0 + k_group, got] = low
            r_new = r_pack[at, :] - (part[at, :] + halo_product(high, low, slice(rows, 2 * rows)))
            d_new = alpha * d_pack[at, :] + beta * r_new
            x_old = x_pack[at, :]
            going = d_new + last * x_old
            for j in range(dirs):
                send_buf[step + 1, j, at, :] = going[:, j * tile : (j + 1) * tile]
            start_sends(step + 1, group)
            r_pack[at, :] = r_new
            d_pack[at, :] = d_new
            x_pack[at, :] = x_old + d_new
        wait_sends(step)
        for start in range(0, rows, CUT):
            at = slice(start, start + CUT)
            r_new = r_own[:, at] - product(slice(0, 2 * rows), at)
            d_new = alpha[:, at] * d_own[:, at] + beta[:, at] * r_new
            r_own[:, at] = r_new
            d_own[:, at] = d_new
        for start in range(0, rows, CUT):
            at = slice(start, start + CUT)
            d_new = d_own[:, at]
            x_old = x_own[:, at]
            x_own[:, at] = x_old + d_new
            high, low = split(d_new + last * x_old)
            ext[0:k_all, at] = high
            ext[k_all : 2 * k_all, at] = low
        packed_part()
        return carry

    lax.fori_loop(0, ITERS - 1, iteration, 0)

    for start in range(0, rows, CUT):
        at = slice(start, start + CUT)
        r_own[:, at] = b_own[:, at] - product(own, at)
    for i in range(blk_rows):
        out_buf[i * tile : (i + 1) * tile, :] = jnp.transpose(x_own[:, i * tile : (i + 1) * tile])

    out_copy = pltpu.make_async_copy(out_buf, x_out, out_sem)
    out_copy.start()
    pl.semaphore_wait(hello_sems.at[1], 2)

    squares = []
    for group in range(groups):
        high, low = take_halo(ITERS - 1, group)
        final = r_own[group * k_group : (group + 1) * k_group, :] - halo_product(high, low, own)
        final = final * final
        total = final[:, 0:tile]
        for i in range(1, blk_rows):
            total = total + final[:, i * tile : (i + 1) * tile]
        squares.append(total)
    squares = jnp.transpose(jnp.concatenate(squares, axis=0))
    mine = jnp.sum(squares, axis=0, keepdims=True)

    plane_send[...] = mine
    plane_recv[my_slot] = mine
    plane_copies = [
        pltpu.make_async_remote_copy(
            src_ref=plane_send,
            dst_ref=plane_recv.at[my_slot],
            send_sem=norm_sems.at[0],
            recv_sem=norm_sems.at[1],
            device_id=plane_target(offset),
            device_id_type=MESH,
        )
        for offset in range(1, in_plane)
    ]
    for copy in plane_copies:
        copy.start()
    others = plane_recv.at[pl.ds(0, in_plane - 1)]
    pltpu.make_async_copy(others, others, norm_sems.at[1]).wait()
    mine = jnp.sum(plane_recv[...], axis=0)

    axis_send[...] = mine
    axis_recv[my_plane] = mine
    axis_copies = [
        pltpu.make_async_remote_copy(
            src_ref=axis_send,
            dst_ref=axis_recv.at[my_plane],
            send_sem=norm_sems.at[2],
            recv_sem=norm_sems.at[3],
            device_id=axis_target(offset),
            device_id_type=MESH,
        )
        for offset in range(1, planes)
    ]
    for copy in axis_copies:
        copy.start()
    wait_sends(ITERS - 1)
    out_copy.wait()
    pltpu.make_async_copy(others, others, norm_sems.at[0]).wait()
    others = axis_recv.at[pl.ds(0, planes - 1)]
    pltpu.make_async_copy(others, others, norm_sems.at[3]).wait()
    norm_out[...] = jnp.sqrt(jnp.sum(axis_recv[...], axis=0))
    pltpu.make_async_copy(others, others, norm_sems.at[2]).wait()


def on_device(n_patch, n_sub, planes, sources, diag_coef, tiles, tile_cols, send_rows, recv_rows, bounds):
    rows = diag_coef.shape[0]
    k_all = sources.shape[0]
    blk_rows, per_row, tile, _ = tiles.shape
    dirs = send_rows.shape[1]
    n_blocks = 2 * blk_rows
    f32, bf16 = jnp.float32, jnp.bfloat16
    vmem = pl.BlockSpec(memory_space=pltpu.VMEM)
    hbm = pl.BlockSpec(memory_space=pltpu.HBM)
    field = pltpu.VMEM((k_all, rows), f32)
    in_plane = n_patch // planes * n_sub
    x, norm = pl.pallas_call(
        functools.partial(kernel, (n_patch, n_sub, planes)),
        out_shape=(jax.ShapeDtypeStruct((rows, k_all), f32), jax.ShapeDtypeStruct((1, k_all), f32)),
        in_specs=[hbm] * 7,
        out_specs=(hbm, vmem),
        scratch_shapes=[
            pltpu.VMEM(sources.shape[::-1], jnp.int32),
            pltpu.VMEM((blk_rows, tile), f32),
            pltpu.SMEM(tile_cols.shape, jnp.int32),
            pltpu.VMEM(send_rows.shape[1:], jnp.int32),
            pltpu.VMEM(recv_rows.shape, jnp.int32),
            pltpu.SMEM(bounds.shape, f32),
            pltpu.VMEM(tiles.shape, f32),
            pltpu.VMEM((n_blocks, 2 * rows, tile), bf16),
            pltpu.VMEM((rows, rows), bf16),
            pltpu.VMEM((2 * tile, per_row * tile), bf16),
            pltpu.VMEM((2 * rows, 2 * rows), bf16),
            pltpu.VMEM((2 * rows, 2 * rows), bf16),
            pltpu.VMEM((2 * k_all, 2 * rows), bf16),
            field,
            field,
            field,
            field,
            field,
            field,
            field,
            field,
            pltpu.VMEM((2 * ITERS, 8, rows), f32),
            pltpu.VMEM((ITERS, dirs, k_all, tile), f32),
            pltpu.VMEM((ITERS, dirs, k_all, tile), f32),
            pltpu.VMEM((1, k_all), f32),
            pltpu.VMEM((in_plane, 1, k_all), f32),
            pltpu.VMEM((1, k_all), f32),
            pltpu.VMEM((planes, 1, k_all), f32),
            pltpu.SemaphoreType.DMA((7,)),
            pltpu.SemaphoreType.DMA((ITERS, GROUPS, dirs)),
            pltpu.SemaphoreType.DMA((ITERS, GROUPS, dirs)),
            pltpu.SemaphoreType.DMA((4,)),
            pltpu.VMEM((rows, k_all), f32),
            pltpu.SemaphoreType.DMA,
            pltpu.SemaphoreType.REGULAR((2,)),
        ],
        compiler_params=pltpu.CompilerParams(
            collective_id=0, has_side_effects=True, vmem_limit_bytes=67_043_328
        ),
    )(
        sources.T,
        diag_coef.reshape(blk_rows, tile),
        tile_cols,
        send_rows[0],
        recv_rows,
        bounds,
        tiles,
    )
    return settle(x, norm)


def settle_kernel(x_in, norm_in, x_out, norm_out, x_buf, norm_buf, sems):
    steps = ((x_in, x_buf, x_out), (norm_in, norm_buf, norm_out))
    reads = [pltpu.make_async_copy(a, b, sems.at[i]) for i, (a, b, _) in enumerate(steps)]
    writes = [pltpu.make_async_copy(b, c, sems.at[2 + i]) for i, (_, b, c) in enumerate(steps)]
    for read in reads:
        read.start()
    for read, write in zip(reads, writes):
        read.wait()
        write.start()
    for write in writes:
        write.wait()


def settle(x, norm):
    hbm = pl.BlockSpec(memory_space=pl.ANY)
    arrays = (x, norm)
    x, norm = pl.pallas_call(
        settle_kernel,
        out_shape=tuple(jax.ShapeDtypeStruct(a.shape, a.dtype) for a in arrays),
        in_specs=[hbm] * 2,
        out_specs=(hbm, hbm),
        scratch_shapes=[pltpu.VMEM(a.shape, a.dtype) for a in arrays] + [pltpu.SemaphoreType.DMA((4,))],
        compiler_params=pltpu.CompilerParams(vmem_limit_bytes=67_043_328),
    )(x, norm)
    return x, norm[0]


def solution(mesh):
    n_patch, n_sub = mesh.shape["patch"], mesh.shape["sub"]
    both = ("patch", "sub")
    return jax.shard_map(
        functools.partial(on_device, n_patch, n_sub, PLANES),
        mesh=mesh,
        in_specs=(
            P(),
            P(both),
            P(both, None, None, None),
            P(both, None),
            P(both, None, None),
            P(both, None),
            P(),
        ),
        out_specs=(P(both, None), P()),
        check_vma=False,
    )
```

```python
import functools

import jax
import jax.numpy as jnp
from jax import lax
from jax.experimental import pallas as pl
from jax.experimental.pallas import tpu as pltpu
from jax.sharding import PartitionSpec as P

MESH = pl.DeviceIdType.MESH
ITERS = 8
GROUPS = 4
PLANES = 8
CUT = 256

NT = (((1,), (1,)), ((), ()))


def dot(a, b):
    return jnp.dot(a, b, preferred_element_type=jnp.float32)


def dot_nt(a, b):
    return lax.dot_general(a, b, NT, preferred_element_type=jnp.float32)


def split(value):
    high = value.astype(jnp.bfloat16)
    low = (value - high.astype(jnp.float32)).astype(jnp.bfloat16)
    return high, low


def one_hot(equal):
    return jnp.where(equal, 1.0, 0.0).astype(jnp.bfloat16)


def kernel(
    shape,
    src_hbm,
    diag_hbm,
    cols_hbm,
    send_hbm,
    recv_hbm,
    bounds_hbm,
    tiles_hbm,
    x_out,
    axis_recv,
    src_lanes,
    diag,
    cols,
    send_rows,
    recv_rows,
    bounds,
    tiles,
    place,
    pick,
    tile_pair,
    w_high,
    w_low,
    ext,
    b_own,
    r_own,
    d_own,
    x_own,
    r_pack,
    d_pack,
    x_pack,
    part,
    coef,
    send_buf,
    recv_buf,
    plane_send,
    plane_recv,
    axis_send,
    load_sems,
    send_sem,
    recv_sem,
    norm_sems,
    out_buf,
    out_sem,
    hello_sems,
):
    n_patch, n_sub, planes = shape
    f32 = jnp.float32
    k_all, rows = b_own.shape
    per_row = tiles.shape[1]
    blk_rows = tiles.shape[0]
    tile = tiles.shape[2]
    n_blocks = place.shape[0]
    halo_blocks = n_blocks - blk_rows
    dirs = 4
    groups = send_sem.shape[1]
    k_group = k_all // groups

    p = lax.axis_index("patch")
    s = lax.axis_index("sub")
    plane = n_patch // planes
    in_plane = plane * n_sub
    my_plane = lax.div(p, plane)
    my_patch = lax.rem(p, plane)
    my_slot = my_patch * n_sub + s

    p_next = lax.rem(p + 1, n_patch)
    p_prev = lax.rem(p + n_patch - 1, n_patch)
    s_next = lax.rem(s + 1, n_sub)
    s_prev = lax.rem(s + n_sub - 1, n_sub)
    targets = ((p_prev, s), (p_next, s), (p, s_prev), (p, s_next))
    lands = (1, 0, 3, 2)

    def plane_target(offset):
        slot = lax.rem(my_slot + offset, in_plane)
        return (my_plane * plane + lax.div(slot, n_sub), lax.rem(slot, n_sub))

    def axis_target(offset):
        return (lax.rem(my_plane + offset, planes) * plane + my_patch, s)

    loads = [
        pltpu.make_async_copy(source, target, load_sems.at[i])
        for i, (source, target) in enumerate(
            (
                (src_hbm, src_lanes),
                (send_hbm, send_rows),
                (bounds_hbm, bounds),
                (recv_hbm, recv_rows),
                (cols_hbm, cols),
                (diag_hbm, diag),
                (tiles_hbm, tiles),
            )
        )
    ]
    for load in loads:
        load.start()
    barrier = pltpu.get_barrier_semaphore()
    greeted = 0
    for target in targets:
        pl.semaphore_signal(barrier, inc=1, device_id=target, device_id_type=MESH)
        greeted += 1
    for offset in (1, planes - 1):
        pl.semaphore_signal(barrier, inc=1, device_id=axis_target(offset), device_id_type=MESH)
        greeted += 1

    for load in loads[:3]:
        load.wait()

    lower = jnp.full((8, rows), bounds[0], f32)
    upper = jnp.full((8, rows), bounds[1], f32)
    centre = (lower + upper) / 2.0
    inverse = (1.0 / centre)[0:1]

    first = (p * n_sub + s) * rows
    src = jnp.transpose(src_lanes[...])
    lane = lax.broadcasted_iota(jnp.int32, (1, tile), 1) + first
    chunk = 32
    for start in range(0, k_all, chunk):
        ids = [send_rows[j : j + 1, :] + first for j in range(dirs)]
        sums = [jnp.zeros((chunk, tile), f32) for _ in ids]
        for source in range(src.shape[1]):
            wide = jnp.broadcast_to(src[start : start + chunk, source : source + 1], (chunk, tile))
            sums = [jnp.where(wide == v, a + 1.0, a) for v, a in zip(ids, sums)]
        for j, total in enumerate(sums):
            r_pack[start : start + chunk, j * tile : (j + 1) * tile] = total
            scaled = total * inverse[:, :tile]
            d_pack[start : start + chunk, j * tile : (j + 1) * tile] = scaled
            x_pack[start : start + chunk, j * tile : (j + 1) * tile] = scaled
            send_buf[0, j, start : start + chunk, :] = scaled

    pl.semaphore_wait(barrier, greeted)

    def send(step, group, j):
        rows_of = pl.ds(group * k_group, k_group)
        return pltpu.make_async_remote_copy(
            src_ref=send_buf.at[step, j, rows_of, :],
            dst_ref=recv_buf.at[step, lands[j], rows_of, :],
            send_sem=send_sem.at[lax.rem(step, 2), group],
            recv_sem=recv_sem.at[lax.rem(step, 2), group],
            device_id=targets[j],
            device_id_type=MESH,
        )

    def start_sends(step, group):
        for j in (2, 3, 0, 1):
            send(step, group, j).start()

    def wait_all(buf, sems, step, group):
        parts = buf.at[step, :, pl.ds(group * k_group, k_group), :]
        pltpu.make_async_copy(parts, parts, sems.at[lax.rem(step, 2), group]).wait()

    def wait_recvs(step, group):
        wait_all(recv_buf, recv_sem, step, group)

    def wait_sends(step):
        for group in range(groups):
            wait_all(send_buf, send_sem, step, group)

    for group in range(groups):
        start_sends(0, group)

    def hello(distance):
        for offset in (distance, planes - distance):
            pl.semaphore_signal(
                hello_sems.at[distance - 1], inc=1, device_id=axis_target(offset), device_id_type=MESH
            )

    hello(1)

    half_width = (upper - lower) / 2.0
    ratio = centre / half_width
    damping = 1.0 / ratio
    for step in range(ITERS - 1):
        following = 1.0 / (2.0 * ratio - damping)
        coef[2 * step] = following * damping
        coef[2 * step + 1] = 2.0 * following / half_width
        damping = following

    for start in range(0, k_all, chunk):
        sums = [jnp.zeros((chunk, tile), f32) for _ in range(blk_rows)]
        for source in range(src.shape[1]):
            wide = jnp.broadcast_to(src[start : start + chunk, source : source + 1], (chunk, tile))
            sums = [jnp.where(wide == lane + i * tile, a + 1.0, a) for i, a in enumerate(sums)]
        for i, total in enumerate(sums):
            where = (slice(start, start + chunk), slice(i * tile, (i + 1) * tile))
            b_own[where] = total
            r_own[where] = total
            scaled = total * inverse[:, :tile]
            d_own[where] = scaled
            x_own[where] = scaled
            high, low = split(scaled)
            ext[start : start + chunk, i * tile : (i + 1) * tile] = high
            ext[k_all + start : k_all + start + chunk, i * tile : (i + 1) * tile] = low

    loads[3].wait()

    eye = lax.broadcasted_iota(jnp.int32, (tile, tile), 0) == lax.broadcasted_iota(jnp.int32, (tile, tile), 1)
    row_id = lax.broadcasted_iota(jnp.int32, (rows, tile), 0)
    for c in range(n_blocks):
        if c < blk_rows:
            place[c] = jnp.zeros(place.shape[1:], jnp.bfloat16)
            place[c, c * tile : (c + 1) * tile, :] = one_hot(eye)
        else:
            h = c - blk_rows
            place[c, 0:rows, :] = jnp.zeros((rows, tile), jnp.bfloat16)
            place[c, rows : 2 * rows, :] = one_hot(recv_rows[:, h * tile : (h + 1) * tile] == row_id)
    for j in range(dirs):
        pick[:, j * tile : (j + 1) * tile] = one_hot(send_rows[j : j + 1, :] == row_id)

    for load in loads[4:]:
        load.wait()

    for b in range(blk_rows):
        for n in range(per_row):
            high, low = split(tiles[b, n])
            tile_pair[0:tile, n * tile : (n + 1) * tile] = high
            tile_pair[tile : 2 * tile, n * tile : (n + 1) * tile] = low
        pair = tile_pair[...]
        for start in range(0, 2 * rows, CUT):
            spots = [place[cols[b, n], start : start + CUT, :] for n in range(per_row)]
            both = dot_nt(jnp.concatenate(spots, axis=1), pair)
            block = both[:, :tile] + both[:, tile:]
            offset = b * tile - start
            if 0 <= offset < CUT:
                extra = jnp.where(eye, diag[b : b + 1, :], 0.0)
                pieces = [jnp.zeros((tile, tile), f32)] * (CUT // tile)
                pieces[offset // tile] = extra
                block = block + jnp.concatenate(pieces, axis=0)
            high, low = split(block)
            w_high[start : start + CUT, b * tile : (b + 1) * tile] = high
            w_low[start : start + CUT, b * tile : (b + 1) * tile] = low

    for start in range(0, 2 * rows, CUT):
        for weights in (w_high, w_low):
            weights[start : start + CUT, rows : 2 * rows] = dot(
                weights[start : start + CUT, 0:rows], pick[...]
            ).astype(jnp.bfloat16)

    def product(k_rows, n_cols):
        both = dot(ext[:, k_rows], w_high[k_rows, n_cols])
        return both[:k_all] + both[k_all:] + dot(ext[0:k_all, k_rows], w_low[k_rows, n_cols])

    own, got = slice(0, rows), slice(rows, 2 * rows)

    def packed_part():
        for start in range(0, rows, CUT):
            part[:, start : start + CUT] = product(own, slice(rows + start, rows + start + CUT))

    packed_part()
    pl.semaphore_wait(hello_sems.at[0], 2)
    hello(2)

    def take_halo(step, group):
        at = pl.ds(group * k_group, k_group)
        wait_recvs(step, group)
        halo = jnp.concatenate([recv_buf[step, j, at, :] for j in range(dirs)], axis=1)
        return split(halo)

    def halo_product(high, low, n_cols):
        both = dot(jnp.concatenate([high, low], axis=0), w_high[got, n_cols])
        return both[:k_group] + both[k_group:] + dot(high, w_low[got, n_cols])

    def iteration(step, carry):
        alpha = coef[2 * step][0:1]
        beta = coef[2 * step + 1][0:1]
        last = (step == ITERS - 2).astype(f32)
        for group in range(groups):
            g0 = group * k_group
            at = slice(g0, g0 + k_group)
            high, low = take_halo(step, group)
            ext[at, got] = high
            ext[k_all + g0 : k_all + g0 + k_group, got] = low
            r_new = r_pack[at, :] - (part[at, :] + halo_product(high, low, slice(rows, 2 * rows)))
            d_new = alpha * d_pack[at, :] + beta * r_new
            x_old = x_pack[at, :]
            going = d_new + last * x_old
            for j in range(dirs):
                send_buf[step + 1, j, at, :] = going[:, j * tile : (j + 1) * tile]
            start_sends(step + 1, group)
            r_pack[at, :] = r_new
            d_pack[at, :] = d_new
            x_pack[at, :] = x_old + d_new
        wait_sends(step)
        for start in range(0, rows, CUT):
            at = slice(start, start + CUT)
            r_new = r_own[:, at] - product(slice(0, 2 * rows), at)
            d_new = alpha[:, at] * d_own[:, at] + beta[:, at] * r_new
            r_own[:, at] = r_new
            d_own[:, at] = d_new
        for start in range(0, rows, CUT):
            at = slice(start, start + CUT)
            d_new = d_own[:, at]
            x_old = x_own[:, at]
            x_own[:, at] = x_old + d_new
            high, low = split(d_new + last * x_old)
            ext[0:k_all, at] = high
            ext[k_all : 2 * k_all, at] = low
        packed_part()
        return carry

    lax.fori_loop(0, ITERS - 1, iteration, 0)

    for start in range(0, rows, CUT):
        at = slice(start, start + CUT)
        r_own[:, at] = b_own[:, at] - product(own, at)
    for i in range(blk_rows):
        out_buf[i * tile : (i + 1) * tile, :] = jnp.transpose(x_own[:, i * tile : (i + 1) * tile])

    out_copy = pltpu.make_async_copy(out_buf, x_out, out_sem)
    out_copy.start()
    pl.semaphore_wait(hello_sems.at[1], 2)

    squares = []
    for group in range(groups):
        high, low = take_halo(ITERS - 1, group)
        final = r_own[group * k_group : (group + 1) * k_group, :] - halo_product(high, low, own)
        final = final * final
        total = final[:, 0:tile]
        for i in range(1, blk_rows):
            total = total + final[:, i * tile : (i + 1) * tile]
        squares.append(total)
    squares = jnp.transpose(jnp.concatenate(squares, axis=0))
    mine = jnp.sum(squares, axis=0, keepdims=True)

    plane_send[...] = mine
    plane_recv[my_slot] = mine
    plane_copies = [
        pltpu.make_async_remote_copy(
            src_ref=plane_send,
            dst_ref=plane_recv.at[my_slot],
            send_sem=norm_sems.at[0],
            recv_sem=norm_sems.at[1],
            device_id=plane_target(offset),
            device_id_type=MESH,
        )
        for offset in range(1, in_plane)
    ]
    for copy in plane_copies:
        copy.start()
    others = plane_recv.at[pl.ds(0, in_plane - 1)]
    pltpu.make_async_copy(others, others, norm_sems.at[1]).wait()
    mine = jnp.sum(plane_recv[...], axis=0)

    axis_send[...] = mine
    own_copy = pltpu.make_async_copy(axis_send, axis_recv.at[my_plane], norm_sems.at[4])
    own_copy.start()
    axis_copies = [
        pltpu.make_async_remote_copy(
            src_ref=axis_send,
            dst_ref=axis_recv.at[my_plane],
            send_sem=norm_sems.at[2],
            recv_sem=norm_sems.at[3],
            device_id=axis_target(offset),
            device_id_type=MESH,
        )
        for offset in range(1, planes)
    ]
    for copy in axis_copies:
        copy.start()
    wait_sends(ITERS - 1)
    out_copy.wait()
    pltpu.make_async_copy(others, others, norm_sems.at[0]).wait()
    others = axis_recv.at[pl.ds(0, planes - 1)]
    pltpu.make_async_copy(others, others, norm_sems.at[3]).wait()
    own_copy.wait()
    pltpu.make_async_copy(others, others, norm_sems.at[2]).wait()


def on_device(n_patch, n_sub, planes, sources, diag_coef, tiles, tile_cols, send_rows, recv_rows, bounds):
    rows = diag_coef.shape[0]
    k_all = sources.shape[0]
    blk_rows, per_row, tile, _ = tiles.shape
    dirs = send_rows.shape[1]
    n_blocks = 2 * blk_rows
    f32, bf16 = jnp.float32, jnp.bfloat16
    hbm = pl.BlockSpec(memory_space=pltpu.HBM)
    field = pltpu.VMEM((k_all, rows), f32)
    in_plane = n_patch // planes * n_sub
    x, sums = pl.pallas_call(
        functools.partial(kernel, (n_patch, n_sub, planes)),
        out_shape=(jax.ShapeDtypeStruct((rows, k_all), f32), jax.ShapeDtypeStruct((planes, 1, k_all), f32)),
        in_specs=[hbm] * 7,
        out_specs=(hbm, hbm),
        scratch_shapes=[
            pltpu.VMEM(sources.shape[::-1], jnp.int32),
            pltpu.VMEM((blk_rows, tile), f32),
            pltpu.SMEM(tile_cols.shape, jnp.int32),
            pltpu.VMEM(send_rows.shape[1:], jnp.int32),
            pltpu.VMEM(recv_rows.shape, jnp.int32),
            pltpu.SMEM(bounds.shape, f32),
            pltpu.VMEM(tiles.shape, f32),
            pltpu.VMEM((n_blocks, 2 * rows, tile), bf16),
            pltpu.VMEM((rows, rows), bf16),
            pltpu.VMEM((2 * tile, per_row * tile), bf16),
            pltpu.VMEM((2 * rows, 2 * rows), bf16),
            pltpu.VMEM((2 * rows, 2 * rows), bf16),
            pltpu.VMEM((2 * k_all, 2 * rows), bf16),
            field,
            field,
            field,
            field,
            field,
            field,
            field,
            field,
            pltpu.VMEM((2 * ITERS, 8, rows), f32),
            pltpu.VMEM((ITERS, dirs, k_all, tile), f32),
            pltpu.VMEM((ITERS, dirs, k_all, tile), f32),
            pltpu.VMEM((1, k_all), f32),
            pltpu.VMEM((in_plane, 1, k_all), f32),
            pltpu.VMEM((1, k_all), f32),
            pltpu.SemaphoreType.DMA((7,)),
            pltpu.SemaphoreType.DMA((2, GROUPS)),
            pltpu.SemaphoreType.DMA((2, GROUPS)),
            pltpu.SemaphoreType.DMA((5,)),
            pltpu.VMEM((rows, k_all), f32),
            pltpu.SemaphoreType.DMA,
            pltpu.SemaphoreType.REGULAR((2,)),
        ],
        compiler_params=pltpu.CompilerParams(
            collective_id=0, has_side_effects=True, vmem_limit_bytes=67_043_328
        ),
    )(
        sources.T,
        diag_coef.reshape(blk_rows, tile),
        tile_cols,
        send_rows[0],
        recv_rows,
        bounds,
        tiles,
    )
    return settle(x, sums)


def settle_kernel(x_in, sums_in, x_out, norm_out, x_buf, sums_buf, norm_buf, sems):
    read_sums = pltpu.make_async_copy(sums_in, sums_buf, sems.at[0])
    read_x = pltpu.make_async_copy(x_in, x_buf, sems.at[1])
    write_norm = pltpu.make_async_copy(norm_buf, norm_out, sems.at[0])
    write_x = pltpu.make_async_copy(x_buf, x_out, sems.at[1])
    read_sums.start()
    read_x.start()
    read_sums.wait()
    norm_buf[...] = jnp.sqrt(jnp.sum(sums_buf[...], axis=0))
    write_norm.start()
    read_x.wait()
    write_x.start()
    write_norm.wait()
    write_x.wait()


def settle(x, sums):
    hbm = pl.BlockSpec(memory_space=pl.ANY)
    norm_shape = jax.ShapeDtypeStruct(sums.shape[1:], sums.dtype)
    x, norm = pl.pallas_call(
        settle_kernel,
        out_shape=(jax.ShapeDtypeStruct(x.shape, x.dtype), norm_shape),
        in_specs=[hbm] * 2,
        out_specs=(hbm, hbm),
        scratch_shapes=[
            pltpu.VMEM(x.shape, x.dtype),
            pltpu.VMEM(sums.shape, sums.dtype),
            pltpu.VMEM(norm_shape.shape, norm_shape.dtype),
            pltpu.SemaphoreType.DMA((2,)),
        ],
        compiler_params=pltpu.CompilerParams(vmem_limit_bytes=67_043_328),
    )(x, sums)
    return x, norm[0]


def solution(mesh):
    n_patch, n_sub = mesh.shape["patch"], mesh.shape["sub"]
    both = ("patch", "sub")
    return jax.shard_map(
        functools.partial(on_device, n_patch, n_sub, PLANES),
        mesh=mesh,
        in_specs=(
            P(),
            P(both),
            P(both, None, None, None),
            P(both, None),
            P(both, None, None),
            P(both, None),
            P(),
        ),
        out_specs=(P(both, None), P()),
        check_vma=False,
    )
```

```python
import functools

import jax
import jax.numpy as jnp
from jax import lax
from jax.experimental import pallas as pl
from jax.experimental.pallas import tpu as pltpu
from jax.sharding import PartitionSpec as P

MESH = pl.DeviceIdType.MESH
ITERS = 8
GROUPS = 4
PLANES = 8
CUT = 256
BUILD_CUT = 256
SELECT_CUT = 256

NT = (((1,), (1,)), ((), ()))


def dot(a, b):
    return jnp.dot(a, b, preferred_element_type=jnp.float32)


def dot_nt(a, b):
    return lax.dot_general(a, b, NT, preferred_element_type=jnp.float32)


def split(value):
    high = value.astype(jnp.bfloat16)
    low = (value - high.astype(jnp.float32)).astype(jnp.bfloat16)
    return high, low


def one_hot(equal):
    return jnp.where(equal, 1.0, 0.0).astype(jnp.bfloat16)


def kernel(
    shape,
    src_hbm,
    diag_hbm,
    cols_hbm,
    send_hbm,
    recv_hbm,
    bounds_hbm,
    tiles_hbm,
    x_out,
    axis_recv,
    src_lanes,
    diag,
    cols,
    send_rows,
    recv_rows,
    bounds,
    tiles,
    place,
    pick,
    tile_pair,
    w_high,
    w_low,
    ext,
    b_own,
    r_own,
    d_own,
    x_own,
    r_pack,
    d_pack,
    x_pack,
    part,
    coef,
    send_buf,
    recv_buf,
    plane_send,
    plane_recv,
    axis_send,
    load_sems,
    send_sem,
    recv_sem,
    norm_sems,
    out_buf,
    out_sem,
    hello_sems,
):
    n_patch, n_sub, planes = shape
    f32 = jnp.float32
    k_all, rows = b_own.shape
    per_row = tiles.shape[1]
    blk_rows = tiles.shape[0]
    tile = tiles.shape[2]
    n_blocks = place.shape[0]
    halo_blocks = n_blocks - blk_rows
    dirs = 4
    groups = send_sem.shape[1]
    k_group = k_all // groups

    p = lax.axis_index("patch")
    s = lax.axis_index("sub")
    plane = n_patch // planes
    in_plane = plane * n_sub
    my_plane = lax.div(p, plane)
    my_patch = lax.rem(p, plane)
    my_slot = my_patch * n_sub + s

    p_next = lax.rem(p + 1, n_patch)
    p_prev = lax.rem(p + n_patch - 1, n_patch)
    s_next = lax.rem(s + 1, n_sub)
    s_prev = lax.rem(s + n_sub - 1, n_sub)
    targets = ((p_prev, s), (p_next, s), (p, s_prev), (p, s_next))
    lands = (1, 0, 3, 2)

    def plane_target(offset):
        slot = lax.rem(my_slot + offset, in_plane)
        return (my_plane * plane + lax.div(slot, n_sub), lax.rem(slot, n_sub))

    def axis_target(offset):
        return (lax.rem(my_plane + offset, planes) * plane + my_patch, s)

    loads = [
        pltpu.make_async_copy(source, target, load_sems.at[i])
        for i, (source, target) in enumerate(
            (
                (src_hbm, src_lanes),
                (send_hbm, send_rows),
                (bounds_hbm, bounds),
                (recv_hbm, recv_rows),
                (cols_hbm, cols),
                (diag_hbm, diag),
                (tiles_hbm, tiles),
            )
        )
    ]
    for load in loads:
        load.start()
    barrier = pltpu.get_barrier_semaphore()
    greeted = 0
    for target in targets:
        pl.semaphore_signal(barrier, inc=1, device_id=target, device_id_type=MESH)
        greeted += 1
    for offset in (1, planes - 1):
        pl.semaphore_signal(barrier, inc=1, device_id=axis_target(offset), device_id_type=MESH)
        greeted += 1

    eye = lax.broadcasted_iota(jnp.int32, (tile, tile), 0) == lax.broadcasted_iota(jnp.int32, (tile, tile), 1)
    row_id = lax.broadcasted_iota(jnp.int32, (rows, tile), 0)
    for c in range(n_blocks):
        if c < blk_rows:
            place[c] = jnp.zeros(place.shape[1:], jnp.bfloat16)
            place[c, c * tile : (c + 1) * tile, :] = one_hot(eye)
        else:
            place[c, 0:rows, :] = jnp.zeros((rows, tile), jnp.bfloat16)

    for load in loads[:3]:
        load.wait()

    lower = jnp.full((8, rows), bounds[0], f32)
    upper = jnp.full((8, rows), bounds[1], f32)
    centre = (lower + upper) / 2.0
    inverse = (1.0 / centre)[0:1]

    first = (p * n_sub + s) * rows
    src = jnp.transpose(src_lanes[...])
    lane = lax.broadcasted_iota(jnp.int32, (1, tile), 1) + first

    def count(start, size, ids):
        sums = [jnp.zeros((size, tile), f32) for _ in ids]
        for source in range(src.shape[1]):
            wide = jnp.broadcast_to(src[start : start + size, source : source + 1], (size, tile))
            sums = [jnp.where(wide == v, a + 1.0, a) for v, a in zip(ids, sums)]
        return sums

    def send(step, group, j):
        rows_of = pl.ds(group * k_group, k_group)
        return pltpu.make_async_remote_copy(
            src_ref=send_buf.at[step, j, rows_of, :],
            dst_ref=recv_buf.at[step, lands[j], rows_of, :],
            send_sem=send_sem.at[lax.rem(step, 2), group],
            recv_sem=recv_sem.at[lax.rem(step, 2), group],
            device_id=targets[j],
            device_id_type=MESH,
        )

    def start_sends(step, group, which=(0, 1, 2, 3)):
        for j in which:
            send(step, group, j).start()

    def wait_all(buf, sems, step, group):
        parts = buf.at[step, :, pl.ds(group * k_group, k_group), :]
        pltpu.make_async_copy(parts, parts, sems.at[lax.rem(step, 2), group]).wait()

    def wait_recvs(step, group):
        wait_all(recv_buf, recv_sem, step, group)

    def wait_sends(step):
        for group in range(groups):
            wait_all(send_buf, send_sem, step, group)

    for group in range(groups):
        at = slice(group * k_group, (group + 1) * k_group)
        ids = [send_rows[j : j + 1, :] + first for j in range(dirs)]
        for j, total in enumerate(count(group * k_group, k_group, ids)):
            scaled = total * inverse[:, :tile]
            send_buf[0, j, at, :] = scaled
            r_pack[at, j * tile : (j + 1) * tile] = total
            d_pack[at, j * tile : (j + 1) * tile] = scaled
            x_pack[at, j * tile : (j + 1) * tile] = scaled

    loads[3].wait()
    for c in range(blk_rows, n_blocks):
        h = c - blk_rows
        place[c, rows : 2 * rows, :] = one_hot(recv_rows[:, h * tile : (h + 1) * tile] == row_id)
    for j in range(dirs):
        pick[:, j * tile : (j + 1) * tile] = one_hot(send_rows[j : j + 1, :] == row_id)

    for load in loads[4:]:
        load.wait()

    def build_rows(b):
        for n in range(per_row):
            high, low = split(tiles[b, n])
            tile_pair[0:tile, n * tile : (n + 1) * tile] = high
            tile_pair[tile : 2 * tile, n * tile : (n + 1) * tile] = low
        pair = tile_pair[...]
        for start in range(0, 2 * rows, BUILD_CUT):
            spots = [place[cols[b, n], start : start + BUILD_CUT, :] for n in range(per_row)]
            both = dot_nt(jnp.concatenate(spots, axis=1), pair)
            block = both[:, :tile] + both[:, tile:]
            offset = b * tile - start
            if 0 <= offset < BUILD_CUT:
                extra = jnp.where(eye, diag[b : b + 1, :], 0.0)
                pieces = [jnp.zeros((tile, tile), f32)] * (BUILD_CUT // tile)
                pieces[offset // tile] = extra
                block = block + jnp.concatenate(pieces, axis=0)
            high, low = split(block)
            w_high[start : start + BUILD_CUT, b * tile : (b + 1) * tile] = high
            w_low[start : start + BUILD_CUT, b * tile : (b + 1) * tile] = low

        share = k_all // blk_rows
        at = slice(b * share, (b + 1) * share)
        low_at = slice(k_all + b * share, k_all + (b + 1) * share)
        for i, total in enumerate(count(b * share, share, [lane + i * tile for i in range(blk_rows)])):
            cols_at = slice(i * tile, (i + 1) * tile)
            b_own[at, cols_at] = total
            r_own[at, cols_at] = total
            scaled = total * inverse[:, :tile]
            d_own[at, cols_at] = scaled
            x_own[at, cols_at] = scaled
            high, low = split(scaled)
            ext[at, cols_at] = high
            ext[low_at, cols_at] = low

    build_rows(0)

    pl.semaphore_wait(barrier, greeted)
    for group in range(groups):
        start_sends(0, group)

    def hello(distance):
        for offset in (distance, planes - distance):
            pl.semaphore_signal(
                hello_sems.at[distance - 1], inc=1, device_id=axis_target(offset), device_id_type=MESH
            )

    hello(1)

    for b in range(1, blk_rows):
        build_rows(b)

    half_width = (upper - lower) / 2.0
    ratio = centre / half_width
    damping = 1.0 / ratio
    for step in range(ITERS - 1):
        following = 1.0 / (2.0 * ratio - damping)
        coef[2 * step] = following * damping
        coef[2 * step + 1] = 2.0 * following / half_width
        damping = following

    for start in range(0, 2 * rows, SELECT_CUT):
        for weights in (w_high, w_low):
            weights[start : start + SELECT_CUT, rows : 2 * rows] = dot(
                weights[start : start + SELECT_CUT, 0:rows], pick[...]
            ).astype(jnp.bfloat16)

    def product(k_rows, n_cols):
        both = dot(ext[:, k_rows], w_high[k_rows, n_cols])
        return both[:k_all] + both[k_all:] + dot(ext[0:k_all, k_rows], w_low[k_rows, n_cols])

    own, got = slice(0, rows), slice(rows, 2 * rows)

    def packed_part():
        for start in range(0, rows, CUT):
            part[:, start : start + CUT] = product(own, slice(rows + start, rows + start + CUT))

    packed_part()
    pl.semaphore_wait(hello_sems.at[0], 2)
    hello(2)

    def take_halo(step, group):
        at = pl.ds(group * k_group, k_group)
        wait_recvs(step, group)
        halo = jnp.concatenate([recv_buf[step, j, at, :] for j in range(dirs)], axis=1)
        return split(halo)

    def halo_product(high, low, n_cols):
        both = dot(jnp.concatenate([high, low], axis=0), w_high[got, n_cols])
        return both[:k_group] + both[k_group:] + dot(high, w_low[got, n_cols])

    def iteration(step, carry):
        alpha = coef[2 * step][0:1]
        beta = coef[2 * step + 1][0:1]
        last = (step == ITERS - 2).astype(f32)
        for group in range(groups):
            g0 = group * k_group
            at = slice(g0, g0 + k_group)
            high, low = take_halo(step, group)
            ext[at, got] = high
            ext[k_all + g0 : k_all + g0 + k_group, got] = low
            coupled = halo_product(high, low, slice(rows, 2 * rows))
            for which in ((0, 1), (2, 3)):
                half = slice(which[0] * tile, (which[-1] + 1) * tile)
                r_new = r_pack[at, half] - (part[at, half] + coupled[:, half])
                d_new = alpha[:, half] * d_pack[at, half] + beta[:, half] * r_new
                x_old = x_pack[at, half]
                going = d_new + last * x_old
                for i, j in enumerate(which):
                    send_buf[step + 1, j, at, :] = going[:, i * tile : (i + 1) * tile]
                start_sends(step + 1, group, which)
                r_pack[at, half] = r_new
                d_pack[at, half] = d_new
                x_pack[at, half] = x_old + d_new
        wait_sends(step)
        for start in range(0, rows, CUT):
            at = slice(start, start + CUT)
            r_new = r_own[:, at] - product(slice(0, 2 * rows), at)
            d_new = alpha[:, at] * d_own[:, at] + beta[:, at] * r_new
            r_own[:, at] = r_new
            d_own[:, at] = d_new
        for start in range(0, rows, CUT):
            at = slice(start, start + CUT)
            d_new = d_own[:, at]
            x_old = x_own[:, at]
            x_own[:, at] = x_old + d_new
            high, low = split(d_new + last * x_old)
            ext[0:k_all, at] = high
            ext[k_all : 2 * k_all, at] = low
        packed_part()
        return carry

    lax.fori_loop(0, ITERS - 1, iteration, 0)

    for start in range(0, rows, CUT):
        at = slice(start, start + CUT)
        r_own[:, at] = b_own[:, at] - product(own, at)
    for i in range(blk_rows):
        out_buf[i * tile : (i + 1) * tile, :] = jnp.transpose(x_own[:, i * tile : (i + 1) * tile])

    out_copy = pltpu.make_async_copy(out_buf, x_out, out_sem)
    out_copy.start()
    pl.semaphore_wait(hello_sems.at[1], 2)

    squares = []
    for group in range(groups):
        high, low = take_halo(ITERS - 1, group)
        final = r_own[group * k_group : (group + 1) * k_group, :] - halo_product(high, low, own)
        final = final * final
        total = final[:, 0:tile]
        for i in range(1, blk_rows):
            total = total + final[:, i * tile : (i + 1) * tile]
        squares.append(total)
    squares = jnp.transpose(jnp.concatenate(squares, axis=0))
    mine = jnp.sum(squares, axis=0, keepdims=True)

    plane_send[...] = mine
    plane_recv[my_slot] = mine
    plane_copies = [
        pltpu.make_async_remote_copy(
            src_ref=plane_send,
            dst_ref=plane_recv.at[my_slot],
            send_sem=norm_sems.at[0],
            recv_sem=norm_sems.at[1],
            device_id=plane_target(offset),
            device_id_type=MESH,
        )
        for offset in range(1, in_plane)
    ]
    for copy in plane_copies:
        copy.start()
    others = plane_recv.at[pl.ds(0, in_plane - 1)]
    pltpu.make_async_copy(others, others, norm_sems.at[1]).wait()
    mine = jnp.sum(plane_recv[...], axis=0)

    axis_send[...] = mine
    own_copy = pltpu.make_async_copy(axis_send, axis_recv.at[my_plane], norm_sems.at[4])
    own_copy.start()
    axis_copies = [
        pltpu.make_async_remote_copy(
            src_ref=axis_send,
            dst_ref=axis_recv.at[my_plane],
            send_sem=norm_sems.at[2],
            recv_sem=norm_sems.at[3],
            device_id=axis_target(offset),
            device_id_type=MESH,
        )
        for offset in range(1, planes)
    ]
    for copy in axis_copies:
        copy.start()
    wait_sends(ITERS - 1)
    out_copy.wait()
    pltpu.make_async_copy(others, others, norm_sems.at[0]).wait()
    others = axis_recv.at[pl.ds(0, planes - 1)]
    pltpu.make_async_copy(others, others, norm_sems.at[3]).wait()
    own_copy.wait()
    pltpu.make_async_copy(others, others, norm_sems.at[2]).wait()


def on_device(n_patch, n_sub, planes, sources, diag_coef, tiles, tile_cols, send_rows, recv_rows, bounds):
    rows = diag_coef.shape[0]
    k_all = sources.shape[0]
    blk_rows, per_row, tile, _ = tiles.shape
    dirs = send_rows.shape[1]
    n_blocks = 2 * blk_rows
    f32, bf16 = jnp.float32, jnp.bfloat16
    hbm = pl.BlockSpec(memory_space=pltpu.HBM)
    field = pltpu.VMEM((k_all, rows), f32)
    in_plane = n_patch // planes * n_sub
    x, sums = pl.pallas_call(
        functools.partial(kernel, (n_patch, n_sub, planes)),
        out_shape=(jax.ShapeDtypeStruct((rows, k_all), f32), jax.ShapeDtypeStruct((planes, 1, k_all), f32)),
        in_specs=[hbm] * 7,
        out_specs=(hbm, hbm),
        scratch_shapes=[
            pltpu.VMEM(sources.shape[::-1], jnp.int32),
            pltpu.VMEM((blk_rows, tile), f32),
            pltpu.SMEM(tile_cols.shape, jnp.int32),
            pltpu.VMEM(send_rows.shape[1:], jnp.int32),
            pltpu.VMEM(recv_rows.shape, jnp.int32),
            pltpu.SMEM(bounds.shape, f32),
            pltpu.VMEM(tiles.shape, f32),
            pltpu.VMEM((n_blocks, 2 * rows, tile), bf16),
            pltpu.VMEM((rows, rows), bf16),
            pltpu.VMEM((2 * tile, per_row * tile), bf16),
            pltpu.VMEM((2 * rows, 2 * rows), bf16),
            pltpu.VMEM((2 * rows, 2 * rows), bf16),
            pltpu.VMEM((2 * k_all, 2 * rows), bf16),
            field,
            field,
            field,
            field,
            field,
            field,
            field,
            field,
            pltpu.VMEM((2 * ITERS, 8, rows), f32),
            pltpu.VMEM((ITERS, dirs, k_all, tile), f32),
            pltpu.VMEM((ITERS, dirs, k_all, tile), f32),
            pltpu.VMEM((1, k_all), f32),
            pltpu.VMEM((in_plane, 1, k_all), f32),
            pltpu.VMEM((1, k_all), f32),
            pltpu.SemaphoreType.DMA((7,)),
            pltpu.SemaphoreType.DMA((2, GROUPS)),
            pltpu.SemaphoreType.DMA((2, GROUPS)),
            pltpu.SemaphoreType.DMA((5,)),
            pltpu.VMEM((rows, k_all), f32),
            pltpu.SemaphoreType.DMA,
            pltpu.SemaphoreType.REGULAR((2,)),
        ],
        compiler_params=pltpu.CompilerParams(
            collective_id=0, has_side_effects=True, vmem_limit_bytes=67_043_328
        ),
    )(
        sources.T,
        diag_coef.reshape(blk_rows, tile),
        tile_cols,
        send_rows[0],
        recv_rows,
        bounds,
        tiles,
    )
    return settle(x, sums)


def settle_kernel(x_in, sums_in, x_out, norm_out, x_buf, sums_buf, norm_buf, sems):
    read_sums = pltpu.make_async_copy(sums_in, sums_buf, sems.at[0])
    read_x = pltpu.make_async_copy(x_in, x_buf, sems.at[1])
    write_norm = pltpu.make_async_copy(norm_buf, norm_out, sems.at[0])
    write_x = pltpu.make_async_copy(x_buf, x_out, sems.at[1])
    read_sums.start()
    read_x.start()
    read_sums.wait()
    norm_buf[...] = jnp.sqrt(jnp.sum(sums_buf[...], axis=0))
    write_norm.start()
    read_x.wait()
    write_x.start()
    write_norm.wait()
    write_x.wait()


def settle(x, sums):
    hbm = pl.BlockSpec(memory_space=pl.ANY)
    norm_shape = jax.ShapeDtypeStruct(sums.shape[1:], sums.dtype)
    x, norm = pl.pallas_call(
        settle_kernel,
        out_shape=(jax.ShapeDtypeStruct(x.shape, x.dtype), norm_shape),
        in_specs=[hbm] * 2,
        out_specs=(hbm, hbm),
        scratch_shapes=[
            pltpu.VMEM(x.shape, x.dtype),
            pltpu.VMEM(sums.shape, sums.dtype),
            pltpu.VMEM(norm_shape.shape, norm_shape.dtype),
            pltpu.SemaphoreType.DMA((2,)),
        ],
        compiler_params=pltpu.CompilerParams(vmem_limit_bytes=67_043_328),
    )(x, sums)
    return x, norm[0]


def solution(mesh):
    n_patch, n_sub = mesh.shape["patch"], mesh.shape["sub"]
    both = ("patch", "sub")
    return jax.shard_map(
        functools.partial(on_device, n_patch, n_sub, PLANES),
        mesh=mesh,
        in_specs=(
            P(),
            P(both),
            P(both, None, None, None),
            P(both, None),
            P(both, None, None),
            P(both, None),
            P(),
        ),
        out_specs=(P(both, None), P()),
        check_vma=False,
    )
```

```python
import functools

import jax
import jax.numpy as jnp
from jax import lax
from jax.experimental import pallas as pl
from jax.experimental.pallas import tpu as pltpu
from jax.sharding import PartitionSpec as P

MESH = pl.DeviceIdType.MESH
ITERS = 8
GROUPS = 4
PLANES = 8
CUT = 256

def split(value):
    high = value.astype(jnp.bfloat16)
    low = (value - high.astype(jnp.float32)).astype(jnp.bfloat16)
    return high, low


def one_hot(equal):
    return jnp.where(equal, 1.0, 0.0).astype(jnp.bfloat16)


def steps(
    accs,
    shape,
    src_hbm,
    diag_hbm,
    cols_hbm,
    send_hbm,
    recv_hbm,
    bounds_hbm,
    tiles_hbm,
    x_out,
    axis_recv,
    src_lanes,
    diag,
    cols,
    send_rows,
    recv_rows,
    bounds,
    tiles,
    place,
    pick,
    tile_pair,
    w_high,
    w_low,
    ext,
    b_own,
    r_own,
    d_own,
    x_own,
    r_pack,
    d_pack,
    x_pack,
    part,
    coef,
    send_buf,
    recv_buf,
    plane_send,
    plane_recv,
    axis_send,
    load_sems,
    send_sem,
    recv_sem,
    norm_sems,
    out_buf,
    out_sem,
    hello_sems,
):
    n_patch, n_sub, planes = shape
    units = range(len(accs))
    build_accs = [unit_accs[0:2] for unit_accs in accs]
    field_accs = [unit_accs[2:4] for unit_accs in accs]
    halo_accs = [unit_accs[4:6] for unit_accs in accs]

    def feed(unit, weights, jobs, transpose=False):
        pltpu.matmul_push_rhs(weights, staging_register=0, mxu_index=unit, transpose=transpose)
        for i, (acc, operand) in enumerate(jobs):
            pltpu.matmul_acc_lhs(acc, operand, load_staged_rhs=0 if i == 0 else None)

    f32 = jnp.float32
    k_all, rows = b_own.shape
    per_row = tiles.shape[1]
    blk_rows = tiles.shape[0]
    tile = tiles.shape[2]
    n_blocks = place.shape[0]
    halo_blocks = n_blocks - blk_rows
    dirs = 4
    groups = send_sem.shape[1]
    k_group = k_all // groups

    p = lax.axis_index("patch")
    s = lax.axis_index("sub")
    plane = n_patch // planes
    in_plane = plane * n_sub
    my_plane = lax.div(p, plane)
    my_patch = lax.rem(p, plane)
    my_slot = my_patch * n_sub + s

    p_next = lax.rem(p + 1, n_patch)
    p_prev = lax.rem(p + n_patch - 1, n_patch)
    s_next = lax.rem(s + 1, n_sub)
    s_prev = lax.rem(s + n_sub - 1, n_sub)
    targets = ((p_prev, s), (p_next, s), (p, s_prev), (p, s_next))
    lands = (1, 0, 3, 2)

    def plane_target(offset):
        slot = lax.rem(my_slot + offset, in_plane)
        return (my_plane * plane + lax.div(slot, n_sub), lax.rem(slot, n_sub))

    def axis_target(offset):
        return (lax.rem(my_plane + offset, planes) * plane + my_patch, s)

    loads = [
        pltpu.make_async_copy(source, target, load_sems.at[i])
        for i, (source, target) in enumerate(
            (
                (src_hbm, src_lanes),
                (send_hbm, send_rows),
                (bounds_hbm, bounds),
                (recv_hbm, recv_rows),
                (cols_hbm, cols),
                (diag_hbm, diag),
                (tiles_hbm, tiles),
            )
        )
    ]
    for load in loads:
        load.start()
    barrier = pltpu.get_barrier_semaphore()
    greeted = 0
    for target in targets:
        pl.semaphore_signal(barrier, inc=1, device_id=target, device_id_type=MESH)
        greeted += 1
    for offset in (1, planes - 1):
        pl.semaphore_signal(barrier, inc=1, device_id=axis_target(offset), device_id_type=MESH)
        greeted += 1

    eye = lax.broadcasted_iota(jnp.int32, (tile, tile), 0) == lax.broadcasted_iota(jnp.int32, (tile, tile), 1)
    row_id = lax.broadcasted_iota(jnp.int32, (rows, tile), 0)
    for c in range(n_blocks):
        if c < blk_rows:
            place[c] = jnp.zeros(place.shape[1:], jnp.bfloat16)
            place[c, c * tile : (c + 1) * tile, :] = one_hot(eye)
        else:
            place[c, 0:rows, :] = jnp.zeros((rows, tile), jnp.bfloat16)

    for load in loads[:3]:
        load.wait()

    lower = jnp.full((8, rows), bounds[0], f32)
    upper = jnp.full((8, rows), bounds[1], f32)
    centre = (lower + upper) / 2.0
    inverse = (1.0 / centre)[0:1]

    first = (p * n_sub + s) * rows
    src = jnp.transpose(src_lanes[...])
    lane = lax.broadcasted_iota(jnp.int32, (1, tile), 1) + first

    def count(start, size, ids):
        sums = [jnp.zeros((size, tile), f32) for _ in ids]
        for source in range(src.shape[1]):
            wide = jnp.broadcast_to(src[start : start + size, source : source + 1], (size, tile))
            sums = [jnp.where(wide == v, a + 1.0, a) for v, a in zip(ids, sums)]
        return sums

    def send(step, group, j):
        rows_of = pl.ds(group * k_group, k_group)
        return pltpu.make_async_remote_copy(
            src_ref=send_buf.at[step, j, rows_of, :],
            dst_ref=recv_buf.at[step, lands[j], rows_of, :],
            send_sem=send_sem.at[lax.rem(step, 2), group],
            recv_sem=recv_sem.at[lax.rem(step, 2), group],
            device_id=targets[j],
            device_id_type=MESH,
        )

    def start_sends(step, group, which=(0, 1, 2, 3)):
        for j in which:
            send(step, group, j).start()

    def wait_all(buf, sems, step, group):
        parts = buf.at[step, :, pl.ds(group * k_group, k_group), :]
        pltpu.make_async_copy(parts, parts, sems.at[lax.rem(step, 2), group]).wait()

    def wait_recvs(step, group):
        wait_all(recv_buf, recv_sem, step, group)

    def wait_sends(step):
        for group in range(groups):
            wait_all(send_buf, send_sem, step, group)

    for group in range(groups):
        at = slice(group * k_group, (group + 1) * k_group)
        ids = [send_rows[j : j + 1, :] + first for j in range(dirs)]
        for j, total in enumerate(count(group * k_group, k_group, ids)):
            scaled = total * inverse[:, :tile]
            send_buf[0, j, at, :] = scaled
            r_pack[at, j * tile : (j + 1) * tile] = total
            d_pack[at, j * tile : (j + 1) * tile] = scaled
            x_pack[at, j * tile : (j + 1) * tile] = scaled

    loads[3].wait()
    for c in range(blk_rows, n_blocks):
        h = c - blk_rows
        place[c, rows : 2 * rows, :] = one_hot(recv_rows[:, h * tile : (h + 1) * tile] == row_id)
    for j in range(dirs):
        pick[:, j * tile : (j + 1) * tile] = one_hot(send_rows[j : j + 1, :] == row_id)

    for load in loads[4:]:
        load.wait()

    def build_rows(b):
        for n in range(per_row):
            high, low = split(tiles[b, n])
            tile_pair[0:tile, n * tile : (n + 1) * tile] = high
            tile_pair[tile : 2 * tile, n * tile : (n + 1) * tile] = low
        starts = [[(u + len(units) * i) * CUT for i in range(2)] for u in units]
        for depth in range(0, per_row * tile, CUT):
            for u in units:
                jobs = []
                for acc, start in zip(build_accs[u], starts[u]):
                    spots = [place[cols[b, n], start : start + CUT, :] for n in range(depth // tile, (depth + CUT) // tile)]
                    jobs.append((acc, jnp.concatenate(spots, axis=1)))
                feed(u, tile_pair[:, depth : depth + CUT], jobs, transpose=True)
        for i in range(2):
            for u in units:
                start = starts[u][i]
                both = pltpu.matmul_pop(build_accs[u][i])
                block = both[:, :tile] + both[:, tile:]
                offset = b * tile - start
                if 0 <= offset < CUT:
                    extra = jnp.where(eye, diag[b : b + 1, :], 0.0)
                    pieces = [jnp.zeros((tile, tile), f32)] * (CUT // tile)
                    pieces[offset // tile] = extra
                    block = block + jnp.concatenate(pieces, axis=0)
                high, low = split(block)
                w_high[start : start + CUT, b * tile : (b + 1) * tile] = high
                w_low[start : start + CUT, b * tile : (b + 1) * tile] = low

        share = k_all // blk_rows
        at = slice(b * share, (b + 1) * share)
        low_at = slice(k_all + b * share, k_all + (b + 1) * share)
        for i, total in enumerate(count(b * share, share, [lane + i * tile for i in range(blk_rows)])):
            cols_at = slice(i * tile, (i + 1) * tile)
            b_own[at, cols_at] = total
            r_own[at, cols_at] = total
            scaled = total * inverse[:, :tile]
            d_own[at, cols_at] = scaled
            x_own[at, cols_at] = scaled
            high, low = split(scaled)
            ext[at, cols_at] = high
            ext[low_at, cols_at] = low

    build_rows(0)

    pl.semaphore_wait(barrier, greeted)
    for group in range(groups):
        start_sends(0, group)

    def hello(distance):
        for offset in (distance, planes - distance):
            pl.semaphore_signal(
                hello_sems.at[distance - 1], inc=1, device_id=axis_target(offset), device_id_type=MESH
            )

    hello(1)

    for b in range(1, blk_rows):
        build_rows(b)

    half_width = (upper - lower) / 2.0
    ratio = centre / half_width
    damping = 1.0 / ratio
    for step in range(ITERS - 1):
        following = 1.0 / (2.0 * ratio - damping)
        coef[2 * step] = following * damping
        coef[2 * step + 1] = 2.0 * following / half_width
        damping = following

    for start in range(0, 2 * rows, CUT):
        chunk_rows = slice(start, start + CUT)
        for depth in range(0, rows, CUT):
            for u in units:
                jobs = [(acc, w[chunk_rows, depth : depth + CUT]) for acc, w in zip(build_accs[u], (w_high, w_low))]
                feed(u, pick[depth : depth + CUT, u * CUT : (u + 1) * CUT], jobs)
        for i, w in enumerate((w_high, w_low)):
            for u in units:
                at = slice(rows + u * CUT, rows + (u + 1) * CUT)
                w[chunk_rows, at] = pltpu.matmul_pop(build_accs[u][i]).astype(jnp.bfloat16)

    own, got = slice(0, rows), slice(rows, 2 * rows)

    def products(depth_all, first_col):
        for depth in range(0, depth_all, CUT):
            at = slice(depth, depth + CUT)
            for weights, lows in ((w_high, True), (w_low, False)):
                for u in units:
                    top, bottom = field_accs[u]
                    jobs = [(top, ext[0:k_all, at])]
                    if lows:
                        jobs.append((bottom, ext[k_all : 2 * k_all, at]))
                    feed(u, weights[at, first_col + u * CUT : first_col + (u + 1) * CUT], jobs)
        return [pltpu.matmul_pop(top) + pltpu.matmul_pop(bottom) for top, bottom in field_accs]

    def packed_part():
        for u, product in enumerate(products(rows, rows)):
            part[:, u * CUT : (u + 1) * CUT] = product

    packed_part()
    pl.semaphore_wait(hello_sems.at[0], 2)
    hello(2)

    def take_halo(step, group):
        at = pl.ds(group * k_group, k_group)
        wait_recvs(step, group)
        halo = jnp.concatenate([recv_buf[step, j, at, :] for j in range(dirs)], axis=1)
        return split(halo)

    depths = range(0, rows, CUT)

    def stage(weights, first_col, unit, i):
        tile_rows = slice(rows + depths[i], rows + depths[i] + CUT)
        tile_cols = slice(first_col + unit * CUT, first_col + (unit + 1) * CUT)
        pltpu.matmul_push_rhs(weights[tile_rows, tile_cols], staging_register=i, mxu_index=unit)

    def stage_first(first_col):
        for i in range(len(depths)):
            for unit in units:
                stage(w_high, first_col, unit, i)

    def multiply(high, low, first_col, slot, more):
        parts = jnp.concatenate([high, low], axis=0)
        for following in (w_low, w_high if more else None):
            for i, depth in enumerate(depths):
                for unit in units:
                    pltpu.matmul_acc_lhs(halo_accs[unit][slot], parts[:, depth : depth + CUT], load_staged_rhs=i)
                    if following is not None:
                        stage(following, first_col, unit, i)

    def collect(slot):
        both = jnp.concatenate([pltpu.matmul_pop(halo_accs[unit][slot]) for unit in units], axis=1)
        return both[:k_group] + both[k_group:]

    def iteration(step, carry):
        alpha = coef[2 * step][0:1]
        beta = coef[2 * step + 1][0:1]
        last = (step == ITERS - 2).astype(f32)

        def finish(group):
            at = slice(group * k_group, (group + 1) * k_group)
            coupled = collect(group % 2)
            for which in ((0, 1), (2, 3)):
                half = slice(which[0] * tile, (which[-1] + 1) * tile)
                r_new = r_pack[at, half] - (part[at, half] + coupled[:, half])
                d_new = alpha[:, half] * d_pack[at, half] + beta[:, half] * r_new
                x_old = x_pack[at, half]
                going = d_new + last * x_old
                for i, j in enumerate(which):
                    send_buf[step + 1, j, at, :] = going[:, i * tile : (i + 1) * tile]
                start_sends(step + 1, group, which)
                r_pack[at, half] = r_new
                d_pack[at, half] = d_new
                x_pack[at, half] = x_old + d_new

        stage_first(rows)
        for group in range(groups):
            g0 = group * k_group
            high, low = take_halo(step, group)
            multiply(high, low, rows, group % 2, group + 1 < groups)
            ext[g0 : g0 + k_group, got] = high
            ext[k_all + g0 : k_all + g0 + k_group, got] = low
            if group > 0:
                finish(group - 1)
        finish(groups - 1)
        wait_sends(step)
        for u, product in enumerate(products(2 * rows, 0)):
            at = slice(u * CUT, (u + 1) * CUT)
            r_new = r_own[:, at] - product
            d_new = alpha[:, at] * d_own[:, at] + beta[:, at] * r_new
            r_own[:, at] = r_new
            d_own[:, at] = d_new
        for start in range(0, rows, CUT):
            at = slice(start, start + CUT)
            d_new = d_own[:, at]
            x_old = x_own[:, at]
            x_own[:, at] = x_old + d_new
            high, low = split(d_new + last * x_old)
            ext[0:k_all, at] = high
            ext[k_all : 2 * k_all, at] = low
        packed_part()
        return carry

    lax.fori_loop(0, ITERS - 1, iteration, 0)

    for u, product in enumerate(products(rows, 0)):
        at = slice(u * CUT, (u + 1) * CUT)
        r_own[:, at] = b_own[:, at] - product
    for i in range(blk_rows):
        out_buf[i * tile : (i + 1) * tile, :] = jnp.transpose(x_own[:, i * tile : (i + 1) * tile])

    out_copy = pltpu.make_async_copy(out_buf, x_out, out_sem)
    out_copy.start()
    pl.semaphore_wait(hello_sems.at[1], 2)

    def square(group):
        final = r_own[group * k_group : (group + 1) * k_group, :] - collect(group % 2)
        final = final * final
        total = final[:, 0:tile]
        for i in range(1, blk_rows):
            total = total + final[:, i * tile : (i + 1) * tile]
        return total

    squares = []
    stage_first(0)
    for group in range(groups):
        high, low = take_halo(ITERS - 1, group)
        multiply(high, low, 0, group % 2, group + 1 < groups)
        if group > 0:
            squares.append(square(group - 1))
    squares.append(square(groups - 1))
    squares = jnp.transpose(jnp.concatenate(squares, axis=0))
    mine = jnp.sum(squares, axis=0, keepdims=True)

    plane_send[...] = mine
    plane_recv[my_slot] = mine
    plane_copies = [
        pltpu.make_async_remote_copy(
            src_ref=plane_send,
            dst_ref=plane_recv.at[my_slot],
            send_sem=norm_sems.at[0],
            recv_sem=norm_sems.at[1],
            device_id=plane_target(offset),
            device_id_type=MESH,
        )
        for offset in range(1, in_plane)
    ]
    for copy in plane_copies:
        copy.start()
    others = plane_recv.at[pl.ds(0, in_plane - 1)]
    pltpu.make_async_copy(others, others, norm_sems.at[1]).wait()
    mine = jnp.sum(plane_recv[...], axis=0)

    axis_send[...] = mine
    own_copy = pltpu.make_async_copy(axis_send, axis_recv.at[my_plane], norm_sems.at[4])
    own_copy.start()
    axis_copies = [
        pltpu.make_async_remote_copy(
            src_ref=axis_send,
            dst_ref=axis_recv.at[my_plane],
            send_sem=norm_sems.at[2],
            recv_sem=norm_sems.at[3],
            device_id=axis_target(offset),
            device_id_type=MESH,
        )
        for offset in range(1, planes)
    ]
    for copy in axis_copies:
        copy.start()
    wait_sends(ITERS - 1)
    out_copy.wait()
    pltpu.make_async_copy(others, others, norm_sems.at[0]).wait()
    others = axis_recv.at[pl.ds(0, planes - 1)]
    pltpu.make_async_copy(others, others, norm_sems.at[3]).wait()
    own_copy.wait()
    pltpu.make_async_copy(others, others, norm_sems.at[2]).wait()


def kernel(shape, groups, k_all, rows, *refs):
    heights = (CUT, CUT, k_all, k_all, 2 * k_all // groups, 2 * k_all // groups)
    units = rows // CUT
    specs = [pltpu.ACC(unit)((height, CUT), jnp.float32) for unit in range(units) for height in heights]

    def body(*accs):
        per_unit = [accs[unit * len(heights) : (unit + 1) * len(heights)] for unit in range(units)]
        steps(per_unit, shape, *refs)

    pl.run_scoped(body, *specs)


def on_device(n_patch, n_sub, planes, sources, diag_coef, tiles, tile_cols, send_rows, recv_rows, bounds):
    rows = diag_coef.shape[0]
    k_all = sources.shape[0]
    blk_rows, per_row, tile, _ = tiles.shape
    dirs = send_rows.shape[1]
    n_blocks = 2 * blk_rows
    f32, bf16 = jnp.float32, jnp.bfloat16
    hbm = pl.BlockSpec(memory_space=pltpu.HBM)
    field = pltpu.VMEM((k_all, rows), f32)
    in_plane = n_patch // planes * n_sub
    x, sums = pl.pallas_call(
        functools.partial(kernel, (n_patch, n_sub, planes), GROUPS, k_all, rows),
        out_shape=(jax.ShapeDtypeStruct((rows, k_all), f32), jax.ShapeDtypeStruct((planes, 1, k_all), f32)),
        in_specs=[hbm] * 7,
        out_specs=(hbm, hbm),
        scratch_shapes=[
            pltpu.VMEM(sources.shape[::-1], jnp.int32),
            pltpu.VMEM((blk_rows, tile), f32),
            pltpu.SMEM(tile_cols.shape, jnp.int32),
            pltpu.VMEM(send_rows.shape[1:], jnp.int32),
            pltpu.VMEM(recv_rows.shape, jnp.int32),
            pltpu.SMEM(bounds.shape, f32),
            pltpu.VMEM(tiles.shape, f32),
            pltpu.VMEM((n_blocks, 2 * rows, tile), bf16),
            pltpu.VMEM((rows, rows), bf16),
            pltpu.VMEM((2 * tile, per_row * tile), bf16),
            pltpu.VMEM((2 * rows, 2 * rows), bf16),
            pltpu.VMEM((2 * rows, 2 * rows), bf16),
            pltpu.VMEM((2 * k_all, 2 * rows), bf16),
            field,
            field,
            field,
            field,
            field,
            field,
            field,
            field,
            pltpu.VMEM((2 * ITERS, 8, rows), f32),
            pltpu.VMEM((ITERS, dirs, k_all, tile), f32),
            pltpu.VMEM((ITERS, dirs, k_all, tile), f32),
            pltpu.VMEM((1, k_all), f32),
            pltpu.VMEM((in_plane, 1, k_all), f32),
            pltpu.VMEM((1, k_all), f32),
            pltpu.SemaphoreType.DMA((7,)),
            pltpu.SemaphoreType.DMA((2, GROUPS)),
            pltpu.SemaphoreType.DMA((2, GROUPS)),
            pltpu.SemaphoreType.DMA((5,)),
            pltpu.VMEM((rows, k_all), f32),
            pltpu.SemaphoreType.DMA,
            pltpu.SemaphoreType.REGULAR((2,)),
        ],
        compiler_params=pltpu.CompilerParams(
            collective_id=0, has_side_effects=True, vmem_limit_bytes=67_043_328
        ),
    )(
        sources.T,
        diag_coef.reshape(blk_rows, tile),
        tile_cols,
        send_rows[0],
        recv_rows,
        bounds,
        tiles,
    )
    return settle(x, sums)


def settle_kernel(x_in, sums_in, x_out, norm_out, x_buf, sums_buf, norm_buf, sems):
    read_sums = pltpu.make_async_copy(sums_in, sums_buf, sems.at[0])
    read_x = pltpu.make_async_copy(x_in, x_buf, sems.at[1])
    write_norm = pltpu.make_async_copy(norm_buf, norm_out, sems.at[0])
    write_x = pltpu.make_async_copy(x_buf, x_out, sems.at[1])
    read_sums.start()
    read_x.start()
    read_sums.wait()
    norm_buf[...] = jnp.sqrt(jnp.sum(sums_buf[...], axis=0))
    write_norm.start()
    read_x.wait()
    write_x.start()
    write_norm.wait()
    write_x.wait()


def settle(x, sums):
    hbm = pl.BlockSpec(memory_space=pl.ANY)
    norm_shape = jax.ShapeDtypeStruct(sums.shape[1:], sums.dtype)
    x, norm = pl.pallas_call(
        settle_kernel,
        out_shape=(jax.ShapeDtypeStruct(x.shape, x.dtype), norm_shape),
        in_specs=[hbm] * 2,
        out_specs=(hbm, hbm),
        scratch_shapes=[
            pltpu.VMEM(x.shape, x.dtype),
            pltpu.VMEM(sums.shape, sums.dtype),
            pltpu.VMEM(norm_shape.shape, norm_shape.dtype),
            pltpu.SemaphoreType.DMA((2,)),
        ],
        compiler_params=pltpu.CompilerParams(vmem_limit_bytes=67_043_328),
    )(x, sums)
    return x, norm[0]


def solution(mesh):
    n_patch, n_sub = mesh.shape["patch"], mesh.shape["sub"]
    both = ("patch", "sub")
    return jax.shard_map(
        functools.partial(on_device, n_patch, n_sub, PLANES),
        mesh=mesh,
        in_specs=(
            P(),
            P(both),
            P(both, None, None, None),
            P(both, None),
            P(both, None, None),
            P(both, None),
            P(),
        ),
        out_specs=(P(both, None), P()),
        check_vma=False,
    )
```

```python
import functools

import jax
import jax.numpy as jnp
from jax import lax
from jax.experimental import pallas as pl
from jax.experimental.pallas import tpu as pltpu
from jax.sharding import PartitionSpec as P

MESH = pl.DeviceIdType.MESH
ITERS = 8
GROUPS = 4
PLANES = 8
CUT = 256

def split(value):
    high = value.astype(jnp.bfloat16)
    low = (value - high.astype(jnp.float32)).astype(jnp.bfloat16)
    return high, low


def one_hot(equal):
    return jnp.where(equal, 1.0, 0.0).astype(jnp.bfloat16)


def steps(
    accs,
    shape,
    src_hbm,
    diag_hbm,
    cols_hbm,
    send_hbm,
    recv_hbm,
    bounds_hbm,
    tiles_hbm,
    x_out,
    axis_recv,
    src_lanes,
    diag,
    cols,
    send_rows,
    recv_rows,
    bounds,
    tiles,
    place,
    pick,
    tile_pair,
    w_high,
    w_low,
    ext,
    b_own,
    r_own,
    d_own,
    x_own,
    r_pack,
    d_pack,
    x_pack,
    part,
    coef,
    send_buf,
    recv_buf,
    plane_send,
    plane_recv,
    axis_send,
    load_sems,
    send_sem,
    recv_sem,
    norm_sems,
    out_buf,
    out_sem,
    hello_sems,
):
    n_patch, n_sub, planes = shape
    units = range(len(accs))
    build_accs = [unit_accs[0:2] for unit_accs in accs]
    field_accs = [unit_accs[2:4] for unit_accs in accs]
    halo_accs = [unit_accs[4:8] for unit_accs in accs]

    def feed(unit, weights, jobs, transpose=False):
        pltpu.matmul_push_rhs(weights, staging_register=0, mxu_index=unit, transpose=transpose)
        for i, (acc, operand) in enumerate(jobs):
            pltpu.matmul_acc_lhs(acc, operand, load_staged_rhs=0 if i == 0 else None)

    f32 = jnp.float32
    k_all, rows = b_own.shape
    per_row = tiles.shape[1]
    blk_rows = tiles.shape[0]
    tile = tiles.shape[2]
    n_blocks = place.shape[0]
    halo_blocks = n_blocks - blk_rows
    dirs = 4
    groups = send_sem.shape[1]
    k_group = k_all // groups

    p = lax.axis_index("patch")
    s = lax.axis_index("sub")
    plane = n_patch // planes
    in_plane = plane * n_sub
    my_plane = lax.div(p, plane)
    my_patch = lax.rem(p, plane)
    my_slot = my_patch * n_sub + s

    p_next = lax.rem(p + 1, n_patch)
    p_prev = lax.rem(p + n_patch - 1, n_patch)
    s_next = lax.rem(s + 1, n_sub)
    s_prev = lax.rem(s + n_sub - 1, n_sub)
    targets = ((p_prev, s), (p_next, s), (p, s_prev), (p, s_next))
    lands = (1, 0, 3, 2)

    def plane_target(offset):
        slot = lax.rem(my_slot + offset, in_plane)
        return (my_plane * plane + lax.div(slot, n_sub), lax.rem(slot, n_sub))

    def axis_target(offset):
        return (lax.rem(my_plane + offset, planes) * plane + my_patch, s)

    loads = [
        pltpu.make_async_copy(source, target, load_sems.at[i])
        for i, (source, target) in enumerate(
            (
                (src_hbm, src_lanes),
                (send_hbm, send_rows),
                (bounds_hbm, bounds),
                (recv_hbm, recv_rows),
                (cols_hbm, cols),
                (diag_hbm, diag),
                (tiles_hbm, tiles),
            )
        )
    ]
    for load in loads:
        load.start()
    barrier = pltpu.get_barrier_semaphore()
    greeted = 0
    for target in targets:
        pl.semaphore_signal(barrier, inc=1, device_id=target, device_id_type=MESH)
        greeted += 1
    for offset in (1, planes - 1):
        pl.semaphore_signal(barrier, inc=1, device_id=axis_target(offset), device_id_type=MESH)
        greeted += 1

    eye = lax.broadcasted_iota(jnp.int32, (tile, tile), 0) == lax.broadcasted_iota(jnp.int32, (tile, tile), 1)
    row_id = lax.broadcasted_iota(jnp.int32, (rows, tile), 0)
    for c in range(n_blocks):
        if c < blk_rows:
            place[c] = jnp.zeros(place.shape[1:], jnp.bfloat16)
            place[c, c * tile : (c + 1) * tile, :] = one_hot(eye)
        else:
            place[c, 0:rows, :] = jnp.zeros((rows, tile), jnp.bfloat16)

    for load in loads[:3]:
        load.wait()

    lower = jnp.full((8, rows), bounds[0], f32)
    upper = jnp.full((8, rows), bounds[1], f32)
    centre = (lower + upper) / 2.0
    inverse = (1.0 / centre)[0:1]

    first = (p * n_sub + s) * rows
    src = jnp.transpose(src_lanes[...])
    lane = lax.broadcasted_iota(jnp.int32, (1, tile), 1) + first

    def count(start, size, ids):
        sums = [jnp.zeros((size, tile), f32) for _ in ids]
        for source in range(src.shape[1]):
            wide = jnp.broadcast_to(src[start : start + size, source : source + 1], (size, tile))
            sums = [jnp.where(wide == v, a + 1.0, a) for v, a in zip(ids, sums)]
        return sums

    def send(step, group, j):
        rows_of = pl.ds(group * k_group, k_group)
        return pltpu.make_async_remote_copy(
            src_ref=send_buf.at[step, j, rows_of, :],
            dst_ref=recv_buf.at[step, lands[j], rows_of, :],
            send_sem=send_sem.at[lax.rem(step, 2), group],
            recv_sem=recv_sem.at[lax.rem(step, 2), group],
            device_id=targets[j],
            device_id_type=MESH,
        )

    def start_sends(step, group, which=(0, 1, 2, 3)):
        for j in which:
            send(step, group, j).start()

    def wait_all(buf, sems, step, group):
        parts = buf.at[step, :, pl.ds(group * k_group, k_group), :]
        pltpu.make_async_copy(parts, parts, sems.at[lax.rem(step, 2), group]).wait()

    def wait_recvs(step, group):
        wait_all(recv_buf, recv_sem, step, group)

    def wait_sends(step):
        for group in range(groups):
            wait_all(send_buf, send_sem, step, group)

    for group in range(groups):
        at = slice(group * k_group, (group + 1) * k_group)
        ids = [send_rows[j : j + 1, :] + first for j in range(dirs)]
        for j, total in enumerate(count(group * k_group, k_group, ids)):
            scaled = total * inverse[:, :tile]
            send_buf[0, j, at, :] = scaled
            r_pack[at, j * tile : (j + 1) * tile] = total
            d_pack[at, j * tile : (j + 1) * tile] = scaled
            x_pack[at, j * tile : (j + 1) * tile] = scaled

    loads[3].wait()
    for c in range(blk_rows, n_blocks):
        h = c - blk_rows
        place[c, rows : 2 * rows, :] = one_hot(recv_rows[:, h * tile : (h + 1) * tile] == row_id)
    for j in range(dirs):
        pick[:, j * tile : (j + 1) * tile] = one_hot(send_rows[j : j + 1, :] == row_id)

    for load in loads[4:]:
        load.wait()

    def build_rows(b):
        for n in range(per_row):
            high, low = split(tiles[b, n])
            tile_pair[0:tile, n * tile : (n + 1) * tile] = high
            tile_pair[tile : 2 * tile, n * tile : (n + 1) * tile] = low
        starts = [[(u + len(units) * i) * CUT for i in range(2)] for u in units]
        for depth in range(0, per_row * tile, CUT):
            for u in units:
                jobs = []
                for acc, start in zip(build_accs[u], starts[u]):
                    spots = [place[cols[b, n], start : start + CUT, :] for n in range(depth // tile, (depth + CUT) // tile)]
                    jobs.append((acc, jnp.concatenate(spots, axis=1)))
                feed(u, tile_pair[:, depth : depth + CUT], jobs, transpose=True)
        for i in range(2):
            for u in units:
                start = starts[u][i]
                both = pltpu.matmul_pop(build_accs[u][i])
                block = both[:, :tile] + both[:, tile:]
                offset = b * tile - start
                if 0 <= offset < CUT:
                    extra = jnp.where(eye, diag[b : b + 1, :], 0.0)
                    pieces = [jnp.zeros((tile, tile), f32)] * (CUT // tile)
                    pieces[offset // tile] = extra
                    block = block + jnp.concatenate(pieces, axis=0)
                high, low = split(block)
                w_high[start : start + CUT, b * tile : (b + 1) * tile] = high
                w_low[start : start + CUT, b * tile : (b + 1) * tile] = low

        share = k_all // blk_rows
        at = slice(b * share, (b + 1) * share)
        low_at = slice(k_all + b * share, k_all + (b + 1) * share)
        for i, total in enumerate(count(b * share, share, [lane + i * tile for i in range(blk_rows)])):
            cols_at = slice(i * tile, (i + 1) * tile)
            b_own[at, cols_at] = total
            r_own[at, cols_at] = total
            scaled = total * inverse[:, :tile]
            d_own[at, cols_at] = scaled
            x_own[at, cols_at] = scaled
            high, low = split(scaled)
            ext[at, cols_at] = high
            ext[low_at, cols_at] = low

    build_rows(0)

    pl.semaphore_wait(barrier, greeted)
    for group in range(groups):
        start_sends(0, group)

    def hello(distance):
        for offset in (distance, planes - distance):
            pl.semaphore_signal(
                hello_sems.at[distance - 1], inc=1, device_id=axis_target(offset), device_id_type=MESH
            )

    hello(1)

    for b in range(1, blk_rows):
        build_rows(b)

    half_width = (upper - lower) / 2.0
    ratio = centre / half_width
    damping = 1.0 / ratio
    for step in range(ITERS - 1):
        following = 1.0 / (2.0 * ratio - damping)
        coef[2 * step] = following * damping
        coef[2 * step + 1] = 2.0 * following / half_width
        damping = following

    for start in range(0, 2 * rows, CUT):
        chunk_rows = slice(start, start + CUT)
        for depth in range(0, rows, CUT):
            for u in units:
                jobs = [(acc, w[chunk_rows, depth : depth + CUT]) for acc, w in zip(build_accs[u], (w_high, w_low))]
                feed(u, pick[depth : depth + CUT, u * CUT : (u + 1) * CUT], jobs)
        for i, w in enumerate((w_high, w_low)):
            for u in units:
                at = slice(rows + u * CUT, rows + (u + 1) * CUT)
                w[chunk_rows, at] = pltpu.matmul_pop(build_accs[u][i]).astype(jnp.bfloat16)

    own, got = slice(0, rows), slice(rows, 2 * rows)

    def products(depth_all, first_col):
        for depth in range(0, depth_all, CUT):
            at = slice(depth, depth + CUT)
            for weights, lows in ((w_high, True), (w_low, False)):
                for u in units:
                    top, bottom = field_accs[u]
                    jobs = [(top, ext[0:k_all, at])]
                    if lows:
                        jobs.append((bottom, ext[k_all : 2 * k_all, at]))
                    feed(u, weights[at, first_col + u * CUT : first_col + (u + 1) * CUT], jobs)
        return [pltpu.matmul_pop(top) + pltpu.matmul_pop(bottom) for top, bottom in field_accs]

    def packed_part():
        for u, product in enumerate(products(rows, rows)):
            part[:, u * CUT : (u + 1) * CUT] = product

    packed_part()
    pl.semaphore_wait(hello_sems.at[0], 2)
    hello(2)

    def take_halo(step, group):
        at = pl.ds(group * k_group, k_group)
        wait_recvs(step, group)
        halo = jnp.concatenate([recv_buf[step, j, at, :] for j in range(dirs)], axis=1)
        return split(halo)

    def stage(first_col, half):
        for i, weights in enumerate((w_high, w_low)):
            for u in units:
                tile_rows = slice(rows + u * CUT, rows + (u + 1) * CUT)
                tile_cols = slice(first_col + half * CUT, first_col + (half + 1) * CUT)
                pltpu.matmul_push_rhs(weights[tile_rows, tile_cols], staging_register=i, mxu_index=u)

    def multiply(parts, half, slot):
        for i in range(2):
            for u in units:
                acc = halo_accs[u][2 * slot + half]
                pltpu.matmul_acc_lhs(acc, parts[:, u * CUT : (u + 1) * CUT], load_staged_rhs=i)

    def collect(half, slot):
        both = pltpu.matmul_pop(halo_accs[0][2 * slot + half])
        for u in units[1:]:
            both = both + pltpu.matmul_pop(halo_accs[u][2 * slot + half])
        return both[:k_group] + both[k_group:]

    def iteration(step, carry):
        alpha = coef[2 * step][0:1]
        beta = coef[2 * step + 1][0:1]
        last = (step == ITERS - 2).astype(f32)

        def finish(group, half):
            at = slice(group * k_group, (group + 1) * k_group)
            lanes = slice(half * CUT, (half + 1) * CUT)
            r_new = r_pack[at, lanes] - (part[at, lanes] + collect(half, group % 2))
            d_new = alpha[:, lanes] * d_pack[at, lanes] + beta[:, lanes] * r_new
            x_old = x_pack[at, lanes]
            going = d_new + last * x_old
            which = range(half * CUT // tile, (half + 1) * CUT // tile)
            for i, j in enumerate(which):
                send_buf[step + 1, j, at, :] = going[:, i * tile : (i + 1) * tile]
            start_sends(step + 1, group, which)
            r_pack[at, lanes] = r_new
            d_pack[at, lanes] = d_new
            x_pack[at, lanes] = x_old + d_new

        stage(rows, 0)
        for group in range(groups):
            g0 = group * k_group
            high, low = take_halo(step, group)
            parts = jnp.concatenate([high, low], axis=0)
            multiply(parts, 0, group % 2)
            stage(rows, 1)
            multiply(parts, 1, group % 2)
            finish(group, 0)
            if group > 0:
                finish(group - 1, 1)
            if group + 1 < groups:
                stage(rows, 0)
            ext[g0 : g0 + k_group, got] = high
            ext[k_all + g0 : k_all + g0 + k_group, got] = low
        finish(groups - 1, 1)
        wait_sends(step)
        for u, product in enumerate(products(2 * rows, 0)):
            at = slice(u * CUT, (u + 1) * CUT)
            r_new = r_own[:, at] - product
            d_new = alpha[:, at] * d_own[:, at] + beta[:, at] * r_new
            r_own[:, at] = r_new
            d_own[:, at] = d_new
        for start in range(0, rows, CUT):
            at = slice(start, start + CUT)
            d_new = d_own[:, at]
            x_old = x_own[:, at]
            x_own[:, at] = x_old + d_new
            high, low = split(d_new + last * x_old)
            ext[0:k_all, at] = high
            ext[k_all : 2 * k_all, at] = low
        packed_part()
        return carry

    lax.fori_loop(0, ITERS - 1, iteration, 0)

    for u, product in enumerate(products(rows, 0)):
        at = slice(u * CUT, (u + 1) * CUT)
        r_own[:, at] = b_own[:, at] - product
    for i in range(blk_rows):
        out_buf[i * tile : (i + 1) * tile, :] = jnp.transpose(x_own[:, i * tile : (i + 1) * tile])

    out_copy = pltpu.make_async_copy(out_buf, x_out, out_sem)
    out_copy.start()
    pl.semaphore_wait(hello_sems.at[1], 2)

    def square(group):
        at = slice(group * k_group, (group + 1) * k_group)
        total = jnp.zeros((k_group, tile), f32)
        for half in range(2):
            final = r_own[at, half * CUT : (half + 1) * CUT] - collect(half, group % 2)
            final = final * final
            for i in range(CUT // tile):
                total = total + final[:, i * tile : (i + 1) * tile]
        return total

    squares = []
    stage(0, 0)
    for group in range(groups):
        high, low = take_halo(ITERS - 1, group)
        parts = jnp.concatenate([high, low], axis=0)
        multiply(parts, 0, group % 2)
        stage(0, 1)
        multiply(parts, 1, group % 2)
        if group > 0:
            squares.append(square(group - 1))
        if group + 1 < groups:
            stage(0, 0)
    squares.append(square(groups - 1))
    squares = jnp.transpose(jnp.concatenate(squares, axis=0))
    mine = jnp.sum(squares, axis=0, keepdims=True)

    plane_send[...] = mine
    plane_recv[my_slot] = mine
    plane_copies = [
        pltpu.make_async_remote_copy(
            src_ref=plane_send,
            dst_ref=plane_recv.at[my_slot],
            send_sem=norm_sems.at[0],
            recv_sem=norm_sems.at[1],
            device_id=plane_target(offset),
            device_id_type=MESH,
        )
        for offset in range(1, in_plane)
    ]
    for copy in plane_copies:
        copy.start()
    others = plane_recv.at[pl.ds(0, in_plane - 1)]
    pltpu.make_async_copy(others, others, norm_sems.at[1]).wait()
    mine = jnp.sum(plane_recv[...], axis=0)

    axis_send[...] = mine
    own_copy = pltpu.make_async_copy(axis_send, axis_recv.at[my_plane], norm_sems.at[4])
    own_copy.start()
    axis_copies = [
        pltpu.make_async_remote_copy(
            src_ref=axis_send,
            dst_ref=axis_recv.at[my_plane],
            send_sem=norm_sems.at[2],
            recv_sem=norm_sems.at[3],
            device_id=axis_target(offset),
            device_id_type=MESH,
        )
        for offset in range(1, planes)
    ]
    for copy in axis_copies:
        copy.start()
    wait_sends(ITERS - 1)
    out_copy.wait()
    pltpu.make_async_copy(others, others, norm_sems.at[0]).wait()
    others = axis_recv.at[pl.ds(0, planes - 1)]
    pltpu.make_async_copy(others, others, norm_sems.at[3]).wait()
    own_copy.wait()
    pltpu.make_async_copy(others, others, norm_sems.at[2]).wait()


def kernel(shape, groups, k_all, rows, *refs):
    heights = (CUT, CUT, k_all, k_all) + 4 * (2 * k_all // groups,)
    units = rows // CUT
    specs = [pltpu.ACC(unit)((height, CUT), jnp.float32) for unit in range(units) for height in heights]

    def body(*accs):
        per_unit = [accs[unit * len(heights) : (unit + 1) * len(heights)] for unit in range(units)]
        steps(per_unit, shape, *refs)

    pl.run_scoped(body, *specs)


def on_device(n_patch, n_sub, planes, sources, diag_coef, tiles, tile_cols, send_rows, recv_rows, bounds):
    rows = diag_coef.shape[0]
    k_all = sources.shape[0]
    blk_rows, per_row, tile, _ = tiles.shape
    dirs = send_rows.shape[1]
    n_blocks = 2 * blk_rows
    f32, bf16 = jnp.float32, jnp.bfloat16
    hbm = pl.BlockSpec(memory_space=pltpu.HBM)
    field = pltpu.VMEM((k_all, rows), f32)
    in_plane = n_patch // planes * n_sub
    x, sums = pl.pallas_call(
        functools.partial(kernel, (n_patch, n_sub, planes), GROUPS, k_all, rows),
        out_shape=(jax.ShapeDtypeStruct((rows, k_all), f32), jax.ShapeDtypeStruct((planes, 1, k_all), f32)),
        in_specs=[hbm] * 7,
        out_specs=(hbm, hbm),
        scratch_shapes=[
            pltpu.VMEM(sources.shape[::-1], jnp.int32),
            pltpu.VMEM((blk_rows, tile), f32),
            pltpu.SMEM(tile_cols.shape, jnp.int32),
            pltpu.VMEM(send_rows.shape[1:], jnp.int32),
            pltpu.VMEM(recv_rows.shape, jnp.int32),
            pltpu.SMEM(bounds.shape, f32),
            pltpu.VMEM(tiles.shape, f32),
            pltpu.VMEM((n_blocks, 2 * rows, tile), bf16),
            pltpu.VMEM((rows, rows), bf16),
            pltpu.VMEM((2 * tile, per_row * tile), bf16),
            pltpu.VMEM((2 * rows, 2 * rows), bf16),
            pltpu.VMEM((2 * rows, 2 * rows), bf16),
            pltpu.VMEM((2 * k_all, 2 * rows), bf16),
            field,
            field,
            field,
            field,
            field,
            field,
            field,
            field,
            pltpu.VMEM((2 * ITERS, 8, rows), f32),
            pltpu.VMEM((ITERS, dirs, k_all, tile), f32),
            pltpu.VMEM((ITERS, dirs, k_all, tile), f32),
            pltpu.VMEM((1, k_all), f32),
            pltpu.VMEM((in_plane, 1, k_all), f32),
            pltpu.VMEM((1, k_all), f32),
            pltpu.SemaphoreType.DMA((7,)),
            pltpu.SemaphoreType.DMA((2, GROUPS)),
            pltpu.SemaphoreType.DMA((2, GROUPS)),
            pltpu.SemaphoreType.DMA((5,)),
            pltpu.VMEM((rows, k_all), f32),
            pltpu.SemaphoreType.DMA,
            pltpu.SemaphoreType.REGULAR((2,)),
        ],
        compiler_params=pltpu.CompilerParams(
            collective_id=0, has_side_effects=True, vmem_limit_bytes=67_043_328
        ),
    )(
        sources.T,
        diag_coef.reshape(blk_rows, tile),
        tile_cols,
        send_rows[0],
        recv_rows,
        bounds,
        tiles,
    )
    return settle(x, sums)


def settle_kernel(x_in, sums_in, x_out, norm_out, x_buf, sums_buf, norm_buf, sems):
    read_sums = pltpu.make_async_copy(sums_in, sums_buf, sems.at[0])
    read_x = pltpu.make_async_copy(x_in, x_buf, sems.at[1])
    write_norm = pltpu.make_async_copy(norm_buf, norm_out, sems.at[0])
    write_x = pltpu.make_async_copy(x_buf, x_out, sems.at[1])
    read_sums.start()
    read_x.start()
    read_sums.wait()
    norm_buf[...] = jnp.sqrt(jnp.sum(sums_buf[...], axis=0))
    write_norm.start()
    read_x.wait()
    write_x.start()
    write_norm.wait()
    write_x.wait()


def settle(x, sums):
    hbm = pl.BlockSpec(memory_space=pl.ANY)
    norm_shape = jax.ShapeDtypeStruct(sums.shape[1:], sums.dtype)
    x, norm = pl.pallas_call(
        settle_kernel,
        out_shape=(jax.ShapeDtypeStruct(x.shape, x.dtype), norm_shape),
        in_specs=[hbm] * 2,
        out_specs=(hbm, hbm),
        scratch_shapes=[
            pltpu.VMEM(x.shape, x.dtype),
            pltpu.VMEM(sums.shape, sums.dtype),
            pltpu.VMEM(norm_shape.shape, norm_shape.dtype),
            pltpu.SemaphoreType.DMA((2,)),
        ],
        compiler_params=pltpu.CompilerParams(vmem_limit_bytes=67_043_328),
    )(x, sums)
    return x, norm[0]


def solution(mesh):
    n_patch, n_sub = mesh.shape["patch"], mesh.shape["sub"]
    both = ("patch", "sub")
    return jax.shard_map(
        functools.partial(on_device, n_patch, n_sub, PLANES),
        mesh=mesh,
        in_specs=(
            P(),
            P(both),
            P(both, None, None, None),
            P(both, None),
            P(both, None, None),
            P(both, None),
            P(),
        ),
        out_specs=(P(both, None), P()),
        check_vma=False,
    )
```

```python
import functools

import jax
import jax.numpy as jnp
from jax import lax
from jax.experimental import pallas as pl
from jax.experimental.pallas import tpu as pltpu
from jax.sharding import PartitionSpec as P

MESH = pl.DeviceIdType.MESH
ITERS = 8
GROUPS = 4
PLANES = 8
CUT = 256

def split(value):
    high = value.astype(jnp.bfloat16)
    low = (value - high.astype(jnp.float32)).astype(jnp.bfloat16)
    return high, low


def one_hot(equal):
    return jnp.where(equal, 1.0, 0.0).astype(jnp.bfloat16)


def steps(
    accs,
    shape,
    src_hbm,
    diag_hbm,
    cols_hbm,
    send_hbm,
    recv_hbm,
    bounds_hbm,
    tiles_hbm,
    x_out,
    axis_recv,
    src_lanes,
    diag,
    cols,
    send_rows,
    recv_rows,
    bounds,
    tiles,
    place,
    pick,
    tile_pair,
    w_high,
    w_low,
    ext,
    b_own,
    r_own,
    d_own,
    x_own,
    r_pack,
    d_pack,
    x_pack,
    part,
    coef,
    send_buf,
    recv_buf,
    plane_send,
    plane_recv,
    axis_send,
    load_sems,
    send_sem,
    recv_sem,
    norm_sems,
    out_buf,
    out_sem,
    hello_sems,
):
    n_patch, n_sub, planes = shape
    units = range(len(accs))
    build_accs = [unit_accs[0:2] for unit_accs in accs]
    field_accs = [unit_accs[2:4] for unit_accs in accs]
    halo_accs = [unit_accs[4:8] for unit_accs in accs]

    def feed(unit, weights, jobs, transpose=False):
        pltpu.matmul_push_rhs(weights, staging_register=0, mxu_index=unit, transpose=transpose)
        for i, (acc, operand) in enumerate(jobs):
            pltpu.matmul_acc_lhs(acc, operand, load_staged_rhs=0 if i == 0 else None)

    f32 = jnp.float32
    k_all, rows = b_own.shape
    per_row = tiles.shape[1]
    blk_rows = tiles.shape[0]
    tile = tiles.shape[2]
    n_blocks = place.shape[0]
    halo_blocks = n_blocks - blk_rows
    dirs = 4
    groups = send_sem.shape[1]
    k_group = k_all // groups

    p = lax.axis_index("patch")
    s = lax.axis_index("sub")
    plane = n_patch // planes
    in_plane = plane * n_sub
    my_plane = lax.div(p, plane)
    my_patch = lax.rem(p, plane)
    my_slot = my_patch * n_sub + s

    p_next = lax.rem(p + 1, n_patch)
    p_prev = lax.rem(p + n_patch - 1, n_patch)
    s_next = lax.rem(s + 1, n_sub)
    s_prev = lax.rem(s + n_sub - 1, n_sub)
    targets = ((p_prev, s), (p_next, s), (p, s_prev), (p, s_next))
    lands = (1, 0, 3, 2)

    def plane_target(step):
        patch_step, sub_step = step
        return (my_plane * plane + lax.rem(my_patch + patch_step, plane), lax.rem(s + sub_step, n_sub))

    def ring(step, size):
        return min(step, size - step)

    plane_steps = [(a, b) for a in range(plane) for b in range(n_sub) if a or b]
    plane_steps.sort(key=lambda step: -(ring(step[0], plane) / 2 + ring(step[1], n_sub)))
    axis_steps = sorted(range(1, planes), key=lambda step: -ring(step, planes))

    def axis_target(offset):
        return (lax.rem(my_plane + offset, planes) * plane + my_patch, s)

    loads = [
        pltpu.make_async_copy(source, target, load_sems.at[i])
        for i, (source, target) in enumerate(
            (
                (src_hbm, src_lanes),
                (send_hbm, send_rows),
                (bounds_hbm, bounds),
                (recv_hbm, recv_rows),
                (cols_hbm, cols),
                (diag_hbm, diag),
                (tiles_hbm, tiles),
            )
        )
    ]
    for load in loads:
        load.start()
    barrier = pltpu.get_barrier_semaphore()
    greeted = 0
    for target in targets:
        pl.semaphore_signal(barrier, inc=1, device_id=target, device_id_type=MESH)
        greeted += 1
    for offset in (1, planes - 1):
        pl.semaphore_signal(barrier, inc=1, device_id=axis_target(offset), device_id_type=MESH)
        greeted += 1

    eye = lax.broadcasted_iota(jnp.int32, (tile, tile), 0) == lax.broadcasted_iota(jnp.int32, (tile, tile), 1)
    row_id = lax.broadcasted_iota(jnp.int32, (rows, tile), 0)
    for c in range(n_blocks):
        if c < blk_rows:
            place[c] = jnp.zeros(place.shape[1:], jnp.bfloat16)
            place[c, c * tile : (c + 1) * tile, :] = one_hot(eye)
        else:
            place[c, 0:rows, :] = jnp.zeros((rows, tile), jnp.bfloat16)

    for load in loads[:3]:
        load.wait()

    lower = jnp.full((8, rows), bounds[0], f32)
    upper = jnp.full((8, rows), bounds[1], f32)
    centre = (lower + upper) / 2.0
    inverse = (1.0 / centre)[0:1]

    first = (p * n_sub + s) * rows
    src = jnp.transpose(src_lanes[...])
    lane = lax.broadcasted_iota(jnp.int32, (1, tile), 1) + first

    def count(start, size, ids):
        sums = [jnp.zeros((size, tile), f32) for _ in ids]
        for source in range(src.shape[1]):
            wide = jnp.broadcast_to(src[start : start + size, source : source + 1], (size, tile))
            sums = [jnp.where(wide == v, a + 1.0, a) for v, a in zip(ids, sums)]
        return sums

    def send(step, group, j):
        rows_of = pl.ds(group * k_group, k_group)
        return pltpu.make_async_remote_copy(
            src_ref=send_buf.at[step, j, rows_of, :],
            dst_ref=recv_buf.at[step, lands[j], rows_of, :],
            send_sem=send_sem.at[lax.rem(step, 2), group],
            recv_sem=recv_sem.at[lax.rem(step, 2), group],
            device_id=targets[j],
            device_id_type=MESH,
        )

    def start_sends(step, group, which=(0, 1, 2, 3)):
        for j in which:
            send(step, group, j).start()

    def wait_all(buf, sems, step, group):
        parts = buf.at[step, :, pl.ds(group * k_group, k_group), :]
        pltpu.make_async_copy(parts, parts, sems.at[lax.rem(step, 2), group]).wait()

    def wait_recvs(step, group):
        wait_all(recv_buf, recv_sem, step, group)

    def wait_sends(step):
        for group in range(groups):
            wait_all(send_buf, send_sem, step, group)

    for group in range(groups):
        at = slice(group * k_group, (group + 1) * k_group)
        ids = [send_rows[j : j + 1, :] + first for j in range(dirs)]
        for j, total in enumerate(count(group * k_group, k_group, ids)):
            scaled = total * inverse[:, :tile]
            send_buf[0, j, at, :] = scaled
            r_pack[at, j * tile : (j + 1) * tile] = total
            d_pack[at, j * tile : (j + 1) * tile] = scaled
            x_pack[at, j * tile : (j + 1) * tile] = scaled

    loads[3].wait()
    for c in range(blk_rows, n_blocks):
        h = c - blk_rows
        place[c, rows : 2 * rows, :] = one_hot(recv_rows[:, h * tile : (h + 1) * tile] == row_id)
    for j in range(dirs):
        pick[:, j * tile : (j + 1) * tile] = one_hot(send_rows[j : j + 1, :] == row_id)

    for load in loads[4:]:
        load.wait()

    def build_rows(b):
        for n in range(per_row):
            high, low = split(tiles[b, n])
            tile_pair[0:tile, n * tile : (n + 1) * tile] = high
            tile_pair[tile : 2 * tile, n * tile : (n + 1) * tile] = low
        starts = [[(u + len(units) * i) * CUT for i in range(2)] for u in units]
        for depth in range(0, per_row * tile, CUT):
            for u in units:
                jobs = []
                for acc, start in zip(build_accs[u], starts[u]):
                    spots = [place[cols[b, n], start : start + CUT, :] for n in range(depth // tile, (depth + CUT) // tile)]
                    jobs.append((acc, jnp.concatenate(spots, axis=1)))
                feed(u, tile_pair[:, depth : depth + CUT], jobs, transpose=True)
        for i in range(2):
            for u in units:
                start = starts[u][i]
                both = pltpu.matmul_pop(build_accs[u][i])
                block = both[:, :tile] + both[:, tile:]
                offset = b * tile - start
                if 0 <= offset < CUT:
                    extra = jnp.where(eye, diag[b : b + 1, :], 0.0)
                    pieces = [jnp.zeros((tile, tile), f32)] * (CUT // tile)
                    pieces[offset // tile] = extra
                    block = block + jnp.concatenate(pieces, axis=0)
                high, low = split(block)
                w_high[start : start + CUT, b * tile : (b + 1) * tile] = high
                w_low[start : start + CUT, b * tile : (b + 1) * tile] = low

        share = k_all // blk_rows
        at = slice(b * share, (b + 1) * share)
        low_at = slice(k_all + b * share, k_all + (b + 1) * share)
        for i, total in enumerate(count(b * share, share, [lane + i * tile for i in range(blk_rows)])):
            cols_at = slice(i * tile, (i + 1) * tile)
            b_own[at, cols_at] = total
            r_own[at, cols_at] = total
            scaled = total * inverse[:, :tile]
            d_own[at, cols_at] = scaled
            x_own[at, cols_at] = scaled
            high, low = split(scaled)
            ext[at, cols_at] = high
            ext[low_at, cols_at] = low

    build_rows(0)

    pl.semaphore_wait(barrier, greeted)
    for group in range(groups):
        start_sends(0, group)

    def hello(distance):
        for offset in (distance, planes - distance):
            pl.semaphore_signal(
                hello_sems.at[distance - 1], inc=1, device_id=axis_target(offset), device_id_type=MESH
            )

    hello(1)

    for b in range(1, blk_rows):
        build_rows(b)

    half_width = (upper - lower) / 2.0
    ratio = centre / half_width
    damping = 1.0 / ratio
    for step in range(ITERS - 1):
        following = 1.0 / (2.0 * ratio - damping)
        coef[2 * step] = following * damping
        coef[2 * step + 1] = 2.0 * following / half_width
        damping = following

    for start in range(0, 2 * rows, CUT):
        chunk_rows = slice(start, start + CUT)
        for depth in range(0, rows, CUT):
            for u in units:
                jobs = [(acc, w[chunk_rows, depth : depth + CUT]) for acc, w in zip(build_accs[u], (w_high, w_low))]
                feed(u, pick[depth : depth + CUT, u * CUT : (u + 1) * CUT], jobs)
        for i, w in enumerate((w_high, w_low)):
            for u in units:
                at = slice(rows + u * CUT, rows + (u + 1) * CUT)
                w[chunk_rows, at] = pltpu.matmul_pop(build_accs[u][i]).astype(jnp.bfloat16)

    own, got = slice(0, rows), slice(rows, 2 * rows)

    def products(depth_all, first_col):
        for depth in range(0, depth_all, CUT):
            at = slice(depth, depth + CUT)
            for weights, lows in ((w_high, True), (w_low, False)):
                for u in units:
                    top, bottom = field_accs[u]
                    jobs = [(top, ext[0:k_all, at])]
                    if lows:
                        jobs.append((bottom, ext[k_all : 2 * k_all, at]))
                    feed(u, weights[at, first_col + u * CUT : first_col + (u + 1) * CUT], jobs)
        return [pltpu.matmul_pop(top) + pltpu.matmul_pop(bottom) for top, bottom in field_accs]

    def packed_part():
        for u, product in enumerate(products(rows, rows)):
            part[:, u * CUT : (u + 1) * CUT] = product

    packed_part()
    pl.semaphore_wait(hello_sems.at[0], 2)
    hello(2)

    def take_halo(step, group):
        at = pl.ds(group * k_group, k_group)
        wait_recvs(step, group)
        halo = jnp.concatenate([recv_buf[step, j, at, :] for j in range(dirs)], axis=1)
        return split(halo)

    def stage(first_col, half):
        for i, weights in enumerate((w_high, w_low)):
            for u in units:
                tile_rows = slice(rows + u * CUT, rows + (u + 1) * CUT)
                tile_cols = slice(first_col + half * CUT, first_col + (half + 1) * CUT)
                pltpu.matmul_push_rhs(weights[tile_rows, tile_cols], staging_register=i, mxu_index=u)

    def multiply(parts, half, slot):
        for i in range(2):
            for u in units:
                acc = halo_accs[u][2 * slot + half]
                pltpu.matmul_acc_lhs(acc, parts[:, u * CUT : (u + 1) * CUT], load_staged_rhs=i)

    def collect(half, slot):
        both = pltpu.matmul_pop(halo_accs[0][2 * slot + half])
        for u in units[1:]:
            both = both + pltpu.matmul_pop(halo_accs[u][2 * slot + half])
        return both[:k_group] + both[k_group:]

    def iteration(step, carry):
        alpha = coef[2 * step][0:1]
        beta = coef[2 * step + 1][0:1]
        last = (step == ITERS - 2).astype(f32)

        def finish(group, half):
            at = slice(group * k_group, (group + 1) * k_group)
            lanes = slice(half * CUT, (half + 1) * CUT)
            r_new = r_pack[at, lanes] - (part[at, lanes] + collect(half, group % 2))
            d_new = alpha[:, lanes] * d_pack[at, lanes] + beta[:, lanes] * r_new
            x_old = x_pack[at, lanes]
            going = d_new + last * x_old
            which = range(half * CUT // tile, (half + 1) * CUT // tile)
            for i, j in enumerate(which):
                send_buf[step + 1, j, at, :] = going[:, i * tile : (i + 1) * tile]
            start_sends(step + 1, group, which)
            r_pack[at, lanes] = r_new
            d_pack[at, lanes] = d_new
            x_pack[at, lanes] = x_old + d_new

        stage(rows, 0)
        for group in range(groups):
            g0 = group * k_group
            high, low = take_halo(step, group)
            parts = jnp.concatenate([high, low], axis=0)
            multiply(parts, 0, group % 2)
            stage(rows, 1)
            multiply(parts, 1, group % 2)
            if group + 1 < groups:
                stage(rows, 0)
            finish(group, 0)
            if group > 0:
                finish(group - 1, 1)
            ext[g0 : g0 + k_group, got] = high
            ext[k_all + g0 : k_all + g0 + k_group, got] = low
        finish(groups - 1, 1)
        wait_sends(step)
        for u, product in enumerate(products(2 * rows, 0)):
            at = slice(u * CUT, (u + 1) * CUT)
            r_new = r_own[:, at] - product
            d_new = alpha[:, at] * d_own[:, at] + beta[:, at] * r_new
            r_own[:, at] = r_new
            d_own[:, at] = d_new
        for start in range(0, rows, CUT):
            at = slice(start, start + CUT)
            d_new = d_own[:, at]
            x_old = x_own[:, at]
            x_own[:, at] = x_old + d_new
            high, low = split(d_new + last * x_old)
            ext[0:k_all, at] = high
            ext[k_all : 2 * k_all, at] = low
        packed_part()
        return carry

    lax.fori_loop(0, ITERS - 1, iteration, 0)

    for u, product in enumerate(products(rows, 0)):
        at = slice(u * CUT, (u + 1) * CUT)
        r_own[:, at] = b_own[:, at] - product
    for i in range(blk_rows):
        out_buf[i * tile : (i + 1) * tile, :] = jnp.transpose(x_own[:, i * tile : (i + 1) * tile])

    out_copy = pltpu.make_async_copy(out_buf, x_out, out_sem)
    out_copy.start()
    pl.semaphore_wait(hello_sems.at[1], 2)

    def square(group):
        at = slice(group * k_group, (group + 1) * k_group)
        total = jnp.zeros((k_group, tile), f32)
        for half in range(2):
            final = r_own[at, half * CUT : (half + 1) * CUT] - collect(half, group % 2)
            final = final * final
            for i in range(CUT // tile):
                total = total + final[:, i * tile : (i + 1) * tile]
        return total

    squares = []
    stage(0, 0)
    for group in range(groups):
        high, low = take_halo(ITERS - 1, group)
        parts = jnp.concatenate([high, low], axis=0)
        multiply(parts, 0, group % 2)
        stage(0, 1)
        multiply(parts, 1, group % 2)
        if group > 0:
            squares.append(square(group - 1))
        if group + 1 < groups:
            stage(0, 0)
    squares.append(square(groups - 1))
    squares = jnp.transpose(jnp.concatenate(squares, axis=0))
    mine = jnp.sum(squares, axis=0, keepdims=True)

    plane_send[...] = mine
    plane_recv[my_slot] = mine
    plane_copies = [
        pltpu.make_async_remote_copy(
            src_ref=plane_send,
            dst_ref=plane_recv.at[my_slot],
            send_sem=norm_sems.at[0],
            recv_sem=norm_sems.at[1],
            device_id=plane_target(step),
            device_id_type=MESH,
        )
        for step in plane_steps
    ]
    for copy in plane_copies:
        copy.start()
    others = plane_recv.at[pl.ds(0, in_plane - 1)]
    pltpu.make_async_copy(others, others, norm_sems.at[1]).wait()
    mine = jnp.sum(plane_recv[...], axis=0)

    axis_send[...] = mine
    own_copy = pltpu.make_async_copy(axis_send, axis_recv.at[my_plane], norm_sems.at[4])
    own_copy.start()
    axis_copies = [
        pltpu.make_async_remote_copy(
            src_ref=axis_send,
            dst_ref=axis_recv.at[my_plane],
            send_sem=norm_sems.at[2],
            recv_sem=norm_sems.at[3],
            device_id=axis_target(offset),
            device_id_type=MESH,
        )
        for offset in axis_steps
    ]
    for copy in axis_copies:
        copy.start()
    wait_sends(ITERS - 1)
    out_copy.wait()
    pltpu.make_async_copy(others, others, norm_sems.at[0]).wait()
    others = axis_recv.at[pl.ds(0, planes - 1)]
    pltpu.make_async_copy(others, others, norm_sems.at[3]).wait()
    own_copy.wait()
    pltpu.make_async_copy(others, others, norm_sems.at[2]).wait()


def kernel(shape, groups, k_all, rows, *refs):
    heights = (CUT, CUT, k_all, k_all) + 4 * (2 * k_all // groups,)
    units = rows // CUT
    specs = [pltpu.ACC(unit)((height, CUT), jnp.float32) for unit in range(units) for height in heights]

    def body(*accs):
        per_unit = [accs[unit * len(heights) : (unit + 1) * len(heights)] for unit in range(units)]
        steps(per_unit, shape, *refs)

    pl.run_scoped(body, *specs)


def on_device(n_patch, n_sub, planes, sources, diag_coef, tiles, tile_cols, send_rows, recv_rows, bounds):
    rows = diag_coef.shape[0]
    k_all = sources.shape[0]
    blk_rows, per_row, tile, _ = tiles.shape
    dirs = send_rows.shape[1]
    n_blocks = 2 * blk_rows
    f32, bf16 = jnp.float32, jnp.bfloat16
    hbm = pl.BlockSpec(memory_space=pltpu.HBM)
    field = pltpu.VMEM((k_all, rows), f32)
    in_plane = n_patch // planes * n_sub
    x, sums = pl.pallas_call(
        functools.partial(kernel, (n_patch, n_sub, planes), GROUPS, k_all, rows),
        out_shape=(jax.ShapeDtypeStruct((rows, k_all), f32), jax.ShapeDtypeStruct((planes, 1, k_all), f32)),
        in_specs=[hbm] * 7,
        out_specs=(hbm, hbm),
        scratch_shapes=[
            pltpu.VMEM(sources.shape[::-1], jnp.int32),
            pltpu.VMEM((blk_rows, tile), f32),
            pltpu.SMEM(tile_cols.shape, jnp.int32),
            pltpu.VMEM(send_rows.shape[1:], jnp.int32),
            pltpu.VMEM(recv_rows.shape, jnp.int32),
            pltpu.SMEM(bounds.shape, f32),
            pltpu.VMEM(tiles.shape, f32),
            pltpu.VMEM((n_blocks, 2 * rows, tile), bf16),
            pltpu.VMEM((rows, rows), bf16),
            pltpu.VMEM((2 * tile, per_row * tile), bf16),
            pltpu.VMEM((2 * rows, 2 * rows), bf16),
            pltpu.VMEM((2 * rows, 2 * rows), bf16),
            pltpu.VMEM((2 * k_all, 2 * rows), bf16),
            field,
            field,
            field,
            field,
            field,
            field,
            field,
            field,
            pltpu.VMEM((2 * ITERS, 8, rows), f32),
            pltpu.VMEM((ITERS, dirs, k_all, tile), f32),
            pltpu.VMEM((ITERS, dirs, k_all, tile), f32),
            pltpu.VMEM((1, k_all), f32),
            pltpu.VMEM((in_plane, 1, k_all), f32),
            pltpu.VMEM((1, k_all), f32),
            pltpu.SemaphoreType.DMA((7,)),
            pltpu.SemaphoreType.DMA((2, GROUPS)),
            pltpu.SemaphoreType.DMA((2, GROUPS)),
            pltpu.SemaphoreType.DMA((5,)),
            pltpu.VMEM((rows, k_all), f32),
            pltpu.SemaphoreType.DMA,
            pltpu.SemaphoreType.REGULAR((2,)),
        ],
        compiler_params=pltpu.CompilerParams(
            collective_id=0, has_side_effects=True, vmem_limit_bytes=67_043_328
        ),
    )(
        sources.T,
        diag_coef.reshape(blk_rows, tile),
        tile_cols,
        send_rows[0],
        recv_rows,
        bounds,
        tiles,
    )
    return settle(x, sums)


def settle_kernel(x_in, sums_in, x_out, norm_out, x_buf, sums_buf, norm_buf, sems):
    read_sums = pltpu.make_async_copy(sums_in, sums_buf, sems.at[0])
    read_x = pltpu.make_async_copy(x_in, x_buf, sems.at[1])
    write_norm = pltpu.make_async_copy(norm_buf, norm_out, sems.at[0])
    write_x = pltpu.make_async_copy(x_buf, x_out, sems.at[1])
    read_sums.start()
    read_x.start()
    read_sums.wait()
    norm_buf[...] = jnp.sqrt(jnp.sum(sums_buf[...], axis=0))
    write_norm.start()
    read_x.wait()
    write_x.start()
    write_norm.wait()
    write_x.wait()


def settle(x, sums):
    hbm = pl.BlockSpec(memory_space=pl.ANY)
    norm_shape = jax.ShapeDtypeStruct(sums.shape[1:], sums.dtype)
    x, norm = pl.pallas_call(
        settle_kernel,
        out_shape=(jax.ShapeDtypeStruct(x.shape, x.dtype), norm_shape),
        in_specs=[hbm] * 2,
        out_specs=(hbm, hbm),
        scratch_shapes=[
            pltpu.VMEM(x.shape, x.dtype),
            pltpu.VMEM(sums.shape, sums.dtype),
            pltpu.VMEM(norm_shape.shape, norm_shape.dtype),
            pltpu.SemaphoreType.DMA((2,)),
        ],
        compiler_params=pltpu.CompilerParams(vmem_limit_bytes=67_043_328),
    )(x, sums)
    return x, norm[0]


def solution(mesh):
    n_patch, n_sub = mesh.shape["patch"], mesh.shape["sub"]
    both = ("patch", "sub")
    return jax.shard_map(
        functools.partial(on_device, n_patch, n_sub, PLANES),
        mesh=mesh,
        in_specs=(
            P(),
            P(both),
            P(both, None, None, None),
            P(both, None),
            P(both, None, None),
            P(both, None),
            P(),
        ),
        out_specs=(P(both, None), P()),
        check_vma=False,
    )
```

```python
import functools

import jax
import jax.numpy as jnp
from jax import lax
from jax.experimental import pallas as pl
from jax.experimental.pallas import tpu as pltpu
from jax.sharding import PartitionSpec as P

MESH = pl.DeviceIdType.MESH
ITERS = 8
GROUPS = 4
PLANES = 8
CUT = 256

def split(value):
    high = value.astype(jnp.bfloat16)
    low = (value - high.astype(jnp.float32)).astype(jnp.bfloat16)
    return high, low


def one_hot(equal):
    return jnp.where(equal, 1.0, 0.0).astype(jnp.bfloat16)


def steps(
    accs,
    shape,
    src_hbm,
    diag_hbm,
    cols_hbm,
    send_hbm,
    recv_hbm,
    bounds_hbm,
    tiles_hbm,
    x_out,
    axis_recv,
    src_lanes,
    diag,
    cols,
    send_rows,
    recv_rows,
    bounds,
    tiles,
    place,
    pick,
    tile_pair,
    w_high,
    w_low,
    ext,
    b_own,
    r_own,
    d_own,
    x_own,
    r_pack,
    d_pack,
    x_pack,
    part,
    coef,
    send_buf,
    recv_buf,
    plane_send,
    plane_recv,
    axis_send,
    load_sems,
    send_sem,
    recv_sem,
    norm_sems,
    out_buf,
    out_sem,
    hello_sems,
    diag_rows,
):
    n_patch, n_sub, planes = shape
    units = range(len(accs))
    build_accs = [unit_accs[0:2] for unit_accs in accs]
    field_accs = [unit_accs[2:4] for unit_accs in accs]
    halo_accs = [unit_accs[4:8] for unit_accs in accs]

    def feed(unit, weights, jobs, transpose=False):
        pltpu.matmul_push_rhs(weights, staging_register=0, mxu_index=unit, transpose=transpose)
        for i, (acc, operand) in enumerate(jobs):
            pltpu.matmul_acc_lhs(acc, operand, load_staged_rhs=0 if i == 0 else None)

    f32 = jnp.float32
    k_all, rows = b_own.shape
    per_row = tiles.shape[1]
    blk_rows = tiles.shape[0]
    tile = tiles.shape[2]
    n_blocks = place.shape[0]
    halo_blocks = n_blocks - blk_rows
    dirs = 4
    groups = send_sem.shape[1]
    k_group = k_all // groups

    p = lax.axis_index("patch")
    s = lax.axis_index("sub")
    plane = n_patch // planes
    in_plane = plane * n_sub
    my_plane = lax.div(p, plane)
    my_patch = lax.rem(p, plane)
    my_slot = my_patch * n_sub + s

    p_next = lax.rem(p + 1, n_patch)
    p_prev = lax.rem(p + n_patch - 1, n_patch)
    s_next = lax.rem(s + 1, n_sub)
    s_prev = lax.rem(s + n_sub - 1, n_sub)
    targets = ((p_prev, s), (p_next, s), (p, s_prev), (p, s_next))
    lands = (1, 0, 3, 2)

    def plane_target(step):
        patch_step, sub_step = step
        return (my_plane * plane + lax.rem(my_patch + patch_step, plane), lax.rem(s + sub_step, n_sub))

    def ring(step, size):
        return min(step, size - step)

    plane_steps = [(a, b) for a in range(plane) for b in range(n_sub) if a or b]
    plane_steps.sort(key=lambda step: -(ring(step[0], plane) / 2 + ring(step[1], n_sub)))
    axis_steps = sorted(range(1, planes), key=lambda step: -ring(step, planes))

    def axis_target(offset):
        return (lax.rem(my_plane + offset, planes) * plane + my_patch, s)

    loads = [
        pltpu.make_async_copy(source, target, load_sems.at[i])
        for i, (source, target) in enumerate(
            (
                (src_hbm, src_lanes),
                (send_hbm, send_rows),
                (bounds_hbm, bounds),
                (recv_hbm, recv_rows),
                (cols_hbm, cols),
                (diag_hbm, diag),
                (tiles_hbm, tiles),
            )
        )
    ]
    for load in loads:
        load.start()
    barrier = pltpu.get_barrier_semaphore()
    greeted = 0
    for target in targets:
        pl.semaphore_signal(barrier, inc=1, device_id=target, device_id_type=MESH)
        greeted += 1
    for offset in (1, planes - 1):
        pl.semaphore_signal(barrier, inc=1, device_id=axis_target(offset), device_id_type=MESH)
        greeted += 1

    eye = lax.broadcasted_iota(jnp.int32, (tile, tile), 0) == lax.broadcasted_iota(jnp.int32, (tile, tile), 1)
    row_id = lax.broadcasted_iota(jnp.int32, (rows, tile), 0)
    for c in range(n_blocks):
        if c < blk_rows:
            place[c] = jnp.zeros(place.shape[1:], jnp.bfloat16)
            place[c, c * tile : (c + 1) * tile, :] = one_hot(eye)
        else:
            place[c, 0:rows, :] = jnp.zeros((rows, tile), jnp.bfloat16)

    for load in loads[:3]:
        load.wait()

    lower = jnp.full((8, rows), bounds[0], f32)
    upper = jnp.full((8, rows), bounds[1], f32)
    centre = (lower + upper) / 2.0
    inverse = (1.0 / centre)[0:1]

    first = (p * n_sub + s) * rows
    src = jnp.transpose(src_lanes[...])
    lane = lax.broadcasted_iota(jnp.int32, (1, tile), 1) + first

    def count(start, size, ids):
        sums = [jnp.zeros((size, tile), f32) for _ in ids]
        for source in range(src.shape[1]):
            wide = jnp.broadcast_to(src[start : start + size, source : source + 1], (size, tile))
            sums = [jnp.where(wide == v, a + 1.0, a) for v, a in zip(ids, sums)]
        return sums

    def send(step, group, j):
        rows_of = pl.ds(group * k_group, k_group)
        return pltpu.make_async_remote_copy(
            src_ref=send_buf.at[step, j, rows_of, :],
            dst_ref=recv_buf.at[step, lands[j], rows_of, :],
            send_sem=send_sem.at[lax.rem(step, 2), group],
            recv_sem=recv_sem.at[lax.rem(step, 2), group],
            device_id=targets[j],
            device_id_type=MESH,
        )

    def start_sends(step, group, which=(0, 1, 2, 3)):
        for j in which:
            send(step, group, j).start()

    def wait_all(buf, sems, step, group):
        parts = buf.at[step, :, pl.ds(group * k_group, k_group), :]
        pltpu.make_async_copy(parts, parts, sems.at[lax.rem(step, 2), group]).wait()

    def wait_recvs(step, group):
        wait_all(recv_buf, recv_sem, step, group)

    def wait_sends(step):
        for group in range(groups):
            wait_all(send_buf, send_sem, step, group)

    for group in range(groups):
        at = slice(group * k_group, (group + 1) * k_group)
        ids = [send_rows[j : j + 1, :] + first for j in range(dirs)]
        for j, total in enumerate(count(group * k_group, k_group, ids)):
            scaled = total * inverse[:, :tile]
            send_buf[0, j, at, :] = scaled
            r_pack[at, j * tile : (j + 1) * tile] = total
            d_pack[at, j * tile : (j + 1) * tile] = scaled
            x_pack[at, j * tile : (j + 1) * tile] = scaled

    loads[3].wait()
    for c in range(blk_rows, n_blocks):
        h = c - blk_rows
        place[c, rows : 2 * rows, :] = one_hot(recv_rows[:, h * tile : (h + 1) * tile] == row_id)
    for j in range(dirs):
        pick[:, j * tile : (j + 1) * tile] = one_hot(send_rows[j : j + 1, :] == row_id)

    for load in loads[4:]:
        load.wait()

    def build_rows(b):
        for n in range(per_row):
            high, low = split(tiles[b, n])
            tile_pair[0:tile, n * tile : (n + 1) * tile] = high
            tile_pair[tile : 2 * tile, n * tile : (n + 1) * tile] = low
        starts = [[(u + len(units) * i) * CUT for i in range(2)] for u in units]
        for depth in range(0, per_row * tile, CUT):
            for u in units:
                jobs = []
                for acc, start in zip(build_accs[u], starts[u]):
                    spots = [place[cols[b, n], start : start + CUT, :] for n in range(depth // tile, (depth + CUT) // tile)]
                    jobs.append((acc, jnp.concatenate(spots, axis=1)))
                feed(u, tile_pair[:, depth : depth + CUT], jobs, transpose=True)
        for i in range(2):
            for u in units:
                start = starts[u][i]
                both = pltpu.matmul_pop(build_accs[u][i])
                block = both[:, :tile] + both[:, tile:]
                high, low = split(block)
                w_high[start : start + CUT, b * tile : (b + 1) * tile] = high
                w_low[start : start + CUT, b * tile : (b + 1) * tile] = low

        share = k_all // blk_rows
        at = slice(b * share, (b + 1) * share)
        low_at = slice(k_all + b * share, k_all + (b + 1) * share)
        for i, total in enumerate(count(b * share, share, [lane + i * tile for i in range(blk_rows)])):
            cols_at = slice(i * tile, (i + 1) * tile)
            b_own[at, cols_at] = total
            r_own[at, cols_at] = total
            scaled = total * inverse[:, :tile]
            d_own[at, cols_at] = scaled
            x_own[at, cols_at] = scaled
            high, low = split(scaled)
            ext[at, cols_at] = high
            ext[low_at, cols_at] = low

    build_rows(0)

    pl.semaphore_wait(barrier, greeted)
    for group in range(groups):
        start_sends(0, group)

    def hello(distance):
        for offset in (distance, planes - distance):
            pl.semaphore_signal(
                hello_sems.at[distance - 1], inc=1, device_id=axis_target(offset), device_id_type=MESH
            )

    hello(1)

    for b in range(1, blk_rows):
        build_rows(b)

    half_width = (upper - lower) / 2.0
    ratio = centre / half_width
    damping = 1.0 / ratio
    for step in range(ITERS - 1):
        following = 1.0 / (2.0 * ratio - damping)
        coef[2 * step] = following * damping
        coef[2 * step + 1] = 2.0 * following / half_width
        damping = following

    for start in range(0, 2 * rows, CUT):
        chunk_rows = slice(start, start + CUT)
        for depth in range(0, rows, CUT):
            for u in units:
                jobs = [(acc, w[chunk_rows, depth : depth + CUT]) for acc, w in zip(build_accs[u], (w_high, w_low))]
                feed(u, pick[depth : depth + CUT, u * CUT : (u + 1) * CUT], jobs)
        for i, w in enumerate((w_high, w_low)):
            for u in units:
                at = slice(rows + u * CUT, rows + (u + 1) * CUT)
                w[chunk_rows, at] = pltpu.matmul_pop(build_accs[u][i]).astype(jnp.bfloat16)

    own, got = slice(0, rows), slice(rows, 2 * rows)

    def products(depth_all, first_col):
        for depth in range(0, depth_all, CUT):
            at = slice(depth, depth + CUT)
            for weights, lows in ((w_high, True), (w_low, False)):
                for u in units:
                    top, bottom = field_accs[u]
                    jobs = [(top, ext[0:k_all, at])]
                    if lows:
                        jobs.append((bottom, ext[k_all : 2 * k_all, at]))
                    feed(u, weights[at, first_col + u * CUT : first_col + (u + 1) * CUT], jobs)
        return [pltpu.matmul_pop(top) + pltpu.matmul_pop(bottom) for top, bottom in field_accs]

    on_own = jnp.concatenate([diag[b : b + 1, :] for b in range(blk_rows)], axis=1)
    line = lax.broadcasted_iota(jnp.int32, (2 * k_group, rows), 0)
    rest, thirds = on_own, jnp.zeros((2 * k_group, rows), f32)
    for i in range(3):
        third = rest.astype(jnp.bfloat16).astype(f32)
        thirds = jnp.where(line == i, third, thirds)
        rest = rest - third
    thirds = thirds.astype(jnp.bfloat16)
    for depth in range(0, rows, CUT):
        for u in units:
            jobs = [(halo_accs[u][0], thirds[:, depth : depth + CUT])]
            feed(u, pick[depth : depth + CUT, u * CUT : (u + 1) * CUT], jobs)
    on_pack = [jnp.sum(pltpu.matmul_pop(halo_accs[u][0])[0:8], axis=0, keepdims=True) for u in units]
    diag_rows[0:1, :] = on_own
    diag_rows[1:2, :] = jnp.concatenate(on_pack, axis=1)

    def packed_part():
        for u, product in enumerate(products(rows, rows)):
            at = slice(u * CUT, (u + 1) * CUT)
            part[:, at] = product + diag_rows[1:2, at] * d_pack[:, at]

    packed_part()
    pl.semaphore_wait(hello_sems.at[0], 2)
    hello(2)

    def take_halo(step, group):
        at = pl.ds(group * k_group, k_group)
        wait_recvs(step, group)
        halo = jnp.concatenate([recv_buf[step, j, at, :] for j in range(dirs)], axis=1)
        return split(halo)

    def stage(first_col, half):
        for i, weights in enumerate((w_high, w_low)):
            for u in units:
                tile_rows = slice(rows + u * CUT, rows + (u + 1) * CUT)
                tile_cols = slice(first_col + half * CUT, first_col + (half + 1) * CUT)
                pltpu.matmul_push_rhs(weights[tile_rows, tile_cols], staging_register=i, mxu_index=u)

    def multiply(parts, half, slot):
        for i in range(2):
            for u in units:
                acc = halo_accs[u][2 * slot + half]
                pltpu.matmul_acc_lhs(acc, parts[:, u * CUT : (u + 1) * CUT], load_staged_rhs=i)

    def collect(half, slot):
        both = pltpu.matmul_pop(halo_accs[0][2 * slot + half])
        for u in units[1:]:
            both = both + pltpu.matmul_pop(halo_accs[u][2 * slot + half])
        return both[:k_group] + both[k_group:]

    def iteration(step, carry):
        alpha = coef[2 * step][0:1]
        beta = coef[2 * step + 1][0:1]
        last = (step == ITERS - 2).astype(f32)

        def finish(group, half):
            at = slice(group * k_group, (group + 1) * k_group)
            lanes = slice(half * CUT, (half + 1) * CUT)
            r_new = r_pack[at, lanes] - (part[at, lanes] + collect(half, group % 2))
            d_new = alpha[:, lanes] * d_pack[at, lanes] + beta[:, lanes] * r_new
            x_old = x_pack[at, lanes]
            going = d_new + last * x_old
            which = range(half * CUT // tile, (half + 1) * CUT // tile)
            for i, j in enumerate(which):
                send_buf[step + 1, j, at, :] = going[:, i * tile : (i + 1) * tile]
            start_sends(step + 1, group, which)
            r_pack[at, lanes] = r_new
            d_pack[at, lanes] = d_new
            x_pack[at, lanes] = x_old + d_new

        stage(rows, 0)
        for group in range(groups):
            g0 = group * k_group
            high, low = take_halo(step, group)
            parts = jnp.concatenate([high, low], axis=0)
            multiply(parts, 0, group % 2)
            stage(rows, 1)
            multiply(parts, 1, group % 2)
            if group + 1 < groups:
                stage(rows, 0)
            finish(group, 0)
            if group > 0:
                finish(group - 1, 1)
            ext[g0 : g0 + k_group, got] = high
            ext[k_all + g0 : k_all + g0 + k_group, got] = low
        finish(groups - 1, 1)
        wait_sends(step)
        for u, product in enumerate(products(2 * rows, 0)):
            at = slice(u * CUT, (u + 1) * CUT)
            r_new = r_own[:, at] - (product + diag_rows[0:1, at] * d_own[:, at])
            d_new = alpha[:, at] * d_own[:, at] + beta[:, at] * r_new
            r_own[:, at] = r_new
            d_own[:, at] = d_new
        for start in range(0, rows, CUT):
            at = slice(start, start + CUT)
            d_new = d_own[:, at]
            x_old = x_own[:, at]
            x_own[:, at] = x_old + d_new
            high, low = split(d_new + last * x_old)
            ext[0:k_all, at] = high
            ext[k_all : 2 * k_all, at] = low
        packed_part()
        return carry

    lax.fori_loop(0, ITERS - 1, iteration, 0)

    for u, product in enumerate(products(rows, 0)):
        at = slice(u * CUT, (u + 1) * CUT)
        r_own[:, at] = b_own[:, at] - (product + diag_rows[0:1, at] * x_own[:, at])
    for i in range(blk_rows):
        out_buf[i * tile : (i + 1) * tile, :] = jnp.transpose(x_own[:, i * tile : (i + 1) * tile])

    out_copy = pltpu.make_async_copy(out_buf, x_out, out_sem)
    out_copy.start()
    pl.semaphore_wait(hello_sems.at[1], 2)

    def square(group):
        at = slice(group * k_group, (group + 1) * k_group)
        total = jnp.zeros((k_group, tile), f32)
        for half in range(2):
            final = r_own[at, half * CUT : (half + 1) * CUT] - collect(half, group % 2)
            final = final * final
            for i in range(CUT // tile):
                total = total + final[:, i * tile : (i + 1) * tile]
        return total

    squares = []
    stage(0, 0)
    for group in range(groups):
        high, low = take_halo(ITERS - 1, group)
        parts = jnp.concatenate([high, low], axis=0)
        multiply(parts, 0, group % 2)
        stage(0, 1)
        multiply(parts, 1, group % 2)
        if group > 0:
            squares.append(square(group - 1))
        if group + 1 < groups:
            stage(0, 0)
    squares.append(square(groups - 1))
    squares = jnp.transpose(jnp.concatenate(squares, axis=0))
    mine = jnp.sum(squares, axis=0, keepdims=True)

    plane_send[...] = mine
    plane_recv[my_slot] = mine
    plane_copies = [
        pltpu.make_async_remote_copy(
            src_ref=plane_send,
            dst_ref=plane_recv.at[my_slot],
            send_sem=norm_sems.at[0],
            recv_sem=norm_sems.at[1],
            device_id=plane_target(step),
            device_id_type=MESH,
        )
        for step in plane_steps
    ]
    for copy in plane_copies:
        copy.start()
    others = plane_recv.at[pl.ds(0, in_plane - 1)]
    pltpu.make_async_copy(others, others, norm_sems.at[1]).wait()
    mine = jnp.sum(plane_recv[...], axis=0)

    axis_send[...] = mine
    own_copy = pltpu.make_async_copy(axis_send, axis_recv.at[my_plane], norm_sems.at[4])
    own_copy.start()
    axis_copies = [
        pltpu.make_async_remote_copy(
            src_ref=axis_send,
            dst_ref=axis_recv.at[my_plane],
            send_sem=norm_sems.at[2],
            recv_sem=norm_sems.at[3],
            device_id=axis_target(offset),
            device_id_type=MESH,
        )
        for offset in axis_steps
    ]
    for copy in axis_copies:
        copy.start()
    wait_sends(ITERS - 1)
    out_copy.wait()
    pltpu.make_async_copy(others, others, norm_sems.at[0]).wait()
    others = axis_recv.at[pl.ds(0, planes - 1)]
    pltpu.make_async_copy(others, others, norm_sems.at[3]).wait()
    own_copy.wait()
    pltpu.make_async_copy(others, others, norm_sems.at[2]).wait()


def kernel(shape, groups, k_all, rows, *refs):
    heights = (CUT, CUT, k_all, k_all) + 4 * (2 * k_all // groups,)
    units = rows // CUT
    specs = [pltpu.ACC(unit)((height, CUT), jnp.float32) for unit in range(units) for height in heights]

    def body(*accs):
        per_unit = [accs[unit * len(heights) : (unit + 1) * len(heights)] for unit in range(units)]
        steps(per_unit, shape, *refs)

    pl.run_scoped(body, *specs)


def on_device(n_patch, n_sub, planes, sources, diag_coef, tiles, tile_cols, send_rows, recv_rows, bounds):
    rows = diag_coef.shape[0]
    k_all = sources.shape[0]
    blk_rows, per_row, tile, _ = tiles.shape
    dirs = send_rows.shape[1]
    n_blocks = 2 * blk_rows
    f32, bf16 = jnp.float32, jnp.bfloat16
    hbm = pl.BlockSpec(memory_space=pltpu.HBM)
    field = pltpu.VMEM((k_all, rows), f32)
    in_plane = n_patch // planes * n_sub
    x, sums = pl.pallas_call(
        functools.partial(kernel, (n_patch, n_sub, planes), GROUPS, k_all, rows),
        out_shape=(jax.ShapeDtypeStruct((rows, k_all), f32), jax.ShapeDtypeStruct((planes, 1, k_all), f32)),
        in_specs=[hbm] * 7,
        out_specs=(hbm, hbm),
        scratch_shapes=[
            pltpu.VMEM(sources.shape[::-1], jnp.int32),
            pltpu.VMEM((blk_rows, tile), f32),
            pltpu.SMEM(tile_cols.shape, jnp.int32),
            pltpu.VMEM(send_rows.shape[1:], jnp.int32),
            pltpu.VMEM(recv_rows.shape, jnp.int32),
            pltpu.SMEM(bounds.shape, f32),
            pltpu.VMEM(tiles.shape, f32),
            pltpu.VMEM((n_blocks, 2 * rows, tile), bf16),
            pltpu.VMEM((rows, rows), bf16),
            pltpu.VMEM((2 * tile, per_row * tile), bf16),
            pltpu.VMEM((2 * rows, 2 * rows), bf16),
            pltpu.VMEM((2 * rows, 2 * rows), bf16),
            pltpu.VMEM((2 * k_all, 2 * rows), bf16),
            field,
            field,
            field,
            field,
            field,
            field,
            field,
            field,
            pltpu.VMEM((2 * ITERS, 8, rows), f32),
            pltpu.VMEM((ITERS, dirs, k_all, tile), f32),
            pltpu.VMEM((ITERS, dirs, k_all, tile), f32),
            pltpu.VMEM((1, k_all), f32),
            pltpu.VMEM((in_plane, 1, k_all), f32),
            pltpu.VMEM((1, k_all), f32),
            pltpu.SemaphoreType.DMA((7,)),
            pltpu.SemaphoreType.DMA((2, GROUPS)),
            pltpu.SemaphoreType.DMA((2, GROUPS)),
            pltpu.SemaphoreType.DMA((5,)),
            pltpu.VMEM((rows, k_all), f32),
            pltpu.SemaphoreType.DMA,
            pltpu.SemaphoreType.REGULAR((2,)),
            pltpu.VMEM((8, rows), f32),
        ],
        compiler_params=pltpu.CompilerParams(
            collective_id=0, has_side_effects=True, vmem_limit_bytes=67_043_328
        ),
    )(
        sources.T,
        diag_coef.reshape(blk_rows, tile),
        tile_cols,
        send_rows[0],
        recv_rows,
        bounds,
        tiles,
    )
    return settle(x, sums)


def settle_kernel(x_in, sums_in, x_out, norm_out, x_buf, sums_buf, norm_buf, sems):
    read_sums = pltpu.make_async_copy(sums_in, sums_buf, sems.at[0])
    read_x = pltpu.make_async_copy(x_in, x_buf, sems.at[1])
    write_norm = pltpu.make_async_copy(norm_buf, norm_out, sems.at[0])
    write_x = pltpu.make_async_copy(x_buf, x_out, sems.at[1])
    read_sums.start()
    read_x.start()
    read_sums.wait()
    norm_buf[...] = jnp.sqrt(jnp.sum(sums_buf[...], axis=0))
    write_norm.start()
    read_x.wait()
    write_x.start()
    write_norm.wait()
    write_x.wait()


def settle(x, sums):
    hbm = pl.BlockSpec(memory_space=pl.ANY)
    norm_shape = jax.ShapeDtypeStruct(sums.shape[1:], sums.dtype)
    x, norm = pl.pallas_call(
        settle_kernel,
        out_shape=(jax.ShapeDtypeStruct(x.shape, x.dtype), norm_shape),
        in_specs=[hbm] * 2,
        out_specs=(hbm, hbm),
        scratch_shapes=[
            pltpu.VMEM(x.shape, x.dtype),
            pltpu.VMEM(sums.shape, sums.dtype),
            pltpu.VMEM(norm_shape.shape, norm_shape.dtype),
            pltpu.SemaphoreType.DMA((2,)),
        ],
        compiler_params=pltpu.CompilerParams(vmem_limit_bytes=67_043_328),
    )(x, sums)
    return x, norm[0]


def solution(mesh):
    n_patch, n_sub = mesh.shape["patch"], mesh.shape["sub"]
    both = ("patch", "sub")
    return jax.shard_map(
        functools.partial(on_device, n_patch, n_sub, PLANES),
        mesh=mesh,
        in_specs=(
            P(),
            P(both),
            P(both, None, None, None),
            P(both, None),
            P(both, None, None),
            P(both, None),
            P(),
        ),
        out_specs=(P(both, None), P()),
        check_vma=False,
    )
```

```python
import functools

import jax
import jax.numpy as jnp
from jax import lax
from jax.experimental import pallas as pl
from jax.experimental.pallas import tpu as pltpu
from jax.sharding import PartitionSpec as P

MESH = pl.DeviceIdType.MESH
ITERS = 8
GROUPS = 4
PLANES = 8
CUT = 256

def split(value):
    high = value.astype(jnp.bfloat16)
    low = (value - high.astype(jnp.float32)).astype(jnp.bfloat16)
    return high, low


def one_hot(equal):
    return jnp.where(equal, 1.0, 0.0).astype(jnp.bfloat16)


def steps(
    accs,
    shape,
    src_hbm,
    diag_hbm,
    cols_hbm,
    send_hbm,
    recv_hbm,
    bounds_hbm,
    tiles_hbm,
    x_out,
    axis_recv,
    src_lanes,
    diag,
    cols,
    send_rows,
    recv_rows,
    bounds,
    tiles,
    place,
    pick,
    tile_pair,
    w_high,
    w_low,
    ext,
    b_own,
    r_own,
    d_own,
    x_own,
    r_pack,
    d_pack,
    x_pack,
    part,
    coef,
    send_buf,
    recv_buf,
    plane_send,
    plane_recv,
    axis_send,
    copy_sems,
    send_sem,
    recv_sem,
    norm_sems,
    out_buf,
    hello_sems,
    diag_rows,
):
    n_patch, n_sub, planes = shape
    units = range(len(accs))
    build_accs = [unit_accs[0:2] for unit_accs in accs]
    field_accs = [unit_accs[2:4] for unit_accs in accs]
    halo_accs = [unit_accs[4:12] for unit_accs in accs]

    def feed(unit, weights, jobs, transpose=False):
        pltpu.matmul_push_rhs(weights, staging_register=0, mxu_index=unit, transpose=transpose)
        for i, (acc, operand) in enumerate(jobs):
            pltpu.matmul_acc_lhs(acc, operand, load_staged_rhs=0 if i == 0 else None)

    f32 = jnp.float32
    k_all, rows = b_own.shape
    per_row = tiles.shape[1]
    blk_rows = tiles.shape[0]
    tile = tiles.shape[2]
    n_blocks = place.shape[0]
    halo_blocks = n_blocks - blk_rows
    dirs = 4
    groups = recv_sem.shape[1]
    k_group = k_all // groups

    p = lax.axis_index("patch")
    s = lax.axis_index("sub")
    plane = n_patch // planes
    in_plane = plane * n_sub
    my_plane = lax.div(p, plane)
    my_patch = lax.rem(p, plane)
    my_slot = my_patch * n_sub + s

    p_next = lax.rem(p + 1, n_patch)
    p_prev = lax.rem(p + n_patch - 1, n_patch)
    s_next = lax.rem(s + 1, n_sub)
    s_prev = lax.rem(s + n_sub - 1, n_sub)
    targets = ((p_prev, s), (p_next, s), (p, s_prev), (p, s_next))
    lands = (1, 0, 3, 2)

    def plane_target(step):
        patch_step, sub_step = step
        return (my_plane * plane + lax.rem(my_patch + patch_step, plane), lax.rem(s + sub_step, n_sub))

    def ring(step, size):
        return min(step, size - step)

    plane_steps = [(a, b) for a in range(plane) for b in range(n_sub) if a or b]
    plane_steps.sort(key=lambda step: -(ring(step[0], plane) / 2 + ring(step[1], n_sub)))
    axis_steps = sorted(range(1, planes), key=lambda step: -ring(step, planes))

    def axis_target(offset):
        return (lax.rem(my_plane + offset, planes) * plane + my_patch, s)

    loads = [
        pltpu.make_async_copy(source, target, copy_sems.at[i])
        for i, (source, target) in enumerate(
            (
                (src_hbm, src_lanes),
                (send_hbm, send_rows),
                (bounds_hbm, bounds),
                (recv_hbm, recv_rows),
                (cols_hbm, cols),
                (diag_hbm, diag),
                (tiles_hbm, tiles),
            )
        )
    ]
    for load in loads:
        load.start()
    barrier = pltpu.get_barrier_semaphore()
    greeted = 0
    for target in targets:
        pl.semaphore_signal(barrier, inc=1, device_id=target, device_id_type=MESH)
        greeted += 1
    for offset in (1, planes - 1):
        pl.semaphore_signal(barrier, inc=1, device_id=axis_target(offset), device_id_type=MESH)
        greeted += 1

    eye = lax.broadcasted_iota(jnp.int32, (tile, tile), 0) == lax.broadcasted_iota(jnp.int32, (tile, tile), 1)
    row_id = lax.broadcasted_iota(jnp.int32, (rows, tile), 0)
    for c in range(n_blocks):
        if c < blk_rows:
            place[c] = jnp.zeros(place.shape[1:], jnp.bfloat16)
            place[c, c * tile : (c + 1) * tile, :] = one_hot(eye)
        else:
            place[c, 0:rows, :] = jnp.zeros((rows, tile), jnp.bfloat16)

    for load in loads[:3]:
        load.wait()

    lower = jnp.full((8, rows), bounds[0], f32)
    upper = jnp.full((8, rows), bounds[1], f32)
    centre = (lower + upper) / 2.0
    inverse = (1.0 / centre)[0:1]

    first = (p * n_sub + s) * rows
    src = jnp.transpose(src_lanes[...])
    lane = lax.broadcasted_iota(jnp.int32, (1, tile), 1) + first

    def count(start, size, ids):
        sums = [jnp.zeros((size, tile), f32) for _ in ids]
        for source in range(src.shape[1]):
            wide = jnp.broadcast_to(src[start : start + size, source : source + 1], (size, tile))
            sums = [jnp.where(wide == v, a + 1.0, a) for v, a in zip(ids, sums)]
        return sums

    def send(step, group, j):
        rows_of = pl.ds(group * k_group, k_group)
        return pltpu.make_async_remote_copy(
            src_ref=send_buf.at[step, j, rows_of, :],
            dst_ref=recv_buf.at[step, lands[j], rows_of, :],
            send_sem=send_sem.at[lax.rem(step, 2)],
            recv_sem=recv_sem.at[lax.rem(step, 2), group],
            device_id=targets[j],
            device_id_type=MESH,
        )

    def start_sends(step, group, which=(0, 1, 2, 3)):
        for j in which:
            send(step, group, j).start()

    def wait_recvs(step, group):
        parts = recv_buf.at[step, :, pl.ds(group * k_group, k_group), :]
        pltpu.make_async_copy(parts, parts, recv_sem.at[lax.rem(step, 2), group]).wait()

    def wait_sends(step):
        whole = send_buf.at[step]
        pltpu.make_async_copy(whole, whole, send_sem.at[lax.rem(step, 2)]).wait()

    for group in range(groups):
        at = slice(group * k_group, (group + 1) * k_group)
        ids = [send_rows[j : j + 1, :] + first for j in range(dirs)]
        for j, total in enumerate(count(group * k_group, k_group, ids)):
            scaled = total * inverse[:, :tile]
            send_buf[0, j, at, :] = scaled
            r_pack[at, j * tile : (j + 1) * tile] = total
            d_pack[at, j * tile : (j + 1) * tile] = scaled
            x_pack[at, j * tile : (j + 1) * tile] = scaled

    loads[3].wait()
    for c in range(blk_rows, n_blocks):
        h = c - blk_rows
        place[c, rows : 2 * rows, :] = one_hot(recv_rows[:, h * tile : (h + 1) * tile] == row_id)
    for j in range(dirs):
        pick[:, j * tile : (j + 1) * tile] = one_hot(send_rows[j : j + 1, :] == row_id)

    for load in loads[4:]:
        load.wait()

    def build_rows(b):
        for n in range(per_row):
            high, low = split(tiles[b, n])
            tile_pair[0:tile, n * tile : (n + 1) * tile] = high
            tile_pair[tile : 2 * tile, n * tile : (n + 1) * tile] = low
        starts = [[(u + len(units) * i) * CUT for i in range(2)] for u in units]
        for depth in range(0, per_row * tile, CUT):
            for u in units:
                jobs = []
                for acc, start in zip(build_accs[u], starts[u]):
                    spots = [place[cols[b, n], start : start + CUT, :] for n in range(depth // tile, (depth + CUT) // tile)]
                    jobs.append((acc, jnp.concatenate(spots, axis=1)))
                feed(u, tile_pair[:, depth : depth + CUT], jobs, transpose=True)
        for i in range(2):
            for u in units:
                start = starts[u][i]
                both = pltpu.matmul_pop(build_accs[u][i])
                block = both[:, :tile] + both[:, tile:]
                high, low = split(block)
                w_high[start : start + CUT, b * tile : (b + 1) * tile] = high
                w_low[start : start + CUT, b * tile : (b + 1) * tile] = low

        share = k_all // blk_rows
        at = slice(b * share, (b + 1) * share)
        low_at = slice(k_all + b * share, k_all + (b + 1) * share)
        for i, total in enumerate(count(b * share, share, [lane + i * tile for i in range(blk_rows)])):
            cols_at = slice(i * tile, (i + 1) * tile)
            b_own[at, cols_at] = total
            r_own[at, cols_at] = total
            scaled = total * inverse[:, :tile]
            d_own[at, cols_at] = scaled
            x_own[at, cols_at] = scaled
            high, low = split(scaled)
            ext[at, cols_at] = high
            ext[low_at, cols_at] = low

    build_rows(0)

    pl.semaphore_wait(barrier, greeted)
    for group in range(groups):
        start_sends(0, group)

    def hello(distance):
        for offset in (distance, planes - distance):
            pl.semaphore_signal(
                hello_sems.at[distance - 1], inc=1, device_id=axis_target(offset), device_id_type=MESH
            )

    hello(1)

    for b in range(1, blk_rows):
        build_rows(b)

    half_width = (upper - lower) / 2.0
    ratio = centre / half_width
    damping = 1.0 / ratio
    for step in range(ITERS - 1):
        following = 1.0 / (2.0 * ratio - damping)
        coef[2 * step] = following * damping
        coef[2 * step + 1] = 2.0 * following / half_width
        damping = following

    for start in range(0, 2 * rows, CUT):
        chunk_rows = slice(start, start + CUT)
        for depth in range(0, rows, CUT):
            for u in units:
                jobs = [(acc, w[chunk_rows, depth : depth + CUT]) for acc, w in zip(build_accs[u], (w_high, w_low))]
                feed(u, pick[depth : depth + CUT, u * CUT : (u + 1) * CUT], jobs)
        for i, w in enumerate((w_high, w_low)):
            for u in units:
                at = slice(rows + u * CUT, rows + (u + 1) * CUT)
                w[chunk_rows, at] = pltpu.matmul_pop(build_accs[u][i]).astype(jnp.bfloat16)

    own, got = slice(0, rows), slice(rows, 2 * rows)

    def products(depth_all, first_col):
        for depth in range(0, depth_all, CUT):
            at = slice(depth, depth + CUT)
            for weights, lows in ((w_high, True), (w_low, False)):
                for u in units:
                    top, bottom = field_accs[u]
                    jobs = [(top, ext[0:k_all, at])]
                    if lows:
                        jobs.append((bottom, ext[k_all : 2 * k_all, at]))
                    feed(u, weights[at, first_col + u * CUT : first_col + (u + 1) * CUT], jobs)
        return [pltpu.matmul_pop(top) + pltpu.matmul_pop(bottom) for top, bottom in field_accs]

    on_own = jnp.concatenate([diag[b : b + 1, :] for b in range(blk_rows)], axis=1)
    line = lax.broadcasted_iota(jnp.int32, (k_group, rows), 0)
    rest, thirds = on_own, jnp.zeros((k_group, rows), f32)
    for i in range(3):
        third = rest.astype(jnp.bfloat16).astype(f32)
        thirds = jnp.where(line == i, third, thirds)
        rest = rest - third
    thirds = thirds.astype(jnp.bfloat16)
    for depth in range(0, rows, CUT):
        for u in units:
            jobs = [(halo_accs[u][0], thirds[:, depth : depth + CUT])]
            feed(u, pick[depth : depth + CUT, u * CUT : (u + 1) * CUT], jobs)
    on_pack = [jnp.sum(pltpu.matmul_pop(halo_accs[u][0])[0:8], axis=0, keepdims=True) for u in units]
    diag_rows[0:1, :] = on_own
    diag_rows[1:2, :] = jnp.concatenate(on_pack, axis=1)

    def packed_part():
        for u, product in enumerate(products(rows, rows)):
            at = slice(u * CUT, (u + 1) * CUT)
            part[:, at] = product + diag_rows[1:2, at] * d_pack[:, at]

    packed_part()
    pl.semaphore_wait(hello_sems.at[0], 2)
    hello(2)

    def take_halo(step, group):
        at = pl.ds(group * k_group, k_group)
        wait_recvs(step, group)
        halo = jnp.concatenate([recv_buf[step, j, at, :] for j in range(dirs)], axis=1)
        return split(halo)

    def stage(first_col, half):
        for i, weights in enumerate((w_high, w_low)):
            for u in units:
                tile_rows = slice(rows + u * CUT, rows + (u + 1) * CUT)
                tile_cols = slice(first_col + half * CUT, first_col + (half + 1) * CUT)
                pltpu.matmul_push_rhs(weights[tile_rows, tile_cols], staging_register=i, mxu_index=u)

    def multiply(high, low, half, slot):
        for operand, part_of, load in ((high, 0, 0), (low, 1, None), (high, 0, 1)):
            for u in units:
                acc = halo_accs[u][4 * slot + 2 * half + part_of]
                pltpu.matmul_acc_lhs(acc, operand[:, u * CUT : (u + 1) * CUT], load_staged_rhs=load)

    def collect(half, slot):
        i = 4 * slot + 2 * half
        return sum(pltpu.matmul_pop(halo_accs[u][i + 1]) for u in units) + sum(
            pltpu.matmul_pop(halo_accs[u][i]) for u in units
        )

    def iteration(step, carry):
        alpha = coef[2 * step][0:1]
        beta = coef[2 * step + 1][0:1]
        last = (step == ITERS - 2).astype(f32)

        def finish(group, half):
            at = slice(group * k_group, (group + 1) * k_group)
            lanes = slice(half * CUT, (half + 1) * CUT)
            r_part = r_pack[at, lanes] - part[at, lanes]
            d_part = alpha[:, lanes] * d_pack[at, lanes] + beta[:, lanes] * r_part
            x_old = x_pack[at, lanes]
            coupled = collect(half, group % 2)
            change = beta[:, lanes] * coupled
            going = (d_part + last * x_old) - change
            which = range(half * CUT // tile, (half + 1) * CUT // tile)
            for i, j in enumerate(which):
                send_buf[step + 1, j, at, :] = going[:, i * tile : (i + 1) * tile]
            start_sends(step + 1, group, which)
            d_new = d_part - change
            r_pack[at, lanes] = r_part - coupled
            d_pack[at, lanes] = d_new
            x_pack[at, lanes] = x_old + d_new

        stage(rows, 0)
        for group in range(groups):
            g0 = group * k_group
            high, low = take_halo(step, group)
            multiply(high, low, 0, group % 2)
            stage(rows, 1)
            multiply(high, low, 1, group % 2)
            if group + 1 < groups:
                stage(rows, 0)
            finish(group, 0)
            if group > 0:
                finish(group - 1, 1)
            ext[g0 : g0 + k_group, got] = high
            ext[k_all + g0 : k_all + g0 + k_group, got] = low
        finish(groups - 1, 1)
        wait_sends(step)
        for u, product in enumerate(products(2 * rows, 0)):
            at = slice(u * CUT, (u + 1) * CUT)
            r_new = r_own[:, at] - (product + diag_rows[0:1, at] * d_own[:, at])
            d_new = alpha[:, at] * d_own[:, at] + beta[:, at] * r_new
            r_own[:, at] = r_new
            d_own[:, at] = d_new
        for start in range(0, rows, CUT):
            at = slice(start, start + CUT)
            d_new = d_own[:, at]
            x_old = x_own[:, at]
            x_own[:, at] = x_old + d_new
            high, low = split(d_new + last * x_old)
            ext[0:k_all, at] = high
            ext[k_all : 2 * k_all, at] = low
        packed_part()
        return carry

    lax.fori_loop(0, ITERS - 1, iteration, 0)

    for u, product in enumerate(products(rows, 0)):
        at = slice(u * CUT, (u + 1) * CUT)
        r_own[:, at] = b_own[:, at] - (product + diag_rows[0:1, at] * x_own[:, at])
    for i in range(blk_rows):
        out_buf[i * tile : (i + 1) * tile, :] = jnp.transpose(x_own[:, i * tile : (i + 1) * tile])

    out_copy = pltpu.make_async_copy(out_buf, x_out, copy_sems.at[5])
    out_copy.start()
    pl.semaphore_wait(hello_sems.at[1], 2)

    def square(group):
        at = slice(group * k_group, (group + 1) * k_group)
        total = jnp.zeros((k_group, tile), f32)
        for half in range(2):
            final = r_own[at, half * CUT : (half + 1) * CUT] - collect(half, group % 2)
            final = final * final
            for i in range(CUT // tile):
                total = total + final[:, i * tile : (i + 1) * tile]
        return total

    squares = []
    stage(0, 0)
    for group in range(groups):
        high, low = take_halo(ITERS - 1, group)
        multiply(high, low, 0, group % 2)
        stage(0, 1)
        multiply(high, low, 1, group % 2)
        if group > 0:
            squares.append(square(group - 1))
        if group + 1 < groups:
            stage(0, 0)
    squares.append(square(groups - 1))
    squares = jnp.transpose(jnp.concatenate(squares, axis=0))
    mine = jnp.sum(squares, axis=0, keepdims=True)

    plane_send[...] = mine
    plane_recv[my_slot] = mine
    plane_copies = [
        pltpu.make_async_remote_copy(
            src_ref=plane_send,
            dst_ref=plane_recv.at[my_slot],
            send_sem=copy_sems.at[0],
            recv_sem=norm_sems.at[0],
            device_id=plane_target(step),
            device_id_type=MESH,
        )
        for step in plane_steps
    ]
    for copy in plane_copies:
        copy.start()
    others = plane_recv.at[pl.ds(0, in_plane - 1)]
    pltpu.make_async_copy(others, others, norm_sems.at[0]).wait()
    mine = jnp.sum(plane_recv[...], axis=0)

    axis_send[...] = mine
    own_copy = pltpu.make_async_copy(axis_send, axis_recv.at[my_plane], copy_sems.at[4])
    own_copy.start()
    axis_copies = [
        pltpu.make_async_remote_copy(
            src_ref=axis_send,
            dst_ref=axis_recv.at[my_plane],
            send_sem=copy_sems.at[2],
            recv_sem=norm_sems.at[1],
            device_id=axis_target(offset),
            device_id_type=MESH,
        )
        for offset in axis_steps
    ]
    for copy in axis_copies:
        copy.start()
    wait_sends(ITERS - 1)
    out_copy.wait()
    pltpu.make_async_copy(others, others, copy_sems.at[0]).wait()
    others = axis_recv.at[pl.ds(0, planes - 1)]
    pltpu.make_async_copy(others, others, norm_sems.at[1]).wait()
    own_copy.wait()
    pltpu.make_async_copy(others, others, copy_sems.at[2]).wait()


def kernel(shape, groups, k_all, rows, *refs):
    heights = (CUT, CUT, k_all, k_all) + 8 * (k_all // groups,)
    units = rows // CUT
    specs = [pltpu.ACC(unit)((height, CUT), jnp.float32) for unit in range(units) for height in heights]

    def body(*accs):
        per_unit = [accs[unit * len(heights) : (unit + 1) * len(heights)] for unit in range(units)]
        steps(per_unit, shape, *refs)

    pl.run_scoped(body, *specs)


def on_device(n_patch, n_sub, planes, sources, diag_coef, tiles, tile_cols, send_rows, recv_rows, bounds):
    rows = diag_coef.shape[0]
    k_all = sources.shape[0]
    blk_rows, per_row, tile, _ = tiles.shape
    dirs = send_rows.shape[1]
    n_blocks = 2 * blk_rows
    f32, bf16 = jnp.float32, jnp.bfloat16
    hbm = pl.BlockSpec(memory_space=pltpu.HBM)
    field = pltpu.VMEM((k_all, rows), f32)
    in_plane = n_patch // planes * n_sub
    x, sums = pl.pallas_call(
        functools.partial(kernel, (n_patch, n_sub, planes), GROUPS, k_all, rows),
        out_shape=(jax.ShapeDtypeStruct((rows, k_all), f32), jax.ShapeDtypeStruct((planes, 1, k_all), f32)),
        in_specs=[hbm] * 7,
        out_specs=(hbm, hbm),
        scratch_shapes=[
            pltpu.VMEM(sources.shape[::-1], jnp.int32),
            pltpu.VMEM((blk_rows, tile), f32),
            pltpu.SMEM(tile_cols.shape, jnp.int32),
            pltpu.VMEM(send_rows.shape[1:], jnp.int32),
            pltpu.VMEM(recv_rows.shape, jnp.int32),
            pltpu.SMEM(bounds.shape, f32),
            pltpu.VMEM(tiles.shape, f32),
            pltpu.VMEM((n_blocks, 2 * rows, tile), bf16),
            pltpu.VMEM((rows, rows), bf16),
            pltpu.VMEM((2 * tile, per_row * tile), bf16),
            pltpu.VMEM((2 * rows, 2 * rows), bf16),
            pltpu.VMEM((2 * rows, 2 * rows), bf16),
            pltpu.VMEM((2 * k_all, 2 * rows), bf16),
            field,
            field,
            field,
            field,
            field,
            field,
            field,
            field,
            pltpu.VMEM((2 * ITERS, 8, rows), f32),
            pltpu.VMEM((ITERS, dirs, k_all, tile), f32),
            pltpu.VMEM((ITERS, dirs, k_all, tile), f32),
            pltpu.VMEM((1, k_all), f32),
            pltpu.VMEM((in_plane, 1, k_all), f32),
            pltpu.VMEM((1, k_all), f32),
            pltpu.SemaphoreType.DMA((7,)),
            pltpu.SemaphoreType.DMA((2,)),
            pltpu.SemaphoreType.DMA((2, GROUPS)),
            pltpu.SemaphoreType.DMA((2,)),
            pltpu.VMEM((rows, k_all), f32),
            pltpu.SemaphoreType.REGULAR((2,)),
            pltpu.VMEM((8, rows), f32),
        ],
        compiler_params=pltpu.CompilerParams(
            collective_id=0, has_side_effects=True, vmem_limit_bytes=67_043_328
        ),
    )(
        sources.T,
        diag_coef.reshape(blk_rows, tile),
        tile_cols,
        send_rows[0],
        recv_rows,
        bounds,
        tiles,
    )
    return settle(x, sums)


def settle_kernel(x_in, sums_in, x_out, norm_out, x_buf, sums_buf, norm_buf, sems):
    read_sums = pltpu.make_async_copy(sums_in, sums_buf, sems.at[0])
    read_x = pltpu.make_async_copy(x_in, x_buf, sems.at[1])
    write_norm = pltpu.make_async_copy(norm_buf, norm_out, sems.at[0])
    write_x = pltpu.make_async_copy(x_buf, x_out, sems.at[1])
    read_sums.start()
    read_x.start()
    read_sums.wait()
    norm_buf[...] = jnp.sqrt(jnp.sum(sums_buf[...], axis=0))
    write_norm.start()
    read_x.wait()
    write_x.start()
    write_norm.wait()
    write_x.wait()


def settle(x, sums):
    hbm = pl.BlockSpec(memory_space=pl.ANY)
    norm_shape = jax.ShapeDtypeStruct(sums.shape[1:], sums.dtype)
    x, norm = pl.pallas_call(
        settle_kernel,
        out_shape=(jax.ShapeDtypeStruct(x.shape, x.dtype), norm_shape),
        in_specs=[hbm] * 2,
        out_specs=(hbm, hbm),
        scratch_shapes=[
            pltpu.VMEM(x.shape, x.dtype),
            pltpu.VMEM(sums.shape, sums.dtype),
            pltpu.VMEM(norm_shape.shape, norm_shape.dtype),
            pltpu.SemaphoreType.DMA((2,)),
        ],
        compiler_params=pltpu.CompilerParams(vmem_limit_bytes=67_043_328),
    )(x, sums)
    return x, norm[0]


def solution(mesh):
    n_patch, n_sub = mesh.shape["patch"], mesh.shape["sub"]
    both = ("patch", "sub")
    return jax.shard_map(
        functools.partial(on_device, n_patch, n_sub, PLANES),
        mesh=mesh,
        in_specs=(
            P(),
            P(both),
            P(both, None, None, None),
            P(both, None),
            P(both, None, None),
            P(both, None),
            P(),
        ),
        out_specs=(P(both, None), P()),
        check_vma=False,
    )
```

```python
import functools

import jax
import jax.numpy as jnp
from jax import lax
from jax.experimental import pallas as pl
from jax.experimental.pallas import tpu as pltpu
from jax.sharding import PartitionSpec as P

MESH = pl.DeviceIdType.MESH
ITERS = 8
GROUPS = 4
PLANES = 8
CUT = 256

def split(value):
    high = value.astype(jnp.bfloat16)
    low = (value - high.astype(jnp.float32)).astype(jnp.bfloat16)
    return high, low


def one_hot(equal):
    return jnp.where(equal, 1.0, 0.0).astype(jnp.bfloat16)


def steps(
    accs,
    shape,
    src_hbm,
    diag_hbm,
    cols_hbm,
    send_hbm,
    recv_hbm,
    bounds_hbm,
    tiles_hbm,
    x_out,
    axis_recv,
    src_lanes,
    diag,
    cols,
    send_rows,
    recv_rows,
    bounds,
    tiles,
    place,
    pick,
    tile_pair,
    w_high,
    w_low,
    ext,
    b_own,
    r_own,
    d_own,
    x_own,
    r_pack,
    d_pack,
    x_pack,
    part,
    coef,
    send_buf,
    recv_buf,
    plane_send,
    plane_recv,
    axis_send,
    copy_sems,
    send_sem,
    recv_sem,
    norm_sems,
    out_buf,
    hello_sems,
    diag_rows,
):
    n_patch, n_sub, planes = shape
    units = range(len(accs))
    build_accs = [unit_accs[0:2] for unit_accs in accs]
    field_accs = [unit_accs[2:4] for unit_accs in accs]
    halo_accs = [unit_accs[4:12] for unit_accs in accs]

    def feed(unit, weights, jobs, transpose=False):
        pltpu.matmul_push_rhs(weights, staging_register=0, mxu_index=unit, transpose=transpose)
        for i, (acc, operand) in enumerate(jobs):
            pltpu.matmul_acc_lhs(acc, operand, load_staged_rhs=0 if i == 0 else None)

    f32 = jnp.float32
    k_all, rows = b_own.shape
    per_row = tiles.shape[1]
    blk_rows = tiles.shape[0]
    tile = tiles.shape[2]
    n_blocks = place.shape[0]
    halo_blocks = n_blocks - blk_rows
    dirs = 4
    groups = recv_sem.shape[1]
    k_group = k_all // groups

    p = lax.axis_index("patch")
    s = lax.axis_index("sub")
    plane = n_patch // planes
    in_plane = plane * n_sub
    my_plane = lax.div(p, plane)
    my_patch = lax.rem(p, plane)
    my_slot = my_patch * n_sub + s

    p_next = lax.rem(p + 1, n_patch)
    p_prev = lax.rem(p + n_patch - 1, n_patch)
    s_next = lax.rem(s + 1, n_sub)
    s_prev = lax.rem(s + n_sub - 1, n_sub)
    targets = ((p_prev, s), (p_next, s), (p, s_prev), (p, s_next))
    lands = (1, 0, 3, 2)

    def plane_target(step):
        patch_step, sub_step = step
        return (my_plane * plane + lax.rem(my_patch + patch_step, plane), lax.rem(s + sub_step, n_sub))

    def ring(step, size):
        return min(step, size - step)

    plane_steps = [(a, b) for a in range(plane) for b in range(n_sub) if a or b]
    plane_steps.sort(key=lambda step: -(ring(step[0], plane) / 2 + ring(step[1], n_sub)))
    axis_steps = sorted(range(1, planes), key=lambda step: -ring(step, planes))

    def axis_target(offset):
        return (lax.rem(my_plane + offset, planes) * plane + my_patch, s)

    loads = [
        pltpu.make_async_copy(source, target, copy_sems.at[i])
        for i, (source, target) in enumerate(
            (
                (src_hbm, src_lanes),
                (send_hbm, send_rows),
                (bounds_hbm, bounds),
                (recv_hbm, recv_rows),
                (cols_hbm, cols),
                (diag_hbm, diag),
                (tiles_hbm, tiles),
            )
        )
    ]
    barrier = pltpu.get_barrier_semaphore()
    greeted = 0
    for target in targets[:2]:
        pl.semaphore_signal(barrier, inc=1, device_id=target, device_id_type=MESH)
        greeted += 1
    for load in loads:
        load.start()
    for target in targets[2:]:
        pl.semaphore_signal(barrier, inc=1, device_id=target, device_id_type=MESH)
        greeted += 1
    for offset in (1, planes - 1):
        pl.semaphore_signal(barrier, inc=1, device_id=axis_target(offset), device_id_type=MESH)
        greeted += 1

    eye = lax.broadcasted_iota(jnp.int32, (tile, tile), 0) == lax.broadcasted_iota(jnp.int32, (tile, tile), 1)
    row_id = lax.broadcasted_iota(jnp.int32, (rows, tile), 0)
    for c in range(n_blocks):
        if c < blk_rows:
            place[c] = jnp.zeros(place.shape[1:], jnp.bfloat16)
            place[c, c * tile : (c + 1) * tile, :] = one_hot(eye)
        else:
            place[c, 0:rows, :] = jnp.zeros((rows, tile), jnp.bfloat16)

    for load in loads[:3]:
        load.wait()

    lower = jnp.full((8, rows), bounds[0], f32)
    upper = jnp.full((8, rows), bounds[1], f32)
    centre = (lower + upper) / 2.0
    inverse = (1.0 / centre)[0:1]

    first = (p * n_sub + s) * rows
    src = jnp.transpose(src_lanes[...])
    lane = lax.broadcasted_iota(jnp.int32, (1, tile), 1) + first

    def count(start, size, ids):
        sums = [jnp.zeros((size, tile), f32) for _ in ids]
        for source in range(src.shape[1]):
            wide = jnp.broadcast_to(src[start : start + size, source : source + 1], (size, tile))
            sums = [jnp.where(wide == v, a + 1.0, a) for v, a in zip(ids, sums)]
        return sums

    def send(step, group, j):
        rows_of = pl.ds(group * k_group, k_group)
        return pltpu.make_async_remote_copy(
            src_ref=send_buf.at[step, j, rows_of, :],
            dst_ref=recv_buf.at[step, lands[j], rows_of, :],
            send_sem=send_sem.at[lax.rem(step, 2)],
            recv_sem=recv_sem.at[lax.rem(step, 2), group],
            device_id=targets[j],
            device_id_type=MESH,
        )

    def start_sends(step, group, which=(0, 1, 2, 3)):
        for j in which:
            send(step, group, j).start()

    def wait_recvs(step, group):
        parts = recv_buf.at[step, :, pl.ds(group * k_group, k_group), :]
        pltpu.make_async_copy(parts, parts, recv_sem.at[lax.rem(step, 2), group]).wait()

    def wait_sends(step):
        whole = send_buf.at[step]
        pltpu.make_async_copy(whole, whole, send_sem.at[lax.rem(step, 2)]).wait()

    for group in range(groups):
        at = slice(group * k_group, (group + 1) * k_group)
        ids = [send_rows[j : j + 1, :] + first for j in range(dirs)]
        for j, total in enumerate(count(group * k_group, k_group, ids)):
            scaled = total * inverse[:, :tile]
            send_buf[0, j, at, :] = scaled
            r_pack[at, j * tile : (j + 1) * tile] = total
            d_pack[at, j * tile : (j + 1) * tile] = scaled
            x_pack[at, j * tile : (j + 1) * tile] = scaled

    loads[3].wait()
    for c in range(blk_rows, n_blocks):
        h = c - blk_rows
        place[c, rows : 2 * rows, :] = one_hot(recv_rows[:, h * tile : (h + 1) * tile] == row_id)
    for j in range(dirs):
        pick[:, j * tile : (j + 1) * tile] = one_hot(send_rows[j : j + 1, :] == row_id)

    for load in loads[4:]:
        load.wait()

    def build_rows(b):
        for n in range(per_row):
            high, low = split(tiles[b, n])
            tile_pair[0:tile, n * tile : (n + 1) * tile] = high
            tile_pair[tile : 2 * tile, n * tile : (n + 1) * tile] = low
        starts = [[(u + len(units) * i) * CUT for i in range(2)] for u in units]
        for depth in range(0, per_row * tile, CUT):
            for u in units:
                jobs = []
                for acc, start in zip(build_accs[u], starts[u]):
                    spots = [place[cols[b, n], start : start + CUT, :] for n in range(depth // tile, (depth + CUT) // tile)]
                    jobs.append((acc, jnp.concatenate(spots, axis=1)))
                feed(u, tile_pair[:, depth : depth + CUT], jobs, transpose=True)
        for i in range(2):
            for u in units:
                start = starts[u][i]
                both = pltpu.matmul_pop(build_accs[u][i])
                block = both[:, :tile] + both[:, tile:]
                high, low = split(block)
                w_high[start : start + CUT, b * tile : (b + 1) * tile] = high
                w_low[start : start + CUT, b * tile : (b + 1) * tile] = low

        share = k_all // blk_rows
        at = slice(b * share, (b + 1) * share)
        low_at = slice(k_all + b * share, k_all + (b + 1) * share)
        for i, total in enumerate(count(b * share, share, [lane + i * tile for i in range(blk_rows)])):
            cols_at = slice(i * tile, (i + 1) * tile)
            b_own[at, cols_at] = total
            r_own[at, cols_at] = total
            scaled = total * inverse[:, :tile]
            d_own[at, cols_at] = scaled
            x_own[at, cols_at] = scaled
            high, low = split(scaled)
            ext[at, cols_at] = high
            ext[low_at, cols_at] = low

    build_rows(0)

    pl.semaphore_wait(barrier, greeted)
    for group in range(groups):
        start_sends(0, group)

    def hello(distance):
        for offset in (distance, planes - distance):
            pl.semaphore_signal(
                hello_sems.at[distance - 1], inc=1, device_id=axis_target(offset), device_id_type=MESH
            )

    hello(1)

    for b in range(1, blk_rows):
        build_rows(b)

    half_width = (upper - lower) / 2.0
    ratio = centre / half_width
    damping = 1.0 / ratio
    for step in range(ITERS - 1):
        following = 1.0 / (2.0 * ratio - damping)
        coef[2 * step] = following * damping
        coef[2 * step + 1] = 2.0 * following / half_width
        damping = following

    for start in range(0, 2 * rows, CUT):
        chunk_rows = slice(start, start + CUT)
        for depth in range(0, rows, CUT):
            for u in units:
                jobs = [(acc, w[chunk_rows, depth : depth + CUT]) for acc, w in zip(build_accs[u], (w_high, w_low))]
                feed(u, pick[depth : depth + CUT, u * CUT : (u + 1) * CUT], jobs)
        for i, w in enumerate((w_high, w_low)):
            for u in units:
                at = slice(rows + u * CUT, rows + (u + 1) * CUT)
                w[chunk_rows, at] = pltpu.matmul_pop(build_accs[u][i]).astype(jnp.bfloat16)

    own, got = slice(0, rows), slice(rows, 2 * rows)

    def products(depth_all, first_col):
        for depth in range(0, depth_all, CUT):
            at = slice(depth, depth + CUT)
            for weights, lows in ((w_high, True), (w_low, False)):
                for u in units:
                    top, bottom = field_accs[u]
                    jobs = [(top, ext[0:k_all, at])]
                    if lows:
                        jobs.append((bottom, ext[k_all : 2 * k_all, at]))
                    feed(u, weights[at, first_col + u * CUT : first_col + (u + 1) * CUT], jobs)
        return [pltpu.matmul_pop(top) + pltpu.matmul_pop(bottom) for top, bottom in field_accs]

    on_own = jnp.concatenate([diag[b : b + 1, :] for b in range(blk_rows)], axis=1)
    line = lax.broadcasted_iota(jnp.int32, (k_group, rows), 0)
    rest, thirds = on_own, jnp.zeros((k_group, rows), f32)
    for i in range(3):
        third = rest.astype(jnp.bfloat16).astype(f32)
        thirds = jnp.where(line == i, third, thirds)
        rest = rest - third
    thirds = thirds.astype(jnp.bfloat16)
    for depth in range(0, rows, CUT):
        for u in units:
            jobs = [(halo_accs[u][0], thirds[:, depth : depth + CUT])]
            feed(u, pick[depth : depth + CUT, u * CUT : (u + 1) * CUT], jobs)
    on_pack = [jnp.sum(pltpu.matmul_pop(halo_accs[u][0])[0:8], axis=0, keepdims=True) for u in units]
    diag_rows[0:1, :] = on_own
    diag_rows[1:2, :] = jnp.concatenate(on_pack, axis=1)

    def packed_part():
        for u, product in enumerate(products(rows, rows)):
            at = slice(u * CUT, (u + 1) * CUT)
            part[:, at] = product + diag_rows[1:2, at] * d_pack[:, at]

    packed_part()
    pl.semaphore_wait(hello_sems.at[0], 2)
    hello(2)

    def take_halo(step, group):
        at = pl.ds(group * k_group, k_group)
        wait_recvs(step, group)
        halo = jnp.concatenate([recv_buf[step, j, at, :] for j in range(dirs)], axis=1)
        return split(halo)

    def stage(first_col, half):
        for i, weights in enumerate((w_high, w_low)):
            for u in units:
                tile_rows = slice(rows + u * CUT, rows + (u + 1) * CUT)
                tile_cols = slice(first_col + half * CUT, first_col + (half + 1) * CUT)
                pltpu.matmul_push_rhs(weights[tile_rows, tile_cols], staging_register=i, mxu_index=u)

    def multiply(high, low, half, slot):
        for operand, part_of, load in ((high, 0, 0), (low, 1, None), (high, 0, 1)):
            for u in units:
                acc = halo_accs[u][4 * slot + 2 * half + part_of]
                pltpu.matmul_acc_lhs(acc, operand[:, u * CUT : (u + 1) * CUT], load_staged_rhs=load)

    def collect(half, slot):
        i = 4 * slot + 2 * half
        return sum(pltpu.matmul_pop(halo_accs[u][i + 1]) for u in units) + sum(
            pltpu.matmul_pop(halo_accs[u][i]) for u in units
        )

    def iteration(step, carry):
        alpha = coef[2 * step][0:1]
        beta = coef[2 * step + 1][0:1]
        last = (step == ITERS - 2).astype(f32)

        def finish(group, half):
            at = slice(group * k_group, (group + 1) * k_group)
            lanes = slice(half * CUT, (half + 1) * CUT)
            r_part = r_pack[at, lanes] - part[at, lanes]
            d_part = alpha[:, lanes] * d_pack[at, lanes] + beta[:, lanes] * r_part
            x_old = x_pack[at, lanes]
            coupled = collect(half, group % 2)
            change = beta[:, lanes] * coupled
            going = (d_part + last * x_old) - change
            which = range(half * CUT // tile, (half + 1) * CUT // tile)
            for i, j in enumerate(which):
                send_buf[step + 1, j, at, :] = going[:, i * tile : (i + 1) * tile]
            start_sends(step + 1, group, which)
            d_new = d_part - change
            r_pack[at, lanes] = r_part - coupled
            d_pack[at, lanes] = d_new
            x_pack[at, lanes] = x_old + d_new

        stage(rows, 0)
        for group in range(groups):
            g0 = group * k_group
            high, low = take_halo(step, group)
            multiply(high, low, 0, group % 2)
            stage(rows, 1)
            multiply(high, low, 1, group % 2)
            if group + 1 < groups:
                stage(rows, 0)
            finish(group, 0)
            if group > 0:
                finish(group - 1, 1)
            ext[g0 : g0 + k_group, got] = high
            ext[k_all + g0 : k_all + g0 + k_group, got] = low
        finish(groups - 1, 1)
        wait_sends(step)
        for u, product in enumerate(products(2 * rows, 0)):
            at = slice(u * CUT, (u + 1) * CUT)
            r_new = r_own[:, at] - (product + diag_rows[0:1, at] * d_own[:, at])
            d_new = alpha[:, at] * d_own[:, at] + beta[:, at] * r_new
            r_own[:, at] = r_new
            d_own[:, at] = d_new
        for start in range(0, rows, CUT):
            at = slice(start, start + CUT)
            d_new = d_own[:, at]
            x_old = x_own[:, at]
            x_own[:, at] = x_old + d_new
            high, low = split(d_new + last * x_old)
            ext[0:k_all, at] = high
            ext[k_all : 2 * k_all, at] = low
        packed_part()
        return carry

    lax.fori_loop(0, ITERS - 1, iteration, 0)

    for u, product in enumerate(products(rows, 0)):
        at = slice(u * CUT, (u + 1) * CUT)
        r_own[:, at] = b_own[:, at] - (product + diag_rows[0:1, at] * x_own[:, at])
    for i in range(blk_rows):
        out_buf[i * tile : (i + 1) * tile, :] = jnp.transpose(x_own[:, i * tile : (i + 1) * tile])

    out_copy = pltpu.make_async_copy(out_buf, x_out, copy_sems.at[5])
    out_copy.start()
    pl.semaphore_wait(hello_sems.at[1], 2)

    def square(group):
        at = slice(group * k_group, (group + 1) * k_group)
        total = jnp.zeros((k_group, tile), f32)
        for half in range(2):
            final = r_own[at, half * CUT : (half + 1) * CUT] - collect(half, group % 2)
            final = final * final
            for i in range(CUT // tile):
                total = total + final[:, i * tile : (i + 1) * tile]
        return total

    squares = []
    stage(0, 0)
    for group in range(groups):
        high, low = take_halo(ITERS - 1, group)
        multiply(high, low, 0, group % 2)
        stage(0, 1)
        multiply(high, low, 1, group % 2)
        if group > 0:
            squares.append(square(group - 1))
        if group + 1 < groups:
            stage(0, 0)
    squares.append(square(groups - 1))
    squares = jnp.transpose(jnp.concatenate(squares, axis=0))
    mine = jnp.sum(squares, axis=0, keepdims=True)

    plane_send[...] = mine
    plane_recv[my_slot] = mine
    plane_copies = [
        pltpu.make_async_remote_copy(
            src_ref=plane_send,
            dst_ref=plane_recv.at[my_slot],
            send_sem=copy_sems.at[0],
            recv_sem=norm_sems.at[0],
            device_id=plane_target(step),
            device_id_type=MESH,
        )
        for step in plane_steps
    ]
    for copy in plane_copies:
        copy.start()
    others = plane_recv.at[pl.ds(0, in_plane - 1)]
    pltpu.make_async_copy(others, others, norm_sems.at[0]).wait()
    sums = [plane_recv[i] for i in range(in_plane)]
    while len(sums) > 1:
        sums = [sum(sums[i : i + 2]) for i in range(0, len(sums), 2)]
    mine = sums[0]

    axis_send[...] = mine
    own_copy = pltpu.make_async_copy(axis_send, axis_recv.at[my_plane], copy_sems.at[4])
    own_copy.start()
    axis_copies = [
        pltpu.make_async_remote_copy(
            src_ref=axis_send,
            dst_ref=axis_recv.at[my_plane],
            send_sem=copy_sems.at[2],
            recv_sem=norm_sems.at[1],
            device_id=axis_target(offset),
            device_id_type=MESH,
        )
        for offset in axis_steps
    ]
    for copy in axis_copies:
        copy.start()
    wait_sends(ITERS - 1)
    out_copy.wait()
    pltpu.make_async_copy(others, others, copy_sems.at[0]).wait()
    others = axis_recv.at[pl.ds(0, planes - 1)]
    pltpu.make_async_copy(others, others, norm_sems.at[1]).wait()
    own_copy.wait()
    pltpu.make_async_copy(others, others, copy_sems.at[2]).wait()


def kernel(shape, groups, k_all, rows, *refs):
    heights = (CUT, CUT, k_all, k_all) + 8 * (k_all // groups,)
    units = rows // CUT
    specs = [pltpu.ACC(unit)((height, CUT), jnp.float32) for unit in range(units) for height in heights]

    def body(*accs):
        per_unit = [accs[unit * len(heights) : (unit + 1) * len(heights)] for unit in range(units)]
        steps(per_unit, shape, *refs)

    pl.run_scoped(body, *specs)


def on_device(n_patch, n_sub, planes, sources, diag_coef, tiles, tile_cols, send_rows, recv_rows, bounds):
    rows = diag_coef.shape[0]
    k_all = sources.shape[0]
    blk_rows, per_row, tile, _ = tiles.shape
    dirs = send_rows.shape[1]
    n_blocks = 2 * blk_rows
    f32, bf16 = jnp.float32, jnp.bfloat16
    hbm = pl.BlockSpec(memory_space=pltpu.HBM)
    field = pltpu.VMEM((k_all, rows), f32)
    in_plane = n_patch // planes * n_sub
    x, sums = pl.pallas_call(
        functools.partial(kernel, (n_patch, n_sub, planes), GROUPS, k_all, rows),
        out_shape=(jax.ShapeDtypeStruct((rows, k_all), f32), jax.ShapeDtypeStruct((planes, 1, k_all), f32)),
        in_specs=[hbm] * 7,
        out_specs=(hbm, hbm),
        scratch_shapes=[
            pltpu.VMEM(sources.shape[::-1], jnp.int32),
            pltpu.VMEM((blk_rows, tile), f32),
            pltpu.SMEM(tile_cols.shape, jnp.int32),
            pltpu.VMEM(send_rows.shape[1:], jnp.int32),
            pltpu.VMEM(recv_rows.shape, jnp.int32),
            pltpu.SMEM(bounds.shape, f32),
            pltpu.VMEM(tiles.shape, f32),
            pltpu.VMEM((n_blocks, 2 * rows, tile), bf16),
            pltpu.VMEM((rows, rows), bf16),
            pltpu.VMEM((2 * tile, per_row * tile), bf16),
            pltpu.VMEM((2 * rows, 2 * rows), bf16),
            pltpu.VMEM((2 * rows, 2 * rows), bf16),
            pltpu.VMEM((2 * k_all, 2 * rows), bf16),
            field,
            field,
            field,
            field,
            field,
            field,
            field,
            field,
            pltpu.VMEM((2 * ITERS, 8, rows), f32),
            pltpu.VMEM((ITERS, dirs, k_all, tile), f32),
            pltpu.VMEM((ITERS, dirs, k_all, tile), f32),
            pltpu.VMEM((1, k_all), f32),
            pltpu.VMEM((in_plane, 1, k_all), f32),
            pltpu.VMEM((1, k_all), f32),
            pltpu.SemaphoreType.DMA((7,)),
            pltpu.SemaphoreType.DMA((2,)),
            pltpu.SemaphoreType.DMA((2, GROUPS)),
            pltpu.SemaphoreType.DMA((2,)),
            pltpu.VMEM((rows, k_all), f32),
            pltpu.SemaphoreType.REGULAR((2,)),
            pltpu.VMEM((8, rows), f32),
        ],
        compiler_params=pltpu.CompilerParams(
            collective_id=0, has_side_effects=True, vmem_limit_bytes=67_043_328
        ),
    )(
        sources.T,
        diag_coef.reshape(blk_rows, tile),
        tile_cols,
        send_rows[0],
        recv_rows,
        bounds,
        tiles,
    )
    return settle(x, sums)


def settle_kernel(x_in, sums_in, x_out, norm_out, x_buf, sums_buf, norm_buf, sems):
    read_sums = pltpu.make_async_copy(sums_in, sums_buf, sems.at[0])
    read_x = pltpu.make_async_copy(x_in, x_buf, sems.at[1])
    write_norm = pltpu.make_async_copy(norm_buf, norm_out, sems.at[0])
    write_x = pltpu.make_async_copy(x_buf, x_out, sems.at[1])
    read_sums.start()
    read_x.start()
    read_sums.wait()
    norm_buf[...] = jnp.sqrt(jnp.sum(sums_buf[...], axis=0))
    write_norm.start()
    read_x.wait()
    write_x.start()
    write_norm.wait()
    write_x.wait()


def settle(x, sums):
    hbm = pl.BlockSpec(memory_space=pl.ANY)
    norm_shape = jax.ShapeDtypeStruct(sums.shape[1:], sums.dtype)
    x, norm = pl.pallas_call(
        settle_kernel,
        out_shape=(jax.ShapeDtypeStruct(x.shape, x.dtype), norm_shape),
        in_specs=[hbm] * 2,
        out_specs=(hbm, hbm),
        scratch_shapes=[
            pltpu.VMEM(x.shape, x.dtype),
            pltpu.VMEM(sums.shape, sums.dtype),
            pltpu.VMEM(norm_shape.shape, norm_shape.dtype),
            pltpu.SemaphoreType.DMA((2,)),
        ],
        compiler_params=pltpu.CompilerParams(vmem_limit_bytes=67_043_328),
    )(x, sums)
    return x, norm[0]


def solution(mesh):
    n_patch, n_sub = mesh.shape["patch"], mesh.shape["sub"]
    both = ("patch", "sub")
    return jax.shard_map(
        functools.partial(on_device, n_patch, n_sub, PLANES),
        mesh=mesh,
        in_specs=(
            P(),
            P(both),
            P(both, None, None, None),
            P(both, None),
            P(both, None, None),
            P(both, None),
            P(),
        ),
        out_specs=(P(both, None), P()),
        check_vma=False,
    )
```
